32 devices in a mesh: px: 2 (over core), py: 4 (over z), ta: 4 (over y, x).
Axes of the slice: x: 2, y: 2, z: 4, core: 2. Of those that a mesh axis runs over, the one named last changes fastest.
Arguments:
- snapshots: bfloat16 [384, 5, 65536], P('ta', None, ('px', 'py')), may hold values from -6 to 6
- quad_weights: float32 [65536], P(('px', 'py')), may hold values from 1 to 10
- spectral_indices: int32 [32], replicated, may hold values from 0 to 127
Outputs:
- spectra: float32 [32, 2, 2, 5, 65536], P('ta', None, None, None, ('px', 'py'))
- gram: float32 [32, 2, 2, 2], P('ta')
The draws below stay inside these ranges and needn't reach their ends.
All inputs are finite; a program needn't handle non-finite values.
Results may differ from the reference program's by a relative error of at most 0.0042.
Values may be sent and summed in bfloat16 or wider, within the bound.
A program may use at most 128 MiB of HBM per device.

```python
import math
import jax
import jax.numpy as jnp
from jax import lax

VARS = 5
BLK = 256
HOP = 128
SEGMENT_NUMBER = 2
RECORD_LENGTH = 384
RETAINED_MODES = 32
POINTS = 65536


def place_ends(values, key, least, high):
    index_at = [jax.random.randint(jax.random.fold_in(key, axis), (), 0, length) for axis, length in enumerate(values.shape)]
    widest = values.shape.index(max(values.shape))
    beside = index_at[:widest] + [(index_at[widest] + 1) % values.shape[widest]] + index_at[widest + 1:]
    return values.at[tuple(index_at)].set(least).at[tuple(beside)].set(high)


def block_levels(key, dims, cuts, low, top_value):
    def one(axis_at, parts):
        draws = jax.random.uniform(jax.random.fold_in(jax.random.fold_in(key, 6), axis_at), (parts,), jnp.float32, low / len(cuts), top_value / len(cuts))
        return jnp.repeat(jnp.exp(draws), dims[axis_at] // parts).reshape((-1,) + (1,) * (len(dims) - axis_at - 1))

    loudness = one(*cuts[0])
    for cut in cuts[1:]:
        loudness = loudness * one(*cut)
    return loudness


def scatter_about(rng, dims, spread, most, pieces=(), kind=jnp.bfloat16):
    loudness = block_levels(rng, dims, pieces, -0.22, 0.18) if pieces else 1.0
    entries = jax.random.normal(rng, dims, jnp.float32) * spread * loudness
    return jnp.minimum(jnp.maximum(entries, -most), most).astype(kind)


def setup_inputs(seed: int = 0) -> dict:
    key_list = jax.random.split(jax.random.key(seed), 4)
    return {
        "snapshots": scatter_about(key_list[0], (RECORD_LENGTH, VARS, POINTS), 1.0, 6.0, ((0, 4), (2, 8))),
        "quad_weights": jnp.clip(jnp.exp(math.log(10.0) - 2.3025851 * jax.random.uniform(key_list[1], (POINTS,), jnp.float32) ** block_levels(key_list[1], (POINTS,), ((0, 8),), -0.2, 0.2)), 1.0, 10.0),
        "spectral_indices": place_ends(jax.random.randint(key_list[2], (RETAINED_MODES,), 0, BLK // 2), jax.random.fold_in(key_list[2], 1), 0, (BLK // 2) - 1).astype(jnp.int32),
    }


def make_rotation_multipliers(spectral_indices, temporal_locations):
    segment_beginnings = jnp.arange(SEGMENT_NUMBER, dtype=jnp.int32) * HOP
    segment_shifts = temporal_locations[None, :] - segment_beginnings[:, None]
    inside = (segment_shifts >= 0) & (segment_shifts < BLK)
    window = 0.5 - 0.5 * jnp.cos(2.0 * math.pi * segment_shifts.astype(jnp.float32) / BLK)
    window = jnp.where(inside, window, jnp.float32(0.0)) / jnp.sqrt(jnp.float32(3.0 * BLK / 8.0))
    phases = jnp.mod(spectral_indices[:, None, None] * segment_shifts[None, :, :], BLK)
    angles = 2.0 * math.pi * phases.astype(jnp.float32) / BLK
    real_part = jnp.cos(angles) * window[None]
    imag_part = -jnp.sin(angles) * window[None]
    gathered_segments = jnp.stack([real_part, imag_part], axis=2)
    return gathered_segments.reshape(RETAINED_MODES * SEGMENT_NUMBER * 2, temporal_locations.shape[0]).astype(jnp.bfloat16)

def gram_terms(spectra):
    flat = spectra.reshape(spectra.shape[0], 2 * SEGMENT_NUMBER, -1)
    inner = jnp.einsum('fam,fbm->fab', flat, flat, precision=lax.Precision.HIGHEST)
    inner = inner.reshape(spectra.shape[0], SEGMENT_NUMBER, 2, SEGMENT_NUMBER, 2)
    real_part = inner[:, :, 0, :, 0] + inner[:, :, 1, :, 1]
    imag_part = inner[:, :, 0, :, 1] - inner[:, :, 1, :, 0]
    return jnp.stack([real_part, imag_part], axis=-1)

def reference(snapshots, quad_weights, spectral_indices):
    temporal_locations = jnp.arange(RECORD_LENGTH, dtype=jnp.int32)
    rotation_multipliers = make_rotation_multipliers(spectral_indices, temporal_locations)
    flat_snapshots = snapshots.reshape(RECORD_LENGTH, VARS * POINTS)
    raw = jnp.dot(rotation_multipliers, flat_snapshots, preferred_element_type=jnp.float32)
    raw = raw.reshape(RETAINED_MODES, SEGMENT_NUMBER, 2, VARS, POINTS)
    spectra = raw * jnp.sqrt(quad_weights)
    gram = gram_terms(spectra) / jnp.float32(POINTS * VARS)
    return (spectra, gram)
```

```python
import functools
import math

import jax
import jax.numpy as jnp
from jax import lax
from jax.experimental import pallas as pl
from jax.experimental.pallas import tpu as pltpu
from jax.sharding import PartitionSpec as P

VARS = 5
BLK = 256
HOP = 128
SEGMENT_NUMBER = 2
RETAINED_MODES = 32

MESH = pl.DeviceIdType.MESH


def make_rotation_multipliers(spectral_indices, temporal_locations):
    segment_beginnings = jnp.arange(SEGMENT_NUMBER, dtype=jnp.int32) * HOP
    segment_shifts = temporal_locations[None, :] - segment_beginnings[:, None]
    inside = (segment_shifts >= 0) & (segment_shifts < BLK)
    window = 0.5 - 0.5 * jnp.cos(2.0 * math.pi * segment_shifts.astype(jnp.float32) / BLK)
    window = jnp.where(inside, window, jnp.float32(0.0)) / jnp.sqrt(jnp.float32(3.0 * BLK / 8.0))
    phases = jnp.mod(spectral_indices[:, None, None] * segment_shifts[None, :, :], BLK)
    angles = 2.0 * math.pi * phases.astype(jnp.float32) / BLK
    real_part = jnp.cos(angles) * window[None]
    imag_part = -jnp.sin(angles) * window[None]
    gathered_segments = jnp.stack([real_part, imag_part], axis=2)
    return gathered_segments.reshape(
        RETAINED_MODES * SEGMENT_NUMBER * 2, temporal_locations.shape[0]
    ).astype(jnp.bfloat16)


def gram_terms(spectra):
    flat = spectra.reshape(spectra.shape[0], 2 * SEGMENT_NUMBER, -1)
    inner = jnp.einsum("fam,fbm->fab", flat, flat, precision=lax.Precision.HIGHEST)
    inner = inner.reshape(spectra.shape[0], SEGMENT_NUMBER, 2, SEGMENT_NUMBER, 2)
    real_part = inner[:, :, 0, :, 0] + inner[:, :, 1, :, 1]
    imag_part = inner[:, :, 0, :, 1] - inner[:, :, 1, :, 0]
    return jnp.stack([real_part, imag_part], axis=-1)


def plain_on_device(snapshots, quad_weights, spectral_indices):
    record_length = snapshots.shape[0]
    point_count = snapshots.shape[2]
    groups = lax.axis_size("ta")
    temporal_locations = lax.axis_index("ta") * record_length + jnp.arange(
        record_length, dtype=jnp.int32
    )
    rotation_multipliers = make_rotation_multipliers(spectral_indices, temporal_locations)
    flat_snapshots = snapshots.reshape(record_length, VARS * point_count)
    raw = lax.psum_scatter(
        jnp.dot(rotation_multipliers, flat_snapshots, preferred_element_type=jnp.float32),
        "ta",
        scatter_dimension=0,
        tiled=True,
    )
    raw = raw.reshape(RETAINED_MODES // groups, SEGMENT_NUMBER, 2, VARS, point_count)
    spectra = raw * jnp.sqrt(quad_weights)
    summed = lax.psum(gram_terms(spectra), ("px", "py"))
    total_points = point_count * lax.axis_size("px") * lax.axis_size("py")
    gram = summed / jnp.float32(total_points * VARS)
    return (spectra, gram)


def sine_of_turn(m):
    quarter = BLK // 4
    r = jnp.bitwise_and(m + quarter, BLK - 1) - quarter
    r = jnp.where(r > quarter, BLK // 2 - r, r)
    x = r.astype(jnp.float32) * (2.0 * math.pi / BLK)
    y = x * x
    total = jnp.full_like(x, -1.0 / math.factorial(11))
    for n in (9, 7, 5, 3, 1):
        total = total * y + (1.0 if n % 4 == 1 else -1.0) / math.factorial(n)
    return total * x


def window_kernel(
    pieces, tail, tile, gram_scale,
    snap_hbm, weight_hbm, index_hbm, out_ref, gram_ref,
    snap, index_ref, weight_ref, twiddle, own, root,
    a_send, a_recv, n1_send, n1_recv, n2_send, n2_recv, m1_send, m1_recv,
    acc, gram_send, gram_recv,
    load_sem, index_sem, weight_sem,
    a_ssem, a_rsem, n1_ssem, n1_rsem, n2_ssem, n2_rsem, m1_ssem, m1_rsem,
    gram_ssem, gram_rsem,
):
    px, py, ta = lax.axis_index("px"), lax.axis_index("py"), lax.axis_index("ta")
    npx, npy = lax.axis_size("px"), lax.axis_size("py")
    variables, record, points = snap_hbm.shape
    modes = out_ref.shape[0]
    unit = 2 * modes
    steps = variables * pieces
    span = points // pieces
    half = span // 2
    short = span // tail
    f32, bf16 = jnp.float32, jnp.bfloat16

    inner = (ta == 1) | (ta == 2)
    outer = jnp.logical_not(inner)
    me = jnp.where(inner, ta - 1, ta // 3)
    sides = (jnp.where(inner, 0, 1), jnp.where(inner, 3, 2))

    def load(variable):
        return pltpu.make_async_copy(snap_hbm.at[variable], snap.at[variable], load_sem.at[variable])

    index_copy = pltpu.make_async_copy(index_hbm, index_ref, index_sem)
    weight_copy = pltpu.make_async_copy(weight_hbm, weight_ref, weight_sem)
    index_copy.start()

    peers = [
        (i, j, lax.rem(px + i, npx), lax.rem(py + j, npy))
        for i in range(npx) for j in range(npy) if i + j > 0
    ]
    barrier = pltpu.get_barrier_semaphore()
    for side in sides:
        pl.semaphore_signal(barrier, inc=1, device_id=(px, py, side), device_id_type=MESH)
    for _, _, x, y in peers:
        pl.semaphore_signal(barrier, inc=1, device_id=(x, y, ta), device_id_type=MESH)

    for variable in range(variables):
        load(variable).start()
    weight_copy.start()

    sublane = lax.broadcasted_iota(jnp.int32, (modes, record), 0)
    moment = lax.broadcasted_iota(jnp.int32, (modes, record), 1) + ta * record
    shifts, windows = [], []
    for block in range(SEGMENT_NUMBER):
        shift = moment - block * HOP
        inside = (shift >= 0) & (shift < BLK)
        hann = 0.5 - 0.5 * sine_of_turn(shift + BLK // 4)
        shifts.append(shift)
        windows.append(jnp.where(inside, hann, 0.0) / math.sqrt(3.0 * BLK / 8.0))
    index_copy.wait()
    for place, owner in enumerate((3 - ta, sides[0], sides[1], ta)):
        bins = jnp.zeros((modes, record), jnp.int32)
        for f in range(modes):
            bins = jnp.where(sublane == f, index_ref[owner * modes + f], bins)
        for block in range(SEGMENT_NUMBER):
            shift, hann = shifts[block], windows[block]
            phase = bins * shift
            rows = jnp.concatenate(
                [sine_of_turn(phase + BLK // 4) * hann, -sine_of_turn(phase) * hann], axis=0)
            if place < 3:
                at = jnp.where(inner, place * SEGMENT_NUMBER + block, block * 3 + place)
                twiddle[pl.ds(pl.multiple_of(at * unit, unit), unit), :] = rows.astype(bf16)
            else:
                own[block * unit:(block + 1) * unit, :] = rows.astype(bf16)
    acc[...] = jnp.zeros_like(acc)

    def remote(send, recv, ssem, rsem, side, *at):
        return pltpu.make_async_remote_copy(
            src_ref=send.at[(side, *at)], dst_ref=recv.at[(me, *at)],
            send_sem=ssem.at[side, at[0]], recv_sem=rsem.at[me, at[0]],
            device_id=(px, py, sides[side]), device_id_type=MESH,
        )

    def landed(send, recv, ssem, rsem, side, *at):
        return pltpu.make_async_remote_copy(
            src_ref=send.at[(side, *at)], dst_ref=recv.at[(side, *at)],
            send_sem=ssem.at[side, at[0]], recv_sem=rsem.at[side, at[0]],
            device_id=(px, py, sides[side]), device_id_type=MESH,
        )

    a_refs = (a_send, a_recv, a_ssem, a_rsem)
    n1_refs = (n1_send, n1_recv, n1_ssem, n1_rsem)
    n2_refs = (n2_send, n2_recv, n2_ssem, n2_rsem)

    def m1_copy(here, side, k, n=None):
        send, recv, ssem, rsem = m1_send.at[side, k], m1_recv.at[here, k], m1_ssem, m1_rsem
        if n is None:
            n = k
        else:
            columns = pl.ds(pl.multiple_of(n * short, short), short)
            send, recv, n = send.at[:, columns], recv.at[:, columns], k + n
        return pltpu.make_async_remote_copy(
            src_ref=send, dst_ref=recv, send_sem=ssem.at[side, n], recv_sem=rsem.at[here, n],
            device_id=(px, py, sides[side]), device_id_type=MESH,
        )

    def columns(k, at):
        return pl.ds(pl.multiple_of(lax.rem(k, pieces) * span + at, 128), tile)

    def transform(rows, k, at):
        return jnp.dot(rows, snap[k // pieces, :, columns(k, at)], preferred_element_type=f32)

    def loaded(k):
        @pl.when(lax.rem(k, pieces) == 0)
        def _():
            load(k // pieces).wait()

    def tiles(width):
        def run(body):
            @pl.loop(0, width // tile)
            def _(i):
                body(pl.multiple_of(i * tile, tile))
        return run

    def meet(k):
        @pl.when(k == 0)
        def _():
            pl.semaphore_wait(barrier, len(sides) + len(peers))

    def finish(k, at, both):
        here = columns(k, at)
        weight = root[:, here]
        (r0, i0), (r1, i1) = parts = [
            (both[b * unit:b * unit + modes] * weight, both[b * unit + modes:(b + 1) * unit] * weight)
            for b in range(SEGMENT_NUMBER)]
        terms = (r0 * r0 + i0 * i0, r1 * r1 + i1 * i1, r0 * r1 + i0 * i1, r0 * i1 - i0 * r1)
        for n, term in enumerate(terms):
            lanes = [term[:, c:c + 128] for c in range(0, tile, 128)]
            acc[n] += functools.reduce(jnp.add, lanes)
        for block, pair in enumerate(parts):
            for c in range(2):
                out_ref[:, block, k // pieces, c, here] = pair[c]

    def weights():
        weight_copy.wait()
        root[...] = jnp.sqrt(weight_ref[...])

    @pl.when(inner)
    def _():
        @pl.loop(0, steps)
        def _(k):
            loaded(k)
            for side in range(2):
                @tiles(half)
                def _(at):
                    a_send[side, k, :, pl.ds(at, tile)] = transform(
                        twiddle[0:2 * unit, :], k, side * half + at).astype(bf16)
                if side == 0:
                    meet(k)
                remote(*a_refs, side, k).start()

        @pl.loop(0, steps)
        def _(k):
            for dependent in range(2):
                first = half * (me if dependent else 1 - me)
                if dependent:
                    for side in range(2):
                        landed(*n2_refs, side, k).wait_recv()

                @tiles(half)
                def _(at):
                    product = transform(twiddle[2 * unit:6 * unit, :], k, first + at)
                    there = pl.ds(pl.multiple_of(first + at, 128), tile)
                    for side in range(2):
                        for block in range(SEGMENT_NUMBER):
                            r = (side * SEGMENT_NUMBER + block) * unit
                            rows = product[r:r + unit]
                            if dependent and block != side:
                                rows = rows + n2_recv[block, k, :, pl.ds(at, tile)].astype(f32)
                            m1_send[side, k, block * unit:(block + 1) * unit, there] = rows.astype(bf16)

            @pl.when(k < steps - 1)
            def _():
                for side in range(2):
                    m1_copy(me, side, k).start()

            @pl.when(k == steps - 1)
            def _():
                for n in range(tail):
                    for side in range(2):
                        m1_copy(me, side, k, n).start()

        weights()

        @pl.loop(0, steps)
        def _(k):
            for side in range(2):
                landed(*a_refs, side, k).wait_recv()
                landed(*n1_refs, side, k).wait_recv()

            for side in range(2):
                @tiles(half)
                def _(at):
                    both = transform(own[...], k, side * half + at)
                    both = both + a_recv[side, k, :, pl.ds(at, tile)].astype(f32)
                    extra = n1_recv[1 - side, k, :, pl.ds(at, tile)].astype(f32)
                    rows = [both[:unit], both[unit:]]
                    rows[1 - side] = rows[1 - side] + extra
                    finish(k, side * half + at, jnp.concatenate(rows, axis=0))

    @pl.when(outer)
    def _():
        base = me * (3 * unit)
        far = pl.ds(pl.multiple_of(base, unit), unit)
        near = pl.ds(pl.multiple_of(base + unit, unit), 2 * unit)

        @pl.loop(0, steps)
        def _(k):
            loaded(k)
            for side in range(2):
                @tiles(half)
                def _(at):
                    n2_send[side, k, :, pl.ds(at, tile)] = transform(
                        twiddle[far, :], k, side * half + at).astype(bf16)
                if side == 0:
                    meet(k)
                remote(*n2_refs, side, k).start()

        @pl.loop(0, steps)
        def _(k):
            @tiles(half)
            def _(at):
                product = transform(twiddle[near, :], k, (1 - me) * half + at)
                for side in range(2):
                    n1_send[side, k, :, pl.ds(at, tile)] = product[side * unit:(side + 1) * unit].astype(bf16)
            for side in range(2):
                remote(*n1_refs, side, k).start()
            for side in range(2):
                landed(*a_refs, side, k).wait_recv()

            @tiles(half)
            def _(at):
                here = pl.ds(at, tile)
                product = transform(twiddle[near, :], k, me * half + at)
                for side in range(2):
                    rows = product[side * unit:(side + 1) * unit]
                    for block in range(SEGMENT_NUMBER):
                        there = slice(block * unit, (block + 1) * unit)
                        came = a_recv[1 - side, k, there, here].astype(f32)
                        total = came + jnp.where(me == block, rows, 0.0)
                        a_send[side, k, there, here] = total.astype(bf16)
            for side in range(2):
                remote(*a_refs, side, k).start()

        weights()

        def arrived(k, at):
            there = pl.ds(at, tile)
            both = transform(own[...], k, at)
            finish(k, at, both + (
                m1_recv[0, k, :, there].astype(f32) + m1_recv[1, k, :, there].astype(f32)))

        @pl.loop(0, steps - 1)
        def _(k):
            for side in range(2):
                m1_copy(side, side, k).wait_recv()
            tiles(span)(functools.partial(arrived, k))

        @pl.loop(0, tail)
        def _(n):
            for side in range(2):
                m1_copy(side, side, steps - 1, n).wait_recv()
            tiles(short)(lambda at: arrived(steps - 1, pl.multiple_of(n * short + at, tile)))

    lane = lax.broadcasted_iota(jnp.int32, gram_send.shape, 1)
    sums = jnp.zeros(gram_send.shape, f32)
    for n in range(4):
        sums = jnp.where(lane == n, jnp.sum(acc[n], axis=1, keepdims=True), sums)
    gram_send[...] = sums

    def gram_copy(n):
        i, j, x, y = peers[n]
        return pltpu.make_async_remote_copy(
            src_ref=gram_send, dst_ref=gram_recv.at[n],
            send_sem=gram_ssem.at[n], recv_sem=gram_rsem.at[n],
            device_id=(x, y, ta), device_id_type=MESH,
        )

    for n in range(len(peers)):
        gram_copy(n).start()

    @pl.when(inner)
    def _():
        @pl.loop(0, steps)
        def _(k):
            for side in range(2):
                remote(*a_refs, side, k).wait_send()

                @pl.when(k < steps - 1)
                def _():
                    m1_copy(me, side, k).wait_send()

        @pl.loop(0, tail)
        def _(n):
            for side in range(2):
                m1_copy(me, side, steps - 1, n).wait_send()

    @pl.when(outer)
    def _():
        @pl.loop(0, steps)
        def _(k):
            for side in range(2):
                for refs in (a_refs, n1_refs, n2_refs):
                    remote(*refs, side, k).wait_send()

    total = sums
    for n in range(len(peers)):
        gram_copy(n).wait()
        total = total + gram_recv[n]
    row = lax.broadcasted_iota(jnp.int32, (8, 128), 0)
    lane = lax.broadcasted_iota(jnp.int32, (8, 128), 1)
    pick = jnp.zeros((8, 128), f32)
    for r, n, sign in ((0, 0, 1.0), (2, 2, 1.0), (3, 3, 1.0), (4, 2, 1.0), (5, 3, -1.0), (6, 1, 1.0)):
        pick = jnp.where((row == r) & (lane == n), sign, pick)
    gram_ref[...] = gram_scale * lax.dot_general(
        pick, total, (((1,), (1,)), ((), ())),
        precision=lax.Precision.HIGHEST, preferred_element_type=f32,
    )


def flush_kernel(spectra, gram, spectra_out, gram_out, sems):
    copies = [pltpu.make_async_copy(gram, gram_out, sems.at[0])]
    for f in range(spectra.shape[0]):
        copies.append(pltpu.make_async_copy(spectra.at[f], spectra_out.at[f], sems.at[f + 1]))
    for copy in copies:
        copy.start()
    for copy in copies:
        copy.wait()


def kernel_on_device(snapshots, quad_weights, spectral_indices):
    record, variables, points = snapshots.shape
    groups = lax.axis_size("ta")
    npx, npy = lax.axis_size("px"), lax.axis_size("py")
    modes = spectral_indices.shape[0] // groups
    unit = 2 * modes
    pieces, tail = 2, 4
    span = points // pieces
    half = span // 2
    tile = math.gcd(512, span // tail)
    steps = variables * pieces
    bf16, f32 = jnp.bfloat16, jnp.float32
    peers = npx * npy - 1
    dma = pltpu.SemaphoreType.DMA
    hbm = pl.BlockSpec(memory_space=pltpu.HBM)
    vmem = pl.BlockSpec(memory_space=pltpu.VMEM)
    spectra, gram = pl.pallas_call(
        functools.partial(
            window_kernel, pieces, tail, tile, 1.0 / (points * npx * npy * variables)),
        out_shape=(
            jax.ShapeDtypeStruct((modes, SEGMENT_NUMBER, variables, 2, points), f32),
            jax.ShapeDtypeStruct((SEGMENT_NUMBER * SEGMENT_NUMBER * 2, modes), f32),
        ),
        in_specs=[hbm, hbm, hbm],
        out_specs=(vmem, vmem),
        scratch_shapes=[
            pltpu.VMEM((variables, record, points), bf16),
            pltpu.SMEM(spectral_indices.shape, jnp.int32),
            pltpu.VMEM((1, points), f32),
            pltpu.VMEM((3 * SEGMENT_NUMBER * unit, record), bf16),
            pltpu.VMEM((SEGMENT_NUMBER * unit, record), bf16),
            pltpu.VMEM((1, points), f32),
            pltpu.VMEM((2, steps, SEGMENT_NUMBER * unit, half), bf16),
            pltpu.VMEM((2, steps, SEGMENT_NUMBER * unit, half), bf16),
            pltpu.VMEM((2, steps, unit, half), bf16),
            pltpu.VMEM((2, steps, unit, half), bf16),
            pltpu.VMEM((2, steps, unit, half), bf16),
            pltpu.VMEM((2, steps, unit, half), bf16),
            pltpu.VMEM((2, steps, SEGMENT_NUMBER * unit, span), bf16),
            pltpu.VMEM((2, steps, SEGMENT_NUMBER * unit, span), bf16),
            pltpu.VMEM((4, modes, 128), f32),
            pltpu.VMEM((modes, 128), f32),
            pltpu.VMEM((peers, modes, 128), f32),
            dma((variables,)), dma, dma,
            dma((2, steps)), dma((2, steps)), dma((2, steps)), dma((2, steps)),
            dma((2, steps)), dma((2, steps)),
            dma((2, steps - 1 + tail)), dma((2, steps - 1 + tail)),
            dma((peers,)), dma((peers,)),
        ],
        compiler_params=pltpu.CompilerParams(
            collective_id=0, has_side_effects=True, vmem_limit_bytes=44 * 1024 * 1024),
        name="window_transform",
    )(*(
        pltpu.with_memory_space_constraint(a, pltpu.HBM)
        for a in (snapshots.transpose(1, 0, 2), quad_weights.reshape(1, points), spectral_indices)
    ))
    spectra, gram = pl.pallas_call(
        flush_kernel,
        out_shape=(
            jax.ShapeDtypeStruct(spectra.shape, f32), jax.ShapeDtypeStruct(gram.shape, f32)),
        in_specs=[vmem, vmem],
        out_specs=(hbm, hbm),
        scratch_shapes=[dma((modes + 1,))],
        compiler_params=pltpu.CompilerParams(vmem_limit_bytes=1024 * 1024),
        name="flush",
    )(*(pltpu.with_memory_space_constraint(a, pltpu.VMEM) for a in (spectra, gram)))
    gram = gram.reshape(SEGMENT_NUMBER, SEGMENT_NUMBER, 2, modes)
    return spectra.transpose(0, 1, 3, 2, 4), gram.transpose(3, 0, 1, 2)


def solution(mesh):
    square = mesh.shape["ta"] == 4
    return jax.shard_map(
        kernel_on_device if square else plain_on_device,
        mesh=mesh,
        in_specs=(P("ta", None, ("px", "py")), P(("px", "py")), P()),
        out_specs=(P("ta", None, None, None, ("px", "py")), P("ta", None, None, None)),
        check_vma=False,
    )
```

```python
import functools
import math

import jax
import jax.numpy as jnp
from jax import lax
from jax.experimental import pallas as pl
from jax.experimental.pallas import tpu as pltpu
from jax.sharding import PartitionSpec as P

VARS = 5
BLK = 256
HOP = 128
SEGMENT_NUMBER = 2
RETAINED_MODES = 32

MESH = pl.DeviceIdType.MESH


def make_rotation_multipliers(spectral_indices, temporal_locations):
    segment_beginnings = jnp.arange(SEGMENT_NUMBER, dtype=jnp.int32) * HOP
    segment_shifts = temporal_locations[None, :] - segment_beginnings[:, None]
    inside = (segment_shifts >= 0) & (segment_shifts < BLK)
    window = 0.5 - 0.5 * jnp.cos(2.0 * math.pi * segment_shifts.astype(jnp.float32) / BLK)
    window = jnp.where(inside, window, jnp.float32(0.0)) / jnp.sqrt(jnp.float32(3.0 * BLK / 8.0))
    phases = jnp.mod(spectral_indices[:, None, None] * segment_shifts[None, :, :], BLK)
    angles = 2.0 * math.pi * phases.astype(jnp.float32) / BLK
    real_part = jnp.cos(angles) * window[None]
    imag_part = -jnp.sin(angles) * window[None]
    gathered_segments = jnp.stack([real_part, imag_part], axis=2)
    return gathered_segments.reshape(
        RETAINED_MODES * SEGMENT_NUMBER * 2, temporal_locations.shape[0]
    ).astype(jnp.bfloat16)


def gram_terms(spectra):
    flat = spectra.reshape(spectra.shape[0], 2 * SEGMENT_NUMBER, -1)
    inner = jnp.einsum("fam,fbm->fab", flat, flat, precision=lax.Precision.HIGHEST)
    inner = inner.reshape(spectra.shape[0], SEGMENT_NUMBER, 2, SEGMENT_NUMBER, 2)
    real_part = inner[:, :, 0, :, 0] + inner[:, :, 1, :, 1]
    imag_part = inner[:, :, 0, :, 1] - inner[:, :, 1, :, 0]
    return jnp.stack([real_part, imag_part], axis=-1)


def plain_on_device(snapshots, quad_weights, spectral_indices):
    record_length = snapshots.shape[0]
    point_count = snapshots.shape[2]
    groups = lax.axis_size("ta")
    temporal_locations = lax.axis_index("ta") * record_length + jnp.arange(
        record_length, dtype=jnp.int32
    )
    rotation_multipliers = make_rotation_multipliers(spectral_indices, temporal_locations)
    flat_snapshots = snapshots.reshape(record_length, VARS * point_count)
    raw = lax.psum_scatter(
        jnp.dot(rotation_multipliers, flat_snapshots, preferred_element_type=jnp.float32),
        "ta",
        scatter_dimension=0,
        tiled=True,
    )
    raw = raw.reshape(RETAINED_MODES // groups, SEGMENT_NUMBER, 2, VARS, point_count)
    spectra = raw * jnp.sqrt(quad_weights)
    summed = lax.psum(gram_terms(spectra), ("px", "py"))
    total_points = point_count * lax.axis_size("px") * lax.axis_size("py")
    gram = summed / jnp.float32(total_points * VARS)
    return (spectra, gram)


def sine_of_turn(m):
    quarter = BLK // 4
    r = jnp.bitwise_and(m + quarter, BLK - 1) - quarter
    r = jnp.where(r > quarter, BLK // 2 - r, r)
    x = r.astype(jnp.float32) * (2.0 * math.pi / BLK)
    y = x * x
    total = jnp.full_like(x, -1.0 / math.factorial(11))
    for n in (9, 7, 5, 3, 1):
        total = total * y + (1.0 if n % 4 == 1 else -1.0) / math.factorial(n)
    return total * x


def window_kernel(
    pieces, tail, tile, gram_scale,
    snap_hbm, weight_hbm, index_hbm, out_ref, gram_ref,
    snap, index_ref, weight_ref, twiddle, own, root,
    a_send, a_recv, n1_send, n1_recv, n2_send, n2_recv, m1_send, m1_recv,
    p_send, p_recv, pre, e_send, e_recv, acc, gram_send, gram_recv,
    load_sem, index_sem, weight_sem,
    a_ssem, a_rsem, n1_ssem, n1_rsem, n2_ssem, n2_rsem, m1_ssem, m1_rsem,
    p_ssem, p_rsem, e_ssem, e_rsem, gram_ssem, gram_rsem,
):
    px, py, ta = lax.axis_index("px"), lax.axis_index("py"), lax.axis_index("ta")
    npx, npy = lax.axis_size("px"), lax.axis_size("py")
    variables, record, points = snap_hbm.shape
    modes = out_ref.shape[0]
    unit = 2 * modes
    steps = variables * pieces
    span = points // pieces
    half = span // 2
    short = span // tail
    common = steps - 2
    f32, bf16 = jnp.float32, jnp.bfloat16

    inner = (ta == 1) | (ta == 2)
    outer = jnp.logical_not(inner)
    me = jnp.where(inner, ta - 1, ta // 3)
    sides = (jnp.where(inner, 0, 1), jnp.where(inner, 3, 2))

    def load(k):
        there = pl.ds(pl.multiple_of(lax.rem(k, pieces) * span, span), span)
        return pltpu.make_async_copy(
            snap_hbm.at[k // pieces, :, there], snap.at[k // pieces, :, there], load_sem.at[k])

    index_copy = pltpu.make_async_copy(index_hbm, index_ref, index_sem)
    weight_copy = pltpu.make_async_copy(weight_hbm, weight_ref, weight_sem)
    index_copy.start()
    load(0).start()

    peers = [
        (i, j, lax.rem(px + i, npx), lax.rem(py + j, npy))
        for i in range(npx) for j in range(npy) if i + j > 0
    ]
    barrier = pltpu.get_barrier_semaphore()
    for side in sides:
        pl.semaphore_signal(barrier, inc=1, device_id=(px, py, side), device_id_type=MESH)
    for _, _, x, y in peers:
        pl.semaphore_signal(barrier, inc=1, device_id=(x, y, ta), device_id_type=MESH)

    sublane = lax.broadcasted_iota(jnp.int32, (modes, record), 0)
    moment = lax.broadcasted_iota(jnp.int32, (modes, record), 1) + ta * record
    shifts, windows = [], []
    for block in range(SEGMENT_NUMBER):
        shift = moment - block * HOP
        inside = (shift >= 0) & (shift < BLK)
        hann = 0.5 - 0.5 * sine_of_turn(shift + BLK // 4)
        shifts.append(shift)
        windows.append(jnp.where(inside, hann, 0.0) / math.sqrt(3.0 * BLK / 8.0))
    index_copy.wait()
    for place, owner in enumerate((3 - ta, sides[0], sides[1], ta)):
        bins = jnp.zeros((modes, record), jnp.int32)
        for f in range(modes):
            bins = jnp.where(sublane == f, index_ref[owner * modes + f], bins)
        for block in range(SEGMENT_NUMBER):
            shift, hann = shifts[block], windows[block]
            phase = bins * shift
            rows = jnp.concatenate(
                [sine_of_turn(phase + BLK // 4) * hann, -sine_of_turn(phase) * hann], axis=0)
            if place < 3:
                at = jnp.where(inner, place * SEGMENT_NUMBER + block, block * 3 + place)
                twiddle[pl.ds(pl.multiple_of(at * unit, unit), unit), :] = rows.astype(bf16)
            else:
                own[block * unit:(block + 1) * unit, :] = rows.astype(bf16)
    acc[...] = jnp.zeros_like(acc)

    def remote(send, recv, ssem, rsem, side, *at):
        return pltpu.make_async_remote_copy(
            src_ref=send.at[(side, *at)], dst_ref=recv.at[(me, *at)],
            send_sem=ssem.at[side, at[0]], recv_sem=rsem.at[me, at[0]],
            device_id=(px, py, sides[side]), device_id_type=MESH,
        )

    def landed(send, recv, ssem, rsem, side, *at):
        return pltpu.make_async_remote_copy(
            src_ref=send.at[(side, *at)], dst_ref=recv.at[(side, *at)],
            send_sem=ssem.at[side, at[0]], recv_sem=rsem.at[side, at[0]],
            device_id=(px, py, sides[side]), device_id_type=MESH,
        )

    a_refs = (a_send, a_recv, a_ssem, a_rsem)
    n1_refs = (n1_send, n1_recv, n1_ssem, n1_rsem)
    n2_refs = (n2_send, n2_recv, n2_ssem, n2_rsem)

    def m1_copy(here, side, k, n=None):
        send, recv, ssem, rsem = m1_send.at[side, k], m1_recv.at[here, k], m1_ssem, m1_rsem
        if n is None:
            n = k
        else:
            columns = pl.ds(pl.multiple_of(n * short, short), short)
            send, recv, n = send.at[:, columns], recv.at[:, columns], steps + n
        return pltpu.make_async_remote_copy(
            src_ref=send, dst_ref=recv, send_sem=ssem.at[side, n], recv_sem=rsem.at[here, n],
            device_id=(px, py, sides[side]), device_id_type=MESH,
        )

    def lone_copy(send, recv, ssem, rsem, here, side):
        return pltpu.make_async_remote_copy(
            src_ref=send.at[side], dst_ref=recv.at[here],
            send_sem=ssem.at[side], recv_sem=rsem.at[here],
            device_id=(px, py, sides[side]), device_id_type=MESH,
        )

    p_refs = (p_send, p_recv, p_ssem, p_rsem)
    e_refs = (e_send, e_recv, e_ssem, e_rsem)

    def columns(k, at):
        return pl.ds(pl.multiple_of(lax.rem(k, pieces) * span + at, 128), tile)

    def transform(rows, k, at):
        return jnp.dot(rows, snap[k // pieces, :, columns(k, at)], preferred_element_type=f32)

    def loaded(k):
        load(k).wait()

        @pl.when(k == 0)
        def _():
            for later in range(1, steps):
                load(later).start()
            weight_copy.start()

    def tiles(width):
        def run(body):
            @pl.loop(0, width // tile)
            def _(i):
                body(pl.multiple_of(i * tile, tile))
        return run

    def meet(k):
        @pl.when(k == 0)
        def _():
            pl.semaphore_wait(barrier, len(sides) + len(peers))

    def weighted(k, at, both):
        weight = root[:, columns(k, at)]
        return [
            (both[b * unit:b * unit + modes] * weight, both[b * unit + modes:(b + 1) * unit] * weight)
            for b in range(SEGMENT_NUMBER)]

    def add_terms(place, parts):
        (r0, i0), (r1, i1) = parts
        terms = (r0 * r0 + i0 * i0, r1 * r1 + i1 * i1, r0 * r1 + i0 * i1, r0 * i1 - i0 * r1)
        for n, term in enumerate(terms):
            lanes = [term[:, c:c + 128] for c in range(0, tile, 128)]
            acc[place, n] += functools.reduce(jnp.add, lanes)

    def store(k, at, parts):
        here = columns(k, at)
        for block, pair in enumerate(parts):
            for c in range(2):
                out_ref[:, block, k // pieces, c, here] = pair[c]

    def sums_of(place):
        lane = lax.broadcasted_iota(jnp.int32, gram_send.shape, 1)
        sums = jnp.zeros(gram_send.shape, f32)
        for n in range(4):
            sums = jnp.where(lane == n, jnp.sum(acc[place, n], axis=1, keepdims=True), sums)
        return sums

    def gram_copy(n):
        i, j, x, y = peers[n]
        return pltpu.make_async_remote_copy(
            src_ref=gram_send, dst_ref=gram_recv.at[n],
            send_sem=gram_ssem.at[n], recv_sem=gram_rsem.at[n],
            device_id=(x, y, ta), device_id_type=MESH,
        )

    def exchange(sums):
        gram_send[...] = sums
        for n in range(len(peers)):
            gram_copy(n).start()

    def weights():
        weight_copy.wait()
        root[...] = jnp.sqrt(weight_ref[...])

    def gather():
        total = gram_send[...]
        for n in range(len(peers)):
            gram_copy(n).wait()
            total = total + gram_recv[n]
        row = lax.broadcasted_iota(jnp.int32, (8, 128), 0)
        lane = lax.broadcasted_iota(jnp.int32, (8, 128), 1)
        pick = jnp.zeros((8, 128), f32)
        for r, n, sign in ((0, 0, 1.0), (2, 2, 1.0), (3, 3, 1.0), (4, 2, 1.0), (5, 3, -1.0), (6, 1, 1.0)):
            pick = jnp.where((row == r) & (lane == n), sign, pick)
        gram_ref[...] = gram_scale * lax.dot_general(
            pick, total, (((1,), (1,)), ((), ())),
            precision=lax.Precision.HIGHEST, preferred_element_type=f32,
        )

    @pl.when(inner)
    def _():
        @pl.loop(0, steps)
        def _(k):
            loaded(k)
            for side in range(2):
                @tiles(half)
                def _(at):
                    a_send[side, k, :, pl.ds(at, tile)] = transform(
                        twiddle[0:2 * unit, :], k, side * half + at).astype(bf16)
                if side == 0:
                    meet(k)
                remote(*a_refs, side, k).start()

        @pl.loop(0, steps)
        def _(j):
            last = j == steps - 1
            k = jnp.where(j == 0, steps - 1 - me, jnp.where(last, common + me, j - 1))
            for dependent in range(2):
                first = half * (me if dependent else 1 - me)
                if dependent:
                    for side in range(2):
                        landed(*n2_refs, side, k).wait_recv()

                @tiles(half)
                def _(at):
                    product = transform(twiddle[2 * unit:6 * unit, :], k, first + at)
                    there = pl.ds(pl.multiple_of(first + at, 128), tile)
                    for side in range(2):
                        for block in range(SEGMENT_NUMBER):
                            r = (side * SEGMENT_NUMBER + block) * unit
                            rows = product[r:r + unit]
                            if dependent and block != side:
                                rows = rows + n2_recv[block, k, :, pl.ds(at, tile)].astype(f32)
                            m1_send[side, k, block * unit:(block + 1) * unit, there] = rows.astype(bf16)

            @pl.when(jnp.logical_not(last))
            def _():
                for side in range(2):
                    m1_copy(me, side, k).start()

        weights()

        @pl.loop(0, steps)
        def _(k):
            for side in range(2):
                landed(*a_refs, side, k).wait_recv()
                landed(*n1_refs, side, k).wait_recv()

            for side in range(2):
                @tiles(half)
                def _(at):
                    both = transform(own[...], k, side * half + at)
                    both = both + a_recv[side, k, :, pl.ds(at, tile)].astype(f32)
                    extra = n1_recv[1 - side, k, :, pl.ds(at, tile)].astype(f32)
                    rows = [both[:unit], both[unit:]]
                    rows[1 - side] = rows[1 - side] + extra
                    parts = weighted(k, side * half + at, jnp.concatenate(rows, axis=0))
                    add_terms(0, parts)
                    store(k, side * half + at, parts)

        exchange(sums_of(0))
        for side in range(2):
            lone_copy(*p_refs, side, side).wait_recv()

            @tiles(span)
            def _(at):
                there = pl.ds(at, tile)
                k = common + me
                both = p_recv[side, :, there].astype(f32) + m1_send[side, k, :, there].astype(f32)
                add_terms(1 + side, weighted(k, at, both))

            e_send[side] = sums_of(1 + side)
            lone_copy(*e_refs, me, side).start()

        for n in range(tail):
            for side in range(2):
                m1_copy(me, side, common + me, n).start()

        gather()
        for side in range(2):
            lone_copy(*e_refs, me, side).wait_send()

        @pl.loop(0, steps)
        def _(k):
            for side in range(2):
                remote(*a_refs, side, k).wait_send()

                @pl.when(k != common + me)
                def _():
                    m1_copy(me, side, k).wait_send()

        @pl.loop(0, tail)
        def _(n):
            for side in range(2):
                m1_copy(me, side, common + me, n).wait_send()

    @pl.when(outer)
    def _():
        base = me * (3 * unit)
        far = pl.ds(pl.multiple_of(base, unit), unit)
        near = pl.ds(pl.multiple_of(base + unit, unit), 2 * unit)

        @pl.loop(0, steps)
        def _(k):
            loaded(k)
            for side in range(2):
                @tiles(half)
                def _(at):
                    n2_send[side, k, :, pl.ds(at, tile)] = transform(
                        twiddle[far, :], k, side * half + at).astype(bf16)
                if side == 0:
                    meet(k)
                remote(*n2_refs, side, k).start()

        @pl.loop(0, steps)
        def _(k):
            @tiles(half)
            def _(at):
                product = transform(twiddle[near, :], k, (1 - me) * half + at)
                for side in range(2):
                    n1_send[side, k, :, pl.ds(at, tile)] = product[side * unit:(side + 1) * unit].astype(bf16)
            for side in range(2):
                remote(*n1_refs, side, k).start()
            for side in range(2):
                landed(*a_refs, side, k).wait_recv()

            @tiles(half)
            def _(at):
                here = pl.ds(at, tile)
                product = transform(twiddle[near, :], k, me * half + at)
                for side in range(2):
                    rows = product[side * unit:(side + 1) * unit]
                    for block in range(SEGMENT_NUMBER):
                        there = slice(block * unit, (block + 1) * unit)
                        came = a_recv[1 - side, k, there, here].astype(f32)
                        total = came + jnp.where(me == block, rows, 0.0)
                        a_send[side, k, there, here] = total.astype(bf16)
            for side in range(2):
                remote(*a_refs, side, k).start()

        weights()

        for side in range(2):
            k = common + side
            m1_copy(1 - side, 1 - side, k).wait_recv()

            @tiles(span)
            def _(at):
                there = pl.ds(at, tile)
                both = transform(own[...], k, at) + m1_recv[1 - side, k, :, there].astype(f32)
                p_send[side, :, there] = both.astype(bf16)
                pre[side, :, there] = both

            lone_copy(*p_refs, me, side).start()

        def arrived(k, at):
            there = pl.ds(at, tile)
            both = transform(own[...], k, at)
            return weighted(k, at, both + (
                m1_recv[0, k, :, there].astype(f32) + m1_recv[1, k, :, there].astype(f32)))

        @pl.loop(0, common)
        def _(k):
            for side in range(2):
                m1_copy(side, side, k).wait_recv()

            @tiles(span)
            def _(at):
                parts = arrived(k, at)
                add_terms(0, parts)
                store(k, at, parts)

        sums = sums_of(0)
        for side in range(2):
            lone_copy(*e_refs, side, side).wait_recv()
            sums = sums + e_recv[side]
        exchange(sums)

        @pl.loop(0, steps)
        def _(k):
            for side in range(2):
                for refs in (a_refs, n1_refs, n2_refs):
                    remote(*refs, side, k).wait_send()

        for side in range(2):
            lone_copy(*p_refs, me, side).wait_send()

        @pl.loop(0, tail)
        def _(n):
            @pl.when(n == tail - 1)
            def _():
                gather()

            for side in range(2):
                k = common + side
                m1_copy(side, side, k, n).wait_recv()

                for c in range(0, short, tile):
                    at = pl.multiple_of(n * short + c, tile)
                    there = pl.ds(at, tile)
                    store(k, at, weighted(
                        k, at, pre[side, :, there] + m1_recv[side, k, :, there].astype(f32)))


def flush_kernel(spectra, gram, spectra_out, gram_out, sems):
    copies = [pltpu.make_async_copy(gram, gram_out, sems.at[0])]
    for f in range(spectra.shape[0]):
        copies.append(pltpu.make_async_copy(spectra.at[f], spectra_out.at[f], sems.at[f + 1]))
    for copy in copies:
        copy.start()
    for copy in copies:
        copy.wait()


def kernel_on_device(snapshots, quad_weights, spectral_indices):
    record, variables, points = snapshots.shape
    groups = lax.axis_size("ta")
    npx, npy = lax.axis_size("px"), lax.axis_size("py")
    modes = spectral_indices.shape[0] // groups
    unit = 2 * modes
    pieces, tail = 2, 4
    span = points // pieces
    half = span // 2
    tile = math.gcd(512, span // tail)
    steps = variables * pieces
    bf16, f32 = jnp.bfloat16, jnp.float32
    peers = npx * npy - 1
    dma = pltpu.SemaphoreType.DMA
    hbm = pl.BlockSpec(memory_space=pltpu.HBM)
    vmem = pl.BlockSpec(memory_space=pltpu.VMEM)
    spectra, gram = pl.pallas_call(
        functools.partial(
            window_kernel, pieces, tail, tile, 1.0 / (points * npx * npy * variables)),
        out_shape=(
            jax.ShapeDtypeStruct((modes, SEGMENT_NUMBER, variables, 2, points), f32),
            jax.ShapeDtypeStruct((SEGMENT_NUMBER * SEGMENT_NUMBER * 2, modes), f32),
        ),
        in_specs=[hbm, hbm, hbm],
        out_specs=(vmem, vmem),
        scratch_shapes=[
            pltpu.VMEM((variables, record, points), bf16),
            pltpu.SMEM(spectral_indices.shape, jnp.int32),
            pltpu.VMEM((1, points), f32),
            pltpu.VMEM((3 * SEGMENT_NUMBER * unit, record), bf16),
            pltpu.VMEM((SEGMENT_NUMBER * unit, record), bf16),
            pltpu.VMEM((1, points), f32),
            pltpu.VMEM((2, steps, SEGMENT_NUMBER * unit, half), bf16),
            pltpu.VMEM((2, steps, SEGMENT_NUMBER * unit, half), bf16),
            pltpu.VMEM((2, steps, unit, half), bf16),
            pltpu.VMEM((2, steps, unit, half), bf16),
            pltpu.VMEM((2, steps, unit, half), bf16),
            pltpu.VMEM((2, steps, unit, half), bf16),
            pltpu.VMEM((2, steps, SEGMENT_NUMBER * unit, span), bf16),
            pltpu.VMEM((2, steps, SEGMENT_NUMBER * unit, span), bf16),
            pltpu.VMEM((2, SEGMENT_NUMBER * unit, span), bf16),
            pltpu.VMEM((2, SEGMENT_NUMBER * unit, span), bf16),
            pltpu.VMEM((2, SEGMENT_NUMBER * unit, span), f32),
            pltpu.VMEM((2, modes, 128), f32),
            pltpu.VMEM((2, modes, 128), f32),
            pltpu.VMEM((3, 4, modes, 128), f32),
            pltpu.VMEM((modes, 128), f32),
            pltpu.VMEM((peers, modes, 128), f32),
            dma((steps,)), dma, dma,
            dma((2, steps)), dma((2, steps)), dma((2, steps)), dma((2, steps)),
            dma((2, steps)), dma((2, steps)),
            dma((2, steps + tail)), dma((2, steps + tail)),
            dma((2,)), dma((2,)), dma((2,)), dma((2,)),
            dma((peers,)), dma((peers,)),
        ],
        compiler_params=pltpu.CompilerParams(
            collective_id=0, has_side_effects=True, vmem_limit_bytes=44 * 1024 * 1024),
        name="window_transform",
    )(*(
        pltpu.with_memory_space_constraint(a, pltpu.HBM)
        for a in (snapshots.transpose(1, 0, 2), quad_weights.reshape(1, points), spectral_indices)
    ))
    spectra, gram = pl.pallas_call(
        flush_kernel,
        out_shape=(
            jax.ShapeDtypeStruct(spectra.shape, f32), jax.ShapeDtypeStruct(gram.shape, f32)),
        in_specs=[vmem, vmem],
        out_specs=(hbm, hbm),
        scratch_shapes=[dma((modes + 1,))],
        compiler_params=pltpu.CompilerParams(vmem_limit_bytes=1024 * 1024),
        name="flush",
    )(*(pltpu.with_memory_space_constraint(a, pltpu.VMEM) for a in (spectra, gram)))
    gram = gram.reshape(SEGMENT_NUMBER, SEGMENT_NUMBER, 2, modes)
    return spectra.transpose(0, 1, 3, 2, 4), gram.transpose(3, 0, 1, 2)


def solution(mesh):
    square = mesh.shape["ta"] == 4
    return jax.shard_map(
        kernel_on_device if square else plain_on_device,
        mesh=mesh,
        in_specs=(P("ta", None, ("px", "py")), P(("px", "py")), P()),
        out_specs=(P("ta", None, None, None, ("px", "py")), P("ta", None, None, None)),
        check_vma=False,
    )
```

```python
import functools
import math

import jax
import jax.numpy as jnp
from jax import lax
from jax.experimental import pallas as pl
from jax.experimental.pallas import tpu as pltpu
from jax.sharding import PartitionSpec as P

VARS = 5
BLK = 256
HOP = 128
SEGMENT_NUMBER = 2
RETAINED_MODES = 32

MESH = pl.DeviceIdType.MESH


def make_rotation_multipliers(spectral_indices, temporal_locations):
    segment_beginnings = jnp.arange(SEGMENT_NUMBER, dtype=jnp.int32) * HOP
    segment_shifts = temporal_locations[None, :] - segment_beginnings[:, None]
    inside = (segment_shifts >= 0) & (segment_shifts < BLK)
    window = 0.5 - 0.5 * jnp.cos(2.0 * math.pi * segment_shifts.astype(jnp.float32) / BLK)
    window = jnp.where(inside, window, jnp.float32(0.0)) / jnp.sqrt(jnp.float32(3.0 * BLK / 8.0))
    phases = jnp.mod(spectral_indices[:, None, None] * segment_shifts[None, :, :], BLK)
    angles = 2.0 * math.pi * phases.astype(jnp.float32) / BLK
    real_part = jnp.cos(angles) * window[None]
    imag_part = -jnp.sin(angles) * window[None]
    gathered_segments = jnp.stack([real_part, imag_part], axis=2)
    return gathered_segments.reshape(
        RETAINED_MODES * SEGMENT_NUMBER * 2, temporal_locations.shape[0]
    ).astype(jnp.bfloat16)


def gram_terms(spectra):
    flat = spectra.reshape(spectra.shape[0], 2 * SEGMENT_NUMBER, -1)
    inner = jnp.einsum("fam,fbm->fab", flat, flat, precision=lax.Precision.HIGHEST)
    inner = inner.reshape(spectra.shape[0], SEGMENT_NUMBER, 2, SEGMENT_NUMBER, 2)
    real_part = inner[:, :, 0, :, 0] + inner[:, :, 1, :, 1]
    imag_part = inner[:, :, 0, :, 1] - inner[:, :, 1, :, 0]
    return jnp.stack([real_part, imag_part], axis=-1)


def plain_on_device(snapshots, quad_weights, spectral_indices):
    record_length = snapshots.shape[0]
    point_count = snapshots.shape[2]
    groups = lax.axis_size("ta")
    temporal_locations = lax.axis_index("ta") * record_length + jnp.arange(
        record_length, dtype=jnp.int32
    )
    rotation_multipliers = make_rotation_multipliers(spectral_indices, temporal_locations)
    flat_snapshots = snapshots.reshape(record_length, VARS * point_count)
    raw = lax.psum_scatter(
        jnp.dot(rotation_multipliers, flat_snapshots, preferred_element_type=jnp.float32),
        "ta",
        scatter_dimension=0,
        tiled=True,
    )
    raw = raw.reshape(RETAINED_MODES // groups, SEGMENT_NUMBER, 2, VARS, point_count)
    spectra = raw * jnp.sqrt(quad_weights)
    summed = lax.psum(gram_terms(spectra), ("px", "py"))
    total_points = point_count * lax.axis_size("px") * lax.axis_size("py")
    gram = summed / jnp.float32(total_points * VARS)
    return (spectra, gram)


def sine_of_turn(m):
    quarter = BLK // 4
    r = jnp.bitwise_and(m + quarter, BLK - 1) - quarter
    r = jnp.where(r > quarter, BLK // 2 - r, r)
    x = r.astype(jnp.float32) * (2.0 * math.pi / BLK)
    y = x * x
    total = jnp.full_like(x, -1.0 / math.factorial(11))
    for n in (9, 7, 5, 3, 1):
        total = total * y + (1.0 if n % 4 == 1 else -1.0) / math.factorial(n)
    return total * x


def window_kernel(
    pieces, tail, tile, gram_scale,
    snap_hbm, weight_hbm, index_hbm, out_ref, gram_ref,
    snap, index_ref, weight_ref, twiddle, own, root,
    a_send, a_recv, n1_send, n1_recv, n2_send, n2_recv, m1_send, m1_recv,
    p_send, p_recv, pre, e_send, e_recv, acc, gram_send, gram_recv,
    load_sem, index_sem, weight_sem,
    a_ssem, a_rsem, n1_ssem, n1_rsem, n2_ssem, n2_rsem, m1_ssem, m1_rsem,
    p_ssem, p_rsem, e_ssem, e_rsem, gram_ssem, gram_rsem, ready_sem,
):
    px, py, ta = lax.axis_index("px"), lax.axis_index("py"), lax.axis_index("ta")
    npx, npy = lax.axis_size("px"), lax.axis_size("py")
    variables, record, points = snap_hbm.shape
    modes = out_ref.shape[0]
    unit = 2 * modes
    steps = variables * pieces
    span = points // pieces
    half = span // 2
    short = span // tail
    common = steps - 2
    f32, bf16 = jnp.float32, jnp.bfloat16

    inner = (ta == 1) | (ta == 2)
    outer = jnp.logical_not(inner)
    me = jnp.where(inner, ta - 1, ta // 3)
    sides = (jnp.where(inner, 0, 1), jnp.where(inner, 3, 2))

    def load(k):
        there = pl.ds(pl.multiple_of(lax.rem(k, pieces) * span, span), span)
        return pltpu.make_async_copy(
            snap_hbm.at[k // pieces, :, there], snap.at[k // pieces, :, there], load_sem.at[k])

    index_copy = pltpu.make_async_copy(index_hbm, index_ref, index_sem)
    weight_copy = pltpu.make_async_copy(weight_hbm, weight_ref, weight_sem)
    index_copy.start()
    load(0).start()

    peers = [
        (i, j, lax.rem(px + i, npx), lax.rem(py + j, npy))
        for i in range(npx) for j in range(npy) if i + j > 0
    ]
    barrier = pltpu.get_barrier_semaphore()
    for side in sides:
        pl.semaphore_signal(barrier, inc=1, device_id=(px, py, side), device_id_type=MESH)
    for i in range(1, npx):
        pl.semaphore_signal(barrier, inc=1, device_id=(lax.rem(px + i, npx), py, ta), device_id_type=MESH)
    below, above = py > 0, py < npy - 1
    for there, step in ((below, -1), (above, 1)):
        @pl.when(there)
        def _():
            pl.semaphore_signal(barrier, inc=1, device_id=(px, py + step, ta), device_id_type=MESH)
    greeted = len(sides) + npx - 1 + jnp.where(below, 1, 0) + jnp.where(above, 1, 0)

    sublane = lax.broadcasted_iota(jnp.int32, (modes, record), 0)
    moment = lax.broadcasted_iota(jnp.int32, (modes, record), 1) + ta * record
    shifts, windows = [], []
    for block in range(SEGMENT_NUMBER):
        shift = moment - block * HOP
        inside = (shift >= 0) & (shift < BLK)
        hann = 0.5 - 0.5 * sine_of_turn(shift + BLK // 4)
        shifts.append(shift)
        windows.append(jnp.where(inside, hann, 0.0) / math.sqrt(3.0 * BLK / 8.0))
    index_copy.wait()
    for place, owner in enumerate((3 - ta, sides[0], sides[1], ta)):
        bins = jnp.zeros((modes, record), jnp.int32)
        for f in range(modes):
            bins = jnp.where(sublane == f, index_ref[owner * modes + f], bins)
        for block in range(SEGMENT_NUMBER):
            shift, hann = shifts[block], windows[block]
            phase = bins * shift
            rows = jnp.concatenate(
                [sine_of_turn(phase + BLK // 4) * hann, -sine_of_turn(phase) * hann], axis=0)
            if place < 3:
                at = jnp.where(inner, place * SEGMENT_NUMBER + block, block * 3 + place)
                twiddle[pl.ds(pl.multiple_of(at * unit, unit), unit), :] = rows.astype(bf16)
            else:
                own[block * unit:(block + 1) * unit, :] = rows.astype(bf16)
    acc[...] = jnp.zeros_like(acc)

    def remote(send, recv, ssem, rsem, side, *at):
        return pltpu.make_async_remote_copy(
            src_ref=send.at[(side, *at)], dst_ref=recv.at[(me, *at)],
            send_sem=ssem.at[side, at[0]], recv_sem=rsem.at[me, at[0]],
            device_id=(px, py, sides[side]), device_id_type=MESH,
        )

    def landed(send, recv, ssem, rsem, side, *at):
        return pltpu.make_async_remote_copy(
            src_ref=send.at[(side, *at)], dst_ref=recv.at[(side, *at)],
            send_sem=ssem.at[side, at[0]], recv_sem=rsem.at[side, at[0]],
            device_id=(px, py, sides[side]), device_id_type=MESH,
        )

    a_refs = (a_send, a_recv, a_ssem, a_rsem)
    n1_refs = (n1_send, n1_recv, n1_ssem, n1_rsem)
    n2_refs = (n2_send, n2_recv, n2_ssem, n2_rsem)

    def m1_copy(here, side, k, n=None):
        send, recv, ssem, rsem = m1_send.at[side, k], m1_recv.at[here, k], m1_ssem, m1_rsem
        if n is None:
            n = k
        else:
            columns = pl.ds(pl.multiple_of(n * short, short), short)
            send, recv, n = send.at[:, columns], recv.at[:, columns], steps + n
        return pltpu.make_async_remote_copy(
            src_ref=send, dst_ref=recv, send_sem=ssem.at[side, n], recv_sem=rsem.at[here, n],
            device_id=(px, py, sides[side]), device_id_type=MESH,
        )

    def lone_copy(send, recv, ssem, rsem, here, side):
        return pltpu.make_async_remote_copy(
            src_ref=send.at[side], dst_ref=recv.at[here],
            send_sem=ssem.at[side], recv_sem=rsem.at[here],
            device_id=(px, py, sides[side]), device_id_type=MESH,
        )

    p_refs = (p_send, p_recv, p_ssem, p_rsem)
    e_refs = (e_send, e_recv, e_ssem, e_rsem)

    def columns(k, at):
        return pl.ds(pl.multiple_of(lax.rem(k, pieces) * span + at, 128), tile)

    def transform(rows, k, at):
        return jnp.dot(rows, snap[k // pieces, :, columns(k, at)], preferred_element_type=f32)

    def loaded(k):
        load(k).wait()

        @pl.when(k == 0)
        def _():
            for later in range(1, steps):
                load(later).start()
            weight_copy.start()

    def tiles(width, unroll=1):
        def run(body):
            @pl.loop(0, width // tile, unroll=unroll)
            def _(i):
                body(pl.multiple_of(i * tile, tile))
        return run

    def meet(k):
        @pl.when(k == 0)
        def _():
            pl.semaphore_wait(barrier, greeted)

    def learn_of_peers():
        for n, (back, forth, step) in enumerate(((below, above, 1), (above, below, -1))):
            @pl.when(back)
            def _():
                pl.semaphore_wait(ready_sem.at[n], 1)

            @pl.when(forth)
            def _():
                pl.semaphore_signal(
                    ready_sem.at[n], inc=1, device_id=(px, py + step, ta), device_id_type=MESH)

        for i in range(1, npx):
            pl.semaphore_signal(
                ready_sem.at[2], inc=1, device_id=(lax.rem(px + i, npx), py, ta), device_id_type=MESH)
        if npx > 1:
            pl.semaphore_wait(ready_sem.at[2], npx - 1)

    def weighted(k, at, both):
        weight = root[:, columns(k, at)]
        return [
            (both[b * unit:b * unit + modes] * weight, both[b * unit + modes:(b + 1) * unit] * weight)
            for b in range(SEGMENT_NUMBER)]

    def add_terms(place, parts):
        (r0, i0), (r1, i1) = parts
        terms = (r0 * r0 + i0 * i0, r1 * r1 + i1 * i1, r0 * r1 + i0 * i1, r0 * i1 - i0 * r1)
        for n, term in enumerate(terms):
            lanes = [term[:, c:c + 128] for c in range(0, tile, 128)]
            acc[place, n] += functools.reduce(jnp.add, lanes)

    def store(k, at, parts):
        here = columns(k, at)
        for block, pair in enumerate(parts):
            for c in range(2):
                out_ref[:, block, k // pieces, c, here] = pair[c]

    def sums_of(place):
        lane = lax.broadcasted_iota(jnp.int32, gram_send.shape, 1)
        sums = jnp.zeros(gram_send.shape, f32)
        for n in range(4):
            sums = jnp.where(lane == n, jnp.sum(acc[place, n], axis=1, keepdims=True), sums)
        return sums

    def gram_copy(n):
        i, j, x, y = peers[n]
        return pltpu.make_async_remote_copy(
            src_ref=gram_send, dst_ref=gram_recv.at[n],
            send_sem=gram_ssem.at[n], recv_sem=gram_rsem.at[n],
            device_id=(x, y, ta), device_id_type=MESH,
        )

    def exchange(sums):
        gram_send[...] = sums
        for n in range(len(peers)):
            gram_copy(n).start()

    def weights():
        weight_copy.wait()
        root[...] = jnp.sqrt(weight_ref[...])

    def gather():
        total = gram_send[...]
        for n in range(len(peers)):
            gram_copy(n).wait()
            total = total + gram_recv[n]
        row = lax.broadcasted_iota(jnp.int32, (8, 128), 0)
        lane = lax.broadcasted_iota(jnp.int32, (8, 128), 1)
        pick = jnp.zeros((8, 128), f32)
        for r, n, sign in ((0, 0, 1.0), (2, 2, 1.0), (3, 3, 1.0), (4, 2, 1.0), (5, 3, -1.0), (6, 1, 1.0)):
            pick = jnp.where((row == r) & (lane == n), sign, pick)
        gram_ref[...] = gram_scale * lax.dot_general(
            pick, total, (((1,), (1,)), ((), ())),
            precision=lax.Precision.HIGHEST, preferred_element_type=f32,
        )

    @pl.when(inner)
    def _():
        @pl.loop(0, steps)
        def _(k):
            loaded(k)
            for side in range(2):
                @tiles(half, 4)
                def _(at):
                    a_send[side, k, :, pl.ds(at, tile)] = transform(
                        twiddle[0:2 * unit, :], k, side * half + at).astype(bf16)
                if side == 0:
                    meet(k)
                remote(*a_refs, side, k).start()

        @pl.loop(0, steps)
        def _(j):
            last = j == steps - 1
            k = jnp.where(j == 0, steps - 1 - me, jnp.where(last, common + me, j - 1))
            for dependent in range(2):
                first = half * (me if dependent else 1 - me)
                if dependent:
                    for side in range(2):
                        landed(*n2_refs, side, k).wait_recv()

                @tiles(half)
                def _(at):
                    product = transform(twiddle[2 * unit:6 * unit, :], k, first + at)
                    there = pl.ds(pl.multiple_of(first + at, 128), tile)
                    for side in range(2):
                        for block in range(SEGMENT_NUMBER):
                            r = (side * SEGMENT_NUMBER + block) * unit
                            rows = product[r:r + unit]
                            if dependent and block != side:
                                rows = rows + n2_recv[block, k, :, pl.ds(at, tile)].astype(f32)
                            m1_send[side, k, block * unit:(block + 1) * unit, there] = rows.astype(bf16)

            @pl.when(jnp.logical_not(last))
            def _():
                for side in range(2):
                    m1_copy(me, side, k).start()

        weights()
        learn_of_peers()

        @pl.loop(0, steps)
        def _(k):
            for side in range(2):
                landed(*a_refs, side, k).wait_recv()
                landed(*n1_refs, side, k).wait_recv()

            for side in range(2):
                @tiles(half)
                def _(at):
                    both = transform(own[...], k, side * half + at)
                    both = both + a_recv[side, k, :, pl.ds(at, tile)].astype(f32)
                    extra = n1_recv[1 - side, k, :, pl.ds(at, tile)].astype(f32)
                    rows = [both[:unit], both[unit:]]
                    rows[1 - side] = rows[1 - side] + extra
                    parts = weighted(k, side * half + at, jnp.concatenate(rows, axis=0))
                    add_terms(0, parts)
                    store(k, side * half + at, parts)

        exchange(sums_of(0))
        for side in range(2):
            lone_copy(*p_refs, side, side).wait_recv()

            @tiles(span)
            def _(at):
                there = pl.ds(at, tile)
                k = common + me
                both = p_recv[side, :, there].astype(f32) + m1_send[side, k, :, there].astype(f32)
                add_terms(1 + side, weighted(k, at, both))

            e_send[side] = sums_of(1 + side)
            lone_copy(*e_refs, me, side).start()

        for n in range(tail):
            for side in range(2):
                m1_copy(me, side, common + me, n).start()

        gather()
        for side in range(2):
            lone_copy(*e_refs, me, side).wait_send()

        @pl.loop(0, steps)
        def _(k):
            for side in range(2):
                remote(*a_refs, side, k).wait_send()

                @pl.when(k != common + me)
                def _():
                    m1_copy(me, side, k).wait_send()

        @pl.loop(0, tail)
        def _(n):
            for side in range(2):
                m1_copy(me, side, common + me, n).wait_send()

    @pl.when(outer)
    def _():
        base = me * (3 * unit)
        far = pl.ds(pl.multiple_of(base, unit), unit)
        near = pl.ds(pl.multiple_of(base + unit, unit), 2 * unit)

        @pl.loop(0, steps)
        def _(k):
            loaded(k)
            for side in range(2):
                @tiles(half, 4)
                def _(at):
                    n2_send[side, k, :, pl.ds(at, tile)] = transform(
                        twiddle[far, :], k, side * half + at).astype(bf16)
                if side == 0:
                    meet(k)
                remote(*n2_refs, side, k).start()

        @pl.loop(0, steps)
        def _(k):
            @tiles(half)
            def _(at):
                product = transform(twiddle[near, :], k, (1 - me) * half + at)
                for side in range(2):
                    n1_send[side, k, :, pl.ds(at, tile)] = product[side * unit:(side + 1) * unit].astype(bf16)
            for side in range(2):
                remote(*n1_refs, side, k).start()
            for side in range(2):
                landed(*a_refs, side, k).wait_recv()

            @tiles(half)
            def _(at):
                here = pl.ds(at, tile)
                product = transform(twiddle[near, :], k, me * half + at)
                for side in range(2):
                    rows = product[side * unit:(side + 1) * unit]
                    for block in range(SEGMENT_NUMBER):
                        there = slice(block * unit, (block + 1) * unit)
                        came = a_recv[1 - side, k, there, here].astype(f32)
                        total = came + jnp.where(me == block, rows, 0.0)
                        a_send[side, k, there, here] = total.astype(bf16)
            for side in range(2):
                remote(*a_refs, side, k).start()

        weights()

        for side in range(2):
            k = common + side
            m1_copy(1 - side, 1 - side, k).wait_recv()

            @tiles(span)
            def _(at):
                there = pl.ds(at, tile)
                both = transform(own[...], k, at) + m1_recv[1 - side, k, :, there].astype(f32)
                p_send[side, :, there] = both.astype(bf16)
                pre[side, :, there] = both

            lone_copy(*p_refs, me, side).start()

        learn_of_peers()

        def arrived(k, at):
            there = pl.ds(at, tile)
            both = transform(own[...], k, at)
            return weighted(k, at, both + (
                m1_recv[0, k, :, there].astype(f32) + m1_recv[1, k, :, there].astype(f32)))

        @pl.loop(0, common)
        def _(k):
            for side in range(2):
                m1_copy(side, side, k).wait_recv()

            @tiles(span, 2)
            def _(at):
                parts = arrived(k, at)
                add_terms(0, parts)
                store(k, at, parts)

        sums = sums_of(0)
        for side in range(2):
            lone_copy(*e_refs, side, side).wait_recv()
            sums = sums + e_recv[side]
        exchange(sums)

        @pl.loop(0, steps)
        def _(k):
            for side in range(2):
                for refs in (a_refs, n1_refs, n2_refs):
                    remote(*refs, side, k).wait_send()

        for side in range(2):
            lone_copy(*p_refs, me, side).wait_send()

        @pl.loop(0, tail)
        def _(n):
            @pl.when(n == tail - 1)
            def _():
                gather()

            for side in range(2):
                k = common + side
                m1_copy(side, side, k, n).wait_recv()

                for c in range(0, short, tile):
                    at = pl.multiple_of(n * short + c, tile)
                    there = pl.ds(at, tile)
                    store(k, at, weighted(
                        k, at, pre[side, :, there] + m1_recv[side, k, :, there].astype(f32)))


def flush_kernel(spectra, gram, spectra_out, gram_out, sems):
    copies = [pltpu.make_async_copy(gram, gram_out, sems.at[0])]
    for f in range(spectra.shape[0]):
        copies.append(pltpu.make_async_copy(spectra.at[f], spectra_out.at[f], sems.at[f + 1]))
    for copy in copies:
        copy.start()
    for copy in copies:
        copy.wait()


def kernel_on_device(snapshots, quad_weights, spectral_indices):
    record, variables, points = snapshots.shape
    groups = lax.axis_size("ta")
    npx, npy = lax.axis_size("px"), lax.axis_size("py")
    modes = spectral_indices.shape[0] // groups
    unit = 2 * modes
    pieces, tail = 2, 4
    span = points // pieces
    half = span // 2
    tile = math.gcd(512, span // tail)
    steps = variables * pieces
    bf16, f32 = jnp.bfloat16, jnp.float32
    peers = npx * npy - 1
    dma = pltpu.SemaphoreType.DMA
    hbm = pl.BlockSpec(memory_space=pltpu.HBM)
    vmem = pl.BlockSpec(memory_space=pltpu.VMEM)
    spectra, gram = pl.pallas_call(
        functools.partial(
            window_kernel, pieces, tail, tile, 1.0 / (points * npx * npy * variables)),
        out_shape=(
            jax.ShapeDtypeStruct((modes, SEGMENT_NUMBER, variables, 2, points), f32),
            jax.ShapeDtypeStruct((SEGMENT_NUMBER * SEGMENT_NUMBER * 2, modes), f32),
        ),
        in_specs=[hbm, hbm, hbm],
        out_specs=(vmem, vmem),
        scratch_shapes=[
            pltpu.VMEM((variables, record, points), bf16),
            pltpu.SMEM(spectral_indices.shape, jnp.int32),
            pltpu.VMEM((1, points), f32),
            pltpu.VMEM((3 * SEGMENT_NUMBER * unit, record), bf16),
            pltpu.VMEM((SEGMENT_NUMBER * unit, record), bf16),
            pltpu.VMEM((1, points), f32),
            pltpu.VMEM((2, steps, SEGMENT_NUMBER * unit, half), bf16),
            pltpu.VMEM((2, steps, SEGMENT_NUMBER * unit, half), bf16),
            pltpu.VMEM((2, steps, unit, half), bf16),
            pltpu.VMEM((2, steps, unit, half), bf16),
            pltpu.VMEM((2, steps, unit, half), bf16),
            pltpu.VMEM((2, steps, unit, half), bf16),
            pltpu.VMEM((2, steps, SEGMENT_NUMBER * unit, span), bf16),
            pltpu.VMEM((2, steps, SEGMENT_NUMBER * unit, span), bf16),
            pltpu.VMEM((2, SEGMENT_NUMBER * unit, span), bf16),
            pltpu.VMEM((2, SEGMENT_NUMBER * unit, span), bf16),
            pltpu.VMEM((2, SEGMENT_NUMBER * unit, span), f32),
            pltpu.VMEM((2, modes, 128), f32),
            pltpu.VMEM((2, modes, 128), f32),
            pltpu.VMEM((3, 4, modes, 128), f32),
            pltpu.VMEM((modes, 128), f32),
            pltpu.VMEM((peers, modes, 128), f32),
            dma((steps,)), dma, dma,
            dma((2, steps)), dma((2, steps)), dma((2, steps)), dma((2, steps)),
            dma((2, steps)), dma((2, steps)),
            dma((2, steps + tail)), dma((2, steps + tail)),
            dma((2,)), dma((2,)), dma((2,)), dma((2,)),
            dma((peers,)), dma((peers,)),
            pltpu.SemaphoreType.REGULAR((3,)),
        ],
        compiler_params=pltpu.CompilerParams(
            collective_id=0, has_side_effects=True, vmem_limit_bytes=44 * 1024 * 1024),
        name="window_transform",
    )(*(
        pltpu.with_memory_space_constraint(a, pltpu.HBM)
        for a in (snapshots.transpose(1, 0, 2), quad_weights.reshape(1, points), spectral_indices)
    ))
    spectra, gram = pl.pallas_call(
        flush_kernel,
        out_shape=(
            jax.ShapeDtypeStruct(spectra.shape, f32), jax.ShapeDtypeStruct(gram.shape, f32)),
        in_specs=[vmem, vmem],
        out_specs=(hbm, hbm),
        scratch_shapes=[dma((modes + 1,))],
        compiler_params=pltpu.CompilerParams(vmem_limit_bytes=1024 * 1024),
        name="flush",
    )(*(pltpu.with_memory_space_constraint(a, pltpu.VMEM) for a in (spectra, gram)))
    gram = gram.reshape(SEGMENT_NUMBER, SEGMENT_NUMBER, 2, modes)
    return spectra.transpose(0, 1, 3, 2, 4), gram.transpose(3, 0, 1, 2)


def solution(mesh):
    square = mesh.shape["ta"] == 4
    return jax.shard_map(
        kernel_on_device if square else plain_on_device,
        mesh=mesh,
        in_specs=(P("ta", None, ("px", "py")), P(("px", "py")), P()),
        out_specs=(P("ta", None, None, None, ("px", "py")), P("ta", None, None, None)),
        check_vma=False,
    )
```

```python
import functools
import math

import jax
import jax.numpy as jnp
from jax import lax
from jax.experimental import pallas as pl
from jax.experimental.pallas import tpu as pltpu
from jax.sharding import PartitionSpec as P

VARS = 5
BLK = 256
HOP = 128
SEGMENT_NUMBER = 2
RETAINED_MODES = 32

MESH = pl.DeviceIdType.MESH


def make_rotation_multipliers(spectral_indices, temporal_locations):
    segment_beginnings = jnp.arange(SEGMENT_NUMBER, dtype=jnp.int32) * HOP
    segment_shifts = temporal_locations[None, :] - segment_beginnings[:, None]
    inside = (segment_shifts >= 0) & (segment_shifts < BLK)
    window = 0.5 - 0.5 * jnp.cos(2.0 * math.pi * segment_shifts.astype(jnp.float32) / BLK)
    window = jnp.where(inside, window, jnp.float32(0.0)) / jnp.sqrt(jnp.float32(3.0 * BLK / 8.0))
    phases = jnp.mod(spectral_indices[:, None, None] * segment_shifts[None, :, :], BLK)
    angles = 2.0 * math.pi * phases.astype(jnp.float32) / BLK
    real_part = jnp.cos(angles) * window[None]
    imag_part = -jnp.sin(angles) * window[None]
    gathered_segments = jnp.stack([real_part, imag_part], axis=2)
    return gathered_segments.reshape(
        RETAINED_MODES * SEGMENT_NUMBER * 2, temporal_locations.shape[0]
    ).astype(jnp.bfloat16)


def gram_terms(spectra):
    flat = spectra.reshape(spectra.shape[0], 2 * SEGMENT_NUMBER, -1)
    inner = jnp.einsum("fam,fbm->fab", flat, flat, precision=lax.Precision.HIGHEST)
    inner = inner.reshape(spectra.shape[0], SEGMENT_NUMBER, 2, SEGMENT_NUMBER, 2)
    real_part = inner[:, :, 0, :, 0] + inner[:, :, 1, :, 1]
    imag_part = inner[:, :, 0, :, 1] - inner[:, :, 1, :, 0]
    return jnp.stack([real_part, imag_part], axis=-1)


def plain_on_device(snapshots, quad_weights, spectral_indices):
    record_length = snapshots.shape[0]
    point_count = snapshots.shape[2]
    groups = lax.axis_size("ta")
    temporal_locations = lax.axis_index("ta") * record_length + jnp.arange(
        record_length, dtype=jnp.int32
    )
    rotation_multipliers = make_rotation_multipliers(spectral_indices, temporal_locations)
    flat_snapshots = snapshots.reshape(record_length, VARS * point_count)
    raw = lax.psum_scatter(
        jnp.dot(rotation_multipliers, flat_snapshots, preferred_element_type=jnp.float32),
        "ta",
        scatter_dimension=0,
        tiled=True,
    )
    raw = raw.reshape(RETAINED_MODES // groups, SEGMENT_NUMBER, 2, VARS, point_count)
    spectra = raw * jnp.sqrt(quad_weights)
    summed = lax.psum(gram_terms(spectra), ("px", "py"))
    total_points = point_count * lax.axis_size("px") * lax.axis_size("py")
    gram = summed / jnp.float32(total_points * VARS)
    return (spectra, gram)


def sine_of_turn(m):
    quarter = BLK // 4
    r = jnp.bitwise_and(m + quarter, BLK - 1) - quarter
    r = jnp.where(r > quarter, BLK // 2 - r, r)
    x = r.astype(jnp.float32) * (2.0 * math.pi / BLK)
    y = x * x
    total = jnp.full_like(x, -1.0 / math.factorial(11))
    for n in (9, 7, 5, 3, 1):
        total = total * y + (1.0 if n % 4 == 1 else -1.0) / math.factorial(n)
    return total * x


def window_kernel(
    pieces, tail, tile, gram_scale,
    snap_hbm, weight_hbm, index_hbm, out_ref, gram_ref,
    snap, index_ref, weight_ref, twiddle, own, root,
    a_send, a_recv, n1_send, n1_recv, n2_send, n2_recv, m1_send, m1_recv,
    relay, p_send, p_recv, pre, e_send, e_recv, acc, gram_send, gram_recv,
    load_sem, index_sem, weight_sem,
    a_ssem, a_rsem, n1_ssem, n1_rsem, n2_ssem, n2_rsem, m1_ssem, m1_rsem,
    relay_ssem, relay_rsem, lift_ssem, lift_rsem,
    p_ssem, p_rsem, e_ssem, e_rsem, gram_ssem, gram_rsem, ready_sem,
):
    px, py, ta = lax.axis_index("px"), lax.axis_index("py"), lax.axis_index("ta")
    npx, npy = lax.axis_size("px"), lax.axis_size("py")
    variables, record, points = snap_hbm.shape
    modes = out_ref.shape[0]
    unit = 2 * modes
    steps = variables * pieces
    span = points // pieces
    half = span // 2
    short = span // tail
    common = steps - 4
    lifts, lift = relay.shape[0], relay.shape[3]
    f32, bf16 = jnp.float32, jnp.bfloat16

    inner = (ta == 1) | (ta == 2)
    outer = jnp.logical_not(inner)
    me = jnp.where(inner, ta - 1, ta // 3)
    sides = (jnp.where(inner, 0, 1), jnp.where(inner, 3, 2))

    def load(k):
        there = pl.ds(pl.multiple_of(lax.rem(k, pieces) * span, span), span)
        return pltpu.make_async_copy(
            snap_hbm.at[k // pieces, :, there], snap.at[k // pieces, :, there], load_sem.at[k])

    index_copy = pltpu.make_async_copy(index_hbm, index_ref, index_sem)
    weight_copy = pltpu.make_async_copy(weight_hbm, weight_ref, weight_sem)
    index_copy.start()
    load(0).start()

    peers = [
        (i, j, lax.rem(px + i, npx), lax.rem(py + j, npy))
        for i in range(npx) for j in range(npy) if i + j > 0
    ]
    barrier = pltpu.get_barrier_semaphore()
    for side in sides:
        pl.semaphore_signal(barrier, inc=1, device_id=(px, py, side), device_id_type=MESH)
    for i in range(1, npx):
        pl.semaphore_signal(barrier, inc=1, device_id=(lax.rem(px + i, npx), py, ta), device_id_type=MESH)
    below, above = py > 0, py < npy - 1
    for there, step in ((below, -1), (above, 1)):
        @pl.when(there)
        def _():
            pl.semaphore_signal(barrier, inc=1, device_id=(px, py + step, ta), device_id_type=MESH)
    greeted = len(sides) + npx - 1 + jnp.where(below, 1, 0) + jnp.where(above, 1, 0)

    sublane = lax.broadcasted_iota(jnp.int32, (modes, record), 0)
    moment = lax.broadcasted_iota(jnp.int32, (modes, record), 1) + ta * record
    shifts, windows = [], []
    for block in range(SEGMENT_NUMBER):
        shift = moment - block * HOP
        inside = (shift >= 0) & (shift < BLK)
        hann = 0.5 - 0.5 * sine_of_turn(shift + BLK // 4)
        shifts.append(shift)
        windows.append(jnp.where(inside, hann, 0.0) / math.sqrt(3.0 * BLK / 8.0))
    index_copy.wait()
    for place, owner in enumerate((3 - ta, sides[0], sides[1], ta)):
        bins = jnp.zeros((modes, record), jnp.int32)
        for f in range(modes):
            bins = jnp.where(sublane == f, index_ref[owner * modes + f], bins)
        for block in range(SEGMENT_NUMBER):
            shift, hann = shifts[block], windows[block]
            phase = bins * shift
            rows = jnp.concatenate(
                [sine_of_turn(phase + BLK // 4) * hann, -sine_of_turn(phase) * hann], axis=0)
            if place < 3:
                at = jnp.where(inner, place * SEGMENT_NUMBER + block, block * 3 + place)
                twiddle[pl.ds(pl.multiple_of(at * unit, unit), unit), :] = rows.astype(bf16)
            else:
                own[block * unit:(block + 1) * unit, :] = rows.astype(bf16)
    acc[...] = jnp.zeros_like(acc)

    def remote(send, recv, ssem, rsem, side, *at):
        return pltpu.make_async_remote_copy(
            src_ref=send.at[(side, *at)], dst_ref=recv.at[(me, *at)],
            send_sem=ssem.at[side, at[0]], recv_sem=rsem.at[me, at[0]],
            device_id=(px, py, sides[side]), device_id_type=MESH,
        )

    def landed(send, recv, ssem, rsem, side, *at):
        return pltpu.make_async_remote_copy(
            src_ref=send.at[(side, *at)], dst_ref=recv.at[(side, *at)],
            send_sem=ssem.at[side, at[0]], recv_sem=rsem.at[side, at[0]],
            device_id=(px, py, sides[side]), device_id_type=MESH,
        )

    a_refs = (a_send, a_recv, a_ssem, a_rsem)
    n1_refs = (n1_send, n1_recv, n1_ssem, n1_rsem)
    n2_refs = (n2_send, n2_recv, n2_ssem, n2_rsem)

    def m1_copy(here, side, k, n=None):
        send, recv, ssem, rsem = m1_send.at[side, k], m1_recv.at[here, k], m1_ssem, m1_rsem
        if n is None:
            n = k
        else:
            columns = pl.ds(pl.multiple_of(n * short, short), short)
            send, recv = send.at[:, columns], recv.at[:, columns]
            n = steps + n + jnp.where(k == common - 1, tail, 0)
        return pltpu.make_async_remote_copy(
            src_ref=send, dst_ref=recv, send_sem=ssem.at[side, n], recv_sem=rsem.at[here, n],
            device_id=(px, py, sides[side]), device_id_type=MESH,
        )

    def lifted_copy(here, side, c):
        columns = pl.ds(c * lift, lift)
        return pltpu.make_async_remote_copy(
            src_ref=m1_send.at[side, 0, :, columns], dst_ref=m1_recv.at[here, 0, :, columns],
            send_sem=lift_ssem.at[c, side], recv_sem=lift_rsem.at[c, here],
            device_id=(px, py, sides[side]), device_id_type=MESH,
        )

    def up_copy(here, side, c):
        return pltpu.make_async_remote_copy(
            src_ref=m1_send.at[side, 0, :, pl.ds(c * lift, lift)], dst_ref=relay.at[c, here],
            send_sem=lift_ssem.at[c, side], recv_sem=relay_rsem.at[c, here],
            device_id=(px, py + 1, sides[side]), device_id_type=MESH,
        )

    def down_copy(side, c):
        return pltpu.make_async_remote_copy(
            src_ref=relay.at[c, side], dst_ref=m1_recv.at[side, 0, :, pl.ds(c * lift, lift)],
            send_sem=relay_ssem.at[c, side], recv_sem=lift_rsem.at[c, side],
            device_id=(px, py - 1, ta), device_id_type=MESH,
        )

    def goes_up(c):
        return c < npy - 1 - py

    def comes_up(c):
        return (py > 0) & (c < npy - py)

    def rest_copy(here, side):
        columns = pl.ds(lifts * lift, span - lifts * lift)
        return pltpu.make_async_remote_copy(
            src_ref=m1_send.at[side, 0, :, columns], dst_ref=m1_recv.at[here, 0, :, columns],
            send_sem=m1_ssem.at[side, 0], recv_sem=m1_rsem.at[here, 0],
            device_id=(px, py, sides[side]), device_id_type=MESH,
        )

    def p_copy(here, side, u):
        return pltpu.make_async_remote_copy(
            src_ref=p_send.at[side, u], dst_ref=p_recv.at[here, u],
            send_sem=p_ssem.at[side, u], recv_sem=p_rsem.at[here, u],
            device_id=(px, py, sides[side]), device_id_type=MESH,
        )

    beside = jnp.bitwise_xor(py, 1) if npy % 2 == 0 else py

    def e_copy(here, side):
        return pltpu.make_async_remote_copy(
            src_ref=e_send.at[side], dst_ref=e_recv.at[here],
            send_sem=e_ssem.at[side], recv_sem=e_rsem.at[here],
            device_id=(px, beside, sides[side]), device_id_type=MESH,
        )

    def columns(k, at):
        return pl.ds(pl.multiple_of(lax.rem(k, pieces) * span + at, 128), tile)

    def transform(rows, k, at):
        return jnp.dot(rows, snap[k // pieces, :, columns(k, at)], preferred_element_type=f32)

    def loaded(k):
        load(k).wait()

        @pl.when(k == 0)
        def _():
            for later in range(1, steps):
                load(later).start()
            weight_copy.start()

    def tiles(width, unroll=1):
        def run(body):
            @pl.loop(0, width // tile, unroll=unroll)
            def _(i):
                body(pl.multiple_of(i * tile, tile))
        return run

    def meet(k):
        @pl.when(k == 0)
        def _():
            pl.semaphore_wait(barrier, greeted)

    def learn_of_peers():
        for n, (back, forth, step) in enumerate(((below, above, 1), (above, below, -1))):
            @pl.when(back)
            def _():
                pl.semaphore_wait(ready_sem.at[n], 1)

            @pl.when(forth)
            def _():
                pl.semaphore_signal(
                    ready_sem.at[n], inc=1, device_id=(px, py + step, ta), device_id_type=MESH)

        for i in range(1, npx):
            pl.semaphore_signal(
                ready_sem.at[2], inc=1, device_id=(lax.rem(px + i, npx), py, ta), device_id_type=MESH)
        if npx > 1:
            pl.semaphore_wait(ready_sem.at[2], npx - 1)

    def weighted(k, at, both):
        weight = root[:, columns(k, at)]
        return [
            (both[b * unit:b * unit + modes] * weight, both[b * unit + modes:(b + 1) * unit] * weight)
            for b in range(SEGMENT_NUMBER)]

    def add_terms(place, parts):
        (r0, i0), (r1, i1) = parts
        terms = (r0 * r0 + i0 * i0, r1 * r1 + i1 * i1, r0 * r1 + i0 * i1, r0 * i1 - i0 * r1)
        for n, term in enumerate(terms):
            lanes = [term[:, c:c + 128] for c in range(0, tile, 128)]
            acc[place, n] += functools.reduce(jnp.add, lanes)

    def store(k, at, parts):
        here = columns(k, at)
        for block, pair in enumerate(parts):
            for c in range(2):
                out_ref[:, block, k // pieces, c, here] = pair[c]

    def sums_of(place):
        lane = lax.broadcasted_iota(jnp.int32, gram_send.shape, 1)
        sums = jnp.zeros(gram_send.shape, f32)
        for n in range(4):
            sums = jnp.where(lane == n, jnp.sum(acc[place, n], axis=1, keepdims=True), sums)
        return sums

    def gram_copy(n):
        i, j, x, y = peers[n]
        return pltpu.make_async_remote_copy(
            src_ref=gram_send, dst_ref=gram_recv.at[n],
            send_sem=gram_ssem.at[n], recv_sem=gram_rsem.at[n],
            device_id=(x, y, ta), device_id_type=MESH,
        )

    def exchange(sums):
        gram_send[...] = sums
        for n in range(len(peers)):
            gram_copy(n).start()

    def weights():
        weight_copy.wait()
        root[...] = jnp.sqrt(weight_ref[...])

    def gather():
        total = gram_send[...]
        for n in range(len(peers)):
            gram_copy(n).wait()
            total = total + gram_recv[n]
        row = lax.broadcasted_iota(jnp.int32, (8, 128), 0)
        lane = lax.broadcasted_iota(jnp.int32, (8, 128), 1)
        pick = jnp.zeros((8, 128), f32)
        for r, n, sign in ((0, 0, 1.0), (2, 2, 1.0), (3, 3, 1.0), (4, 2, 1.0), (5, 3, -1.0), (6, 1, 1.0)):
            pick = jnp.where((row == r) & (lane == n), sign, pick)
        gram_ref[...] = gram_scale * lax.dot_general(
            pick, total, (((1,), (1,)), ((), ())),
            precision=lax.Precision.HIGHEST, preferred_element_type=f32,
        )

    @pl.when(inner)
    def _():
        @pl.loop(0, steps)
        def _(k):
            loaded(k)
            for side in range(2):
                @tiles(half, 4)
                def _(at):
                    a_send[side, k, :, pl.ds(at, tile)] = transform(
                        twiddle[0:2 * unit, :], k, side * half + at).astype(bf16)
                if side == 0:
                    meet(k)
                remote(*a_refs, side, k).start()

        @pl.loop(0, steps)
        def _(j):
            k = jnp.where(
                j < 2, common + 2 * j + 1 - me,
                jnp.where(j < common + 2, j - 2, common + 2 * (j - common - 2) + me))
            for dependent in range(2):
                first = half * (me if dependent else 1 - me)
                if dependent:
                    for side in range(2):
                        landed(*n2_refs, side, k).wait_recv()

                @tiles(half)
                def _(at):
                    product = transform(twiddle[2 * unit:6 * unit, :], k, first + at)
                    there = pl.ds(pl.multiple_of(first + at, 128), tile)
                    for side in range(2):
                        for block in range(SEGMENT_NUMBER):
                            r = (side * SEGMENT_NUMBER + block) * unit
                            rows = product[r:r + unit]
                            if dependent and block != side:
                                rows = rows + n2_recv[block, k, :, pl.ds(at, tile)].astype(f32)
                            m1_send[side, k, block * unit:(block + 1) * unit, there] = rows.astype(bf16)

            split = (k == common - 1) | (j == steps - 1)

            @pl.when(split)
            def _():
                for n in range(tail):
                    for side in range(2):
                        m1_copy(me, side, k, n).start()

            @pl.when(k == 0)
            def _():
                for c in range(lifts):
                    for side in range(2):
                        @pl.when(goes_up(c))
                        def _():
                            up_copy(me, side, c).start()

                        @pl.when(jnp.logical_not(goes_up(c)))
                        def _():
                            lifted_copy(me, side, c).start()
                for side in range(2):
                    rest_copy(me, side).start()

            @pl.when(jnp.logical_not(split) & (k != 0))
            def _():
                for side in range(2):
                    m1_copy(me, side, k).start()


        weights()
        learn_of_peers()

        @pl.loop(0, steps)
        def _(k):
            for side in range(2):
                landed(*a_refs, side, k).wait_recv()
                landed(*n1_refs, side, k).wait_recv()

            for side in range(2):
                @tiles(half)
                def _(at):
                    both = transform(own[...], k, side * half + at)
                    both = both + a_recv[side, k, :, pl.ds(at, tile)].astype(f32)
                    extra = n1_recv[1 - side, k, :, pl.ds(at, tile)].astype(f32)
                    rows = [both[:unit], both[unit:]]
                    rows[1 - side] = rows[1 - side] + extra
                    parts = weighted(k, side * half + at, jnp.concatenate(rows, axis=0))
                    add_terms(0, parts)
                    store(k, side * half + at, parts)

        exchange(sums_of(0))
        for u in range(2):
            for side in range(2):
                p_copy(side, side, u).wait_recv()

                @tiles(span, 2)
                def _(at):
                    there = pl.ds(at, tile)
                    k = common + 2 * u + me
                    both = p_recv[side, u, :, there].astype(f32) + m1_send[side, k, :, there].astype(f32)
                    add_terms(1 + side, weighted(k, at, both))

        for side in range(2):
            e_send[side] = sums_of(1 + side)
            e_copy(me, side).start()

        gather()
        for side in range(2):
            e_copy(me, side).wait_send()

        @pl.loop(0, steps)
        def _(k):
            for side in range(2):
                remote(*a_refs, side, k).wait_send()

                @pl.when((k != common + 2 + me) & (k != common - 1) & (k > 0))
                def _():
                    m1_copy(me, side, k).wait_send()

        for side in range(2):
            rest_copy(me, side).wait_send()
            for c in range(lifts):
                lifted_copy(me, side, c).wait_send()

        @pl.loop(0, tail)
        def _(n):
            for side in range(2):
                m1_copy(me, side, common - 1, n).wait_send()
                m1_copy(me, side, common + 2 + me, n).wait_send()

    @pl.when(outer)
    def _():
        base = me * (3 * unit)
        far = pl.ds(pl.multiple_of(base, unit), unit)
        near = pl.ds(pl.multiple_of(base + unit, unit), 2 * unit)

        @pl.loop(0, steps)
        def _(k):
            loaded(k)
            for side in range(2):
                @tiles(half, 4)
                def _(at):
                    n2_send[side, k, :, pl.ds(at, tile)] = transform(
                        twiddle[far, :], k, side * half + at).astype(bf16)
                if side == 0:
                    meet(k)
                remote(*n2_refs, side, k).start()

        @pl.loop(0, steps)
        def _(k):
            @tiles(half)
            def _(at):
                product = transform(twiddle[near, :], k, (1 - me) * half + at)
                for side in range(2):
                    n1_send[side, k, :, pl.ds(at, tile)] = product[side * unit:(side + 1) * unit].astype(bf16)
            for side in range(2):
                remote(*n1_refs, side, k).start()
            for side in range(2):
                landed(*a_refs, side, k).wait_recv()

            @tiles(half)
            def _(at):
                here = pl.ds(at, tile)
                product = transform(twiddle[near, :], k, me * half + at)
                for side in range(2):
                    rows = product[side * unit:(side + 1) * unit]
                    for block in range(SEGMENT_NUMBER):
                        there = slice(block * unit, (block + 1) * unit)
                        came = a_recv[1 - side, k, there, here].astype(f32)
                        total = came + jnp.where(me == block, rows, 0.0)
                        a_send[side, k, there, here] = total.astype(bf16)
            for side in range(2):
                remote(*a_refs, side, k).start()

        weights()

        for c in range(lifts):
            @pl.when(comes_up(c))
            def _():
                for side in range(2):
                    up_copy(side, side, c).wait_recv()
                    down_copy(side, c).start()

        for u in range(2):
            for side in range(2):
                k = common + 2 * u + side
                m1_copy(1 - side, 1 - side, k).wait_recv()

                @tiles(span, 2)
                def _(at):
                    there = pl.ds(at, tile)
                    both = transform(own[...], k, at) + m1_recv[1 - side, k, :, there].astype(f32)
                    p_send[side, u, :, there] = both.astype(bf16)
                    pre[side, u, :, there] = both

                p_copy(me, side, u).start()

        learn_of_peers()

        def arrived(k, at):
            there = pl.ds(at, tile)
            both = transform(own[...], k, at)
            return weighted(k, at, both + (
                m1_recv[0, k, :, there].astype(f32) + m1_recv[1, k, :, there].astype(f32)))

        def arrive(k, first, width):
            @tiles(width, 2)
            def _(at):
                at = pl.multiple_of(first + at, tile)
                parts = arrived(k, at)
                add_terms(0, parts)
                store(k, at, parts)

        @pl.loop(0, common - 1)
        def _(k):
            for side in range(2):
                @pl.when(k == 0)
                def _():
                    for c in range(lifts):
                        lifted_copy(side, side, c).wait_recv()
                    rest_copy(side, side).wait_recv()

                @pl.when(k > 0)
                def _():
                    m1_copy(side, side, k).wait_recv()
            arrive(k, 0, span)

        @pl.loop(0, tail)
        def _(n):
            for side in range(2):
                m1_copy(side, side, common - 1, n).wait_recv()
            arrive(common - 1, n * short, short)

        sums = sums_of(0)
        for side in range(2):
            e_copy(side, side).wait_recv()
            sums = sums + e_recv[side]
        exchange(sums)

        @pl.loop(0, steps)
        def _(k):
            for side in range(2):
                for refs in (a_refs, n1_refs, n2_refs):
                    remote(*refs, side, k).wait_send()

        for side in range(2):
            for u in range(2):
                p_copy(me, side, u).wait_send()

        for c in range(lifts):
            @pl.when(comes_up(c))
            def _():
                for side in range(2):
                    down_copy(side, c).wait_send()

        def complete(side, u, at):
            k = common + 2 * u + side
            there = pl.ds(at, tile)
            store(k, at, weighted(
                k, at, pre[side, u, :, there] + m1_recv[side, k, :, there].astype(f32)))

        for side in range(2):
            m1_copy(side, side, common + side).wait_recv()
            tiles(span, 2)(functools.partial(complete, side, 0))

        @pl.loop(0, tail)
        def _(n):
            @pl.when(n == tail // 2)
            def _():
                gather()

            for side in range(2):
                m1_copy(side, side, common + 2 + side, n).wait_recv()
                for c in range(0, short, tile):
                    complete(side, 1, pl.multiple_of(n * short + c, tile))


def flush_kernel(spectra, gram, spectra_out, gram_out, sems):
    copies = [pltpu.make_async_copy(gram, gram_out, sems.at[0])]
    for f in range(spectra.shape[0]):
        copies.append(pltpu.make_async_copy(spectra.at[f], spectra_out.at[f], sems.at[f + 1]))
    for copy in copies:
        copy.start()
    for copy in copies:
        copy.wait()


def kernel_on_device(snapshots, quad_weights, spectral_indices):
    record, variables, points = snapshots.shape
    groups = lax.axis_size("ta")
    npx, npy = lax.axis_size("px"), lax.axis_size("py")
    modes = spectral_indices.shape[0] // groups
    unit = 2 * modes
    pieces, tail = 2, 4
    span = points // pieces
    half = span // 2
    tile = math.gcd(512, span // tail)
    steps = variables * pieces
    lift = min(256, span // npy)
    lifts = npy - 1
    bf16, f32 = jnp.bfloat16, jnp.float32
    peers = npx * npy - 1
    dma = pltpu.SemaphoreType.DMA
    hbm = pl.BlockSpec(memory_space=pltpu.HBM)
    vmem = pl.BlockSpec(memory_space=pltpu.VMEM)
    spectra, gram = pl.pallas_call(
        functools.partial(
            window_kernel, pieces, tail, tile, 1.0 / (points * npx * npy * variables)),
        out_shape=(
            jax.ShapeDtypeStruct((modes, SEGMENT_NUMBER, variables, 2, points), f32),
            jax.ShapeDtypeStruct((SEGMENT_NUMBER * SEGMENT_NUMBER * 2, modes), f32),
        ),
        in_specs=[hbm, hbm, hbm],
        out_specs=(vmem, vmem),
        scratch_shapes=[
            pltpu.VMEM((variables, record, points), bf16),
            pltpu.SMEM(spectral_indices.shape, jnp.int32),
            pltpu.VMEM((1, points), f32),
            pltpu.VMEM((3 * SEGMENT_NUMBER * unit, record), bf16),
            pltpu.VMEM((SEGMENT_NUMBER * unit, record), bf16),
            pltpu.VMEM((1, points), f32),
            pltpu.VMEM((2, steps, SEGMENT_NUMBER * unit, half), bf16),
            pltpu.VMEM((2, steps, SEGMENT_NUMBER * unit, half), bf16),
            pltpu.VMEM((2, steps, unit, half), bf16),
            pltpu.VMEM((2, steps, unit, half), bf16),
            pltpu.VMEM((2, steps, unit, half), bf16),
            pltpu.VMEM((2, steps, unit, half), bf16),
            pltpu.VMEM((2, steps, SEGMENT_NUMBER * unit, span), bf16),
            pltpu.VMEM((2, steps, SEGMENT_NUMBER * unit, span), bf16),
            pltpu.VMEM((lifts, 2, SEGMENT_NUMBER * unit, lift), bf16),
            pltpu.VMEM((2, 2, SEGMENT_NUMBER * unit, span), bf16),
            pltpu.VMEM((2, 2, SEGMENT_NUMBER * unit, span), bf16),
            pltpu.VMEM((2, 2, SEGMENT_NUMBER * unit, span), f32),
            pltpu.VMEM((2, modes, 128), f32),
            pltpu.VMEM((2, modes, 128), f32),
            pltpu.VMEM((3, 4, modes, 128), f32),
            pltpu.VMEM((modes, 128), f32),
            pltpu.VMEM((peers, modes, 128), f32),
            dma((steps,)), dma, dma,
            dma((2, steps)), dma((2, steps)), dma((2, steps)), dma((2, steps)),
            dma((2, steps)), dma((2, steps)),
            dma((2, steps + 2 * tail)), dma((2, steps + 2 * tail)),
            dma((lifts, 2)), dma((lifts, 2)), dma((lifts, 2)), dma((lifts, 2)),
            dma((2, 2)), dma((2, 2)), dma((2,)), dma((2,)),
            dma((peers,)), dma((peers,)),
            pltpu.SemaphoreType.REGULAR((3,)),
        ],
        compiler_params=pltpu.CompilerParams(
            collective_id=0, has_side_effects=True, vmem_limit_bytes=44 * 1024 * 1024),
        name="window_transform",
    )(*(
        pltpu.with_memory_space_constraint(a, pltpu.HBM)
        for a in (snapshots.transpose(1, 0, 2), quad_weights.reshape(1, points), spectral_indices)
    ))
    spectra, gram = pl.pallas_call(
        flush_kernel,
        out_shape=(
            jax.ShapeDtypeStruct(spectra.shape, f32), jax.ShapeDtypeStruct(gram.shape, f32)),
        in_specs=[vmem, vmem],
        out_specs=(hbm, hbm),
        scratch_shapes=[dma((modes + 1,))],
        compiler_params=pltpu.CompilerParams(vmem_limit_bytes=1024 * 1024),
        name="flush",
    )(*(pltpu.with_memory_space_constraint(a, pltpu.VMEM) for a in (spectra, gram)))
    gram = gram.reshape(SEGMENT_NUMBER, SEGMENT_NUMBER, 2, modes)
    return spectra.transpose(0, 1, 3, 2, 4), gram.transpose(3, 0, 1, 2)


def solution(mesh):
    square = mesh.shape["ta"] == 4
    return jax.shard_map(
        kernel_on_device if square else plain_on_device,
        mesh=mesh,
        in_specs=(P("ta", None, ("px", "py")), P(("px", "py")), P()),
        out_specs=(P("ta", None, None, None, ("px", "py")), P("ta", None, None, None)),
        check_vma=False,
    )
```

```python
import functools
import math

import jax
import jax.numpy as jnp
from jax import lax
from jax.experimental import pallas as pl
from jax.experimental.pallas import tpu as pltpu
from jax.sharding import PartitionSpec as P

VARS = 5
BLK = 256
HOP = 128
SEGMENT_NUMBER = 2
RETAINED_MODES = 32

MESH = pl.DeviceIdType.MESH


def make_rotation_multipliers(spectral_indices, temporal_locations):
    segment_beginnings = jnp.arange(SEGMENT_NUMBER, dtype=jnp.int32) * HOP
    segment_shifts = temporal_locations[None, :] - segment_beginnings[:, None]
    inside = (segment_shifts >= 0) & (segment_shifts < BLK)
    window = 0.5 - 0.5 * jnp.cos(2.0 * math.pi * segment_shifts.astype(jnp.float32) / BLK)
    window = jnp.where(inside, window, jnp.float32(0.0)) / jnp.sqrt(jnp.float32(3.0 * BLK / 8.0))
    phases = jnp.mod(spectral_indices[:, None, None] * segment_shifts[None, :, :], BLK)
    angles = 2.0 * math.pi * phases.astype(jnp.float32) / BLK
    real_part = jnp.cos(angles) * window[None]
    imag_part = -jnp.sin(angles) * window[None]
    gathered_segments = jnp.stack([real_part, imag_part], axis=2)
    return gathered_segments.reshape(
        RETAINED_MODES * SEGMENT_NUMBER * 2, temporal_locations.shape[0]
    ).astype(jnp.bfloat16)


def gram_terms(spectra):
    flat = spectra.reshape(spectra.shape[0], 2 * SEGMENT_NUMBER, -1)
    inner = jnp.einsum("fam,fbm->fab", flat, flat, precision=lax.Precision.HIGHEST)
    inner = inner.reshape(spectra.shape[0], SEGMENT_NUMBER, 2, SEGMENT_NUMBER, 2)
    real_part = inner[:, :, 0, :, 0] + inner[:, :, 1, :, 1]
    imag_part = inner[:, :, 0, :, 1] - inner[:, :, 1, :, 0]
    return jnp.stack([real_part, imag_part], axis=-1)


def plain_on_device(snapshots, quad_weights, spectral_indices):
    record_length = snapshots.shape[0]
    point_count = snapshots.shape[2]
    groups = lax.axis_size("ta")
    temporal_locations = lax.axis_index("ta") * record_length + jnp.arange(
        record_length, dtype=jnp.int32
    )
    rotation_multipliers = make_rotation_multipliers(spectral_indices, temporal_locations)
    flat_snapshots = snapshots.reshape(record_length, VARS * point_count)
    raw = lax.psum_scatter(
        jnp.dot(rotation_multipliers, flat_snapshots, preferred_element_type=jnp.float32),
        "ta",
        scatter_dimension=0,
        tiled=True,
    )
    raw = raw.reshape(RETAINED_MODES // groups, SEGMENT_NUMBER, 2, VARS, point_count)
    spectra = raw * jnp.sqrt(quad_weights)
    summed = lax.psum(gram_terms(spectra), ("px", "py"))
    total_points = point_count * lax.axis_size("px") * lax.axis_size("py")
    gram = summed / jnp.float32(total_points * VARS)
    return (spectra, gram)


def sine_of_turn(m):
    quarter = BLK // 4
    r = jnp.bitwise_and(m + quarter, BLK - 1) - quarter
    r = jnp.where(r > quarter, BLK // 2 - r, r)
    x = r.astype(jnp.float32) * (2.0 * math.pi / BLK)
    y = x * x
    total = jnp.full_like(x, -1.0 / math.factorial(11))
    for n in (9, 7, 5, 3, 1):
        total = total * y + (1.0 if n % 4 == 1 else -1.0) / math.factorial(n)
    return total * x


def window_kernel(
    pieces, tail, tile, gram_scale,
    snap_hbm, weight_hbm, index_hbm, out_ref, gram_ref,
    snap, index_ref, weight_ref, twiddle, own, root,
    a_send, a_recv, n1_send, n1_recv, n2_send, n2_recv, m1_send, m1_recv,
    relay, p_send, p_recv, pre, e_send, e_recv, acc, gram_send, gram_recv,
    load_sem, index_sem, weight_sem,
    a_ssem, a_rsem, n1_ssem, n1_rsem, n2_ssem, n2_rsem, m1_ssem, m1_rsem,
    relay_ssem, relay_rsem, lift_ssem, lift_rsem,
    p_ssem, p_rsem, e_ssem, e_rsem, gram_ssem, gram_rsem, ready_sem,
):
    px, py, ta = lax.axis_index("px"), lax.axis_index("py"), lax.axis_index("ta")
    npx, npy = lax.axis_size("px"), lax.axis_size("py")
    variables, record, points = snap_hbm.shape
    modes = out_ref.shape[0]
    unit = 2 * modes
    steps = variables * pieces
    span = points // pieces
    half = span // 2
    short = span // tail
    common = steps - 4
    batch = 3 if steps % 3 == 1 else 1
    lifts, lift = relay.shape[0], relay.shape[3]
    f32, bf16 = jnp.float32, jnp.bfloat16

    inner = (ta == 1) | (ta == 2)
    outer = jnp.logical_not(inner)
    me = jnp.where(inner, ta - 1, ta // 3)
    sides = (jnp.where(inner, 0, 1), jnp.where(inner, 3, 2))

    def load(k):
        there = pl.ds(pl.multiple_of(lax.rem(k, pieces) * span, span), span)
        return pltpu.make_async_copy(
            snap_hbm.at[k // pieces, :, there], snap.at[k // pieces, :, there], load_sem.at[k])

    index_copy = pltpu.make_async_copy(index_hbm, index_ref, index_sem)
    weight_copy = pltpu.make_async_copy(weight_hbm, weight_ref, weight_sem)
    index_copy.start()
    load(0).start()

    peers = [
        (i, j, lax.rem(px + i, npx), lax.rem(py + j, npy))
        for i in range(npx) for j in range(npy) if i + j > 0
    ]
    barrier = pltpu.get_barrier_semaphore()
    for side in sides:
        pl.semaphore_signal(barrier, inc=1, device_id=(px, py, side), device_id_type=MESH)
    for i in range(1, npx):
        pl.semaphore_signal(barrier, inc=1, device_id=(lax.rem(px + i, npx), py, ta), device_id_type=MESH)
    below, above = py > 0, py < npy - 1
    for there, step in ((below, -1), (above, 1)):
        @pl.when(there)
        def _():
            pl.semaphore_signal(barrier, inc=1, device_id=(px, py + step, ta), device_id_type=MESH)
    greeted = len(sides) + npx - 1 + jnp.where(below, 1, 0) + jnp.where(above, 1, 0)

    sublane = lax.broadcasted_iota(jnp.int32, (modes, record), 0)
    moment = lax.broadcasted_iota(jnp.int32, (modes, record), 1) + ta * record
    shifts, windows = [], []
    for block in range(SEGMENT_NUMBER):
        shift = moment - block * HOP
        inside = (shift >= 0) & (shift < BLK)
        hann = 0.5 - 0.5 * sine_of_turn(shift + BLK // 4)
        shifts.append(shift)
        windows.append(jnp.where(inside, hann, 0.0) / math.sqrt(3.0 * BLK / 8.0))
    index_copy.wait()
    for place, owner in enumerate((3 - ta, sides[0], sides[1], ta)):
        bins = jnp.zeros((modes, record), jnp.int32)
        for f in range(modes):
            bins = jnp.where(sublane == f, index_ref[owner * modes + f], bins)
        for block in range(SEGMENT_NUMBER):
            shift, hann = shifts[block], windows[block]
            phase = bins * shift
            rows = jnp.concatenate(
                [sine_of_turn(phase + BLK // 4) * hann, -sine_of_turn(phase) * hann], axis=0)
            if place < 3:
                at = jnp.where(inner, place * SEGMENT_NUMBER + block, block * 3 + place)
                twiddle[pl.ds(pl.multiple_of(at * unit, unit), unit), :] = rows.astype(bf16)
            else:
                own[block * unit:(block + 1) * unit, :] = rows.astype(bf16)
    acc[...] = jnp.zeros_like(acc)

    a_refs = (a_send, a_recv, a_ssem, a_rsem)
    n1_refs = (n1_send, n1_recv, n1_ssem, n1_rsem)
    n2_refs = (n2_send, n2_recv, n2_ssem, n2_rsem)

    def batch_copy(refs, here, side, first, count):
        send, recv, ssem, rsem = refs
        units = pl.ds(first, count)
        return pltpu.make_async_remote_copy(
            src_ref=send.at[side, units], dst_ref=recv.at[here, units],
            send_sem=ssem.at[side, first], recv_sem=rsem.at[here, first],
            device_id=(px, py, sides[side]), device_id_type=MESH,
        )

    m1_refs = (m1_send, m1_recv, m1_ssem, m1_rsem)

    def start_batch(refs, side, k):
        @pl.when(k == 0)
        def _():
            batch_copy(refs, me, side, 0, 1).start()

        @pl.when((k > 0) & (lax.rem(k, batch) == 0))
        def _():
            batch_copy(refs, me, side, k + 1 - batch, batch).start()

    def wait_batch(refs, side, k):
        @pl.when(k == 0)
        def _():
            batch_copy(refs, side, side, 0, 1).wait_recv()

        @pl.when((k > 0) & (lax.rem(k - 1, batch) == 0))
        def _():
            batch_copy(refs, side, side, k, batch).wait_recv()

    def wait_sent(refs, side):
        batch_copy(refs, me, side, 0, 1).wait_send()

        @pl.loop(0, (steps - 1) // batch)
        def _(n):
            batch_copy(refs, me, side, 1 + n * batch, batch).wait_send()

    def tail_copy(here, side, k, n):
        columns = pl.ds(pl.multiple_of(n * short, short), short)
        return pltpu.make_async_remote_copy(
            src_ref=m1_send.at[side, k, :, columns], dst_ref=m1_recv.at[here, k, :, columns],
            send_sem=m1_ssem.at[side, steps + n], recv_sem=m1_rsem.at[here, steps + n],
            device_id=(px, py, sides[side]), device_id_type=MESH,
        )

    def up_copy(here, c):
        return pltpu.make_async_remote_copy(
            src_ref=m1_send.at[0, 0, :, pl.ds(c * lift, lift)], dst_ref=relay.at[c, here],
            send_sem=lift_ssem.at[c], recv_sem=relay_rsem.at[c, here],
            device_id=(px, py + 1, sides[0]), device_id_type=MESH,
        )

    def down_copy(side, c):
        return pltpu.make_async_remote_copy(
            src_ref=relay.at[c, side], dst_ref=m1_recv.at[side, 0, :, pl.ds(c * lift, lift)],
            send_sem=relay_ssem.at[c, side], recv_sem=lift_rsem.at[c, side],
            device_id=(px, py - 1, ta), device_id_type=MESH,
        )

    def comes_up(c):
        return (py > 0) & (c < npy - py)

    def rest_copy(here, side, n):
        columns = pl.ds(n * lift, span - n * lift)
        return pltpu.make_async_remote_copy(
            src_ref=m1_send.at[side, 0, :, columns], dst_ref=m1_recv.at[here, 0, :, columns],
            send_sem=m1_ssem.at[side, 0], recv_sem=m1_rsem.at[here, 0],
            device_id=(px, py, sides[side]), device_id_type=MESH,
        )

    def p_copy(here, side, u):
        return pltpu.make_async_remote_copy(
            src_ref=p_send.at[side, u], dst_ref=p_recv.at[here, u],
            send_sem=p_ssem.at[side, u], recv_sem=p_rsem.at[here, u],
            device_id=(px, py, sides[side]), device_id_type=MESH,
        )

    beside = jnp.bitwise_xor(py, 1) if npy % 2 == 0 else py

    def e_copy(here, side):
        return pltpu.make_async_remote_copy(
            src_ref=e_send.at[side], dst_ref=e_recv.at[here],
            send_sem=e_ssem.at[side], recv_sem=e_rsem.at[here],
            device_id=(px, beside, sides[side]), device_id_type=MESH,
        )

    def columns(k, at):
        return pl.ds(pl.multiple_of(lax.rem(k, pieces) * span + at, 128), tile)

    def transform(rows, k, at):
        return jnp.dot(rows, snap[k // pieces, :, columns(k, at)], preferred_element_type=f32)

    def loaded(k):
        load(k).wait()

        @pl.when(k == 0)
        def _():
            for later in range(1, steps):
                load(later).start()
            weight_copy.start()

    def tiles(width, unroll=1):
        def run(body):
            @pl.loop(0, width // tile, unroll=unroll)
            def _(i):
                body(pl.multiple_of(i * tile, tile))
        return run

    def meet(k):
        @pl.when(k == 0)
        def _():
            pl.semaphore_wait(barrier, greeted)

    def learn_of_peers():
        for n, (back, forth, step) in enumerate(((below, above, 1), (above, below, -1))):
            @pl.when(back)
            def _():
                pl.semaphore_wait(ready_sem.at[n], 1)

            @pl.when(forth)
            def _():
                pl.semaphore_signal(
                    ready_sem.at[n], inc=1, device_id=(px, py + step, ta), device_id_type=MESH)

        for i in range(1, npx):
            pl.semaphore_signal(
                ready_sem.at[2], inc=1, device_id=(lax.rem(px + i, npx), py, ta), device_id_type=MESH)
        if npx > 1:
            pl.semaphore_wait(ready_sem.at[2], npx - 1)

    def weighted(k, at, both):
        weight = root[:, columns(k, at)]
        return [
            (both[b * unit:b * unit + modes] * weight, both[b * unit + modes:(b + 1) * unit] * weight)
            for b in range(SEGMENT_NUMBER)]

    def add_terms(place, parts):
        (r0, i0), (r1, i1) = parts
        terms = (r0 * r0 + i0 * i0, r1 * r1 + i1 * i1, r0 * r1 + i0 * i1, r0 * i1 - i0 * r1)
        for n, term in enumerate(terms):
            lanes = [term[:, c:c + 128] for c in range(0, tile, 128)]
            acc[place, n] += functools.reduce(jnp.add, lanes)

    def store(k, at, parts):
        here = columns(k, at)
        for block, pair in enumerate(parts):
            for c in range(2):
                out_ref[:, block, k // pieces, c, here] = pair[c]

    def sums_of(place):
        lane = lax.broadcasted_iota(jnp.int32, gram_send.shape, 1)
        sums = jnp.zeros(gram_send.shape, f32)
        for n in range(4):
            sums = jnp.where(lane == n, jnp.sum(acc[place, n], axis=1, keepdims=True), sums)
        return sums

    def gram_copy(n):
        i, j, x, y = peers[n]
        return pltpu.make_async_remote_copy(
            src_ref=gram_send, dst_ref=gram_recv.at[n],
            send_sem=gram_ssem.at[n], recv_sem=gram_rsem.at[n],
            device_id=(x, y, ta), device_id_type=MESH,
        )

    def exchange(sums):
        gram_send[...] = sums
        for n in range(len(peers)):
            gram_copy(n).start()

    def weights():
        weight_copy.wait()
        root[...] = jnp.sqrt(weight_ref[...])

    def gather():
        total = gram_send[...]
        for n in range(len(peers)):
            gram_copy(n).wait()
            total = total + gram_recv[n]
        row = lax.broadcasted_iota(jnp.int32, (8, 128), 0)
        lane = lax.broadcasted_iota(jnp.int32, (8, 128), 1)
        pick = jnp.zeros((8, 128), f32)
        for r, n, sign in ((0, 0, 1.0), (2, 2, 1.0), (3, 3, 1.0), (4, 2, 1.0), (5, 3, -1.0), (6, 1, 1.0)):
            pick = jnp.where((row == r) & (lane == n), sign, pick)
        gram_ref[...] = gram_scale * lax.dot_general(
            pick, total, (((1,), (1,)), ((), ())),
            precision=lax.Precision.HIGHEST, preferred_element_type=f32,
        )

    @pl.when(inner)
    def _():
        @pl.loop(0, steps)
        def _(k):
            loaded(k)
            for side in range(2):
                @tiles(half, 4)
                def _(at):
                    a_send[side, k, :, pl.ds(at, tile)] = transform(
                        twiddle[0:2 * unit, :], k, side * half + at).astype(bf16)
                if side == 0:
                    meet(k)

                start_batch(a_refs, side, k)

        @pl.loop(0, steps)
        def _(k):
            for side in range(2):
                wait_batch(n2_refs, side, k)

        @pl.loop(0, steps)
        def _(j):
            k = jnp.where(
                j < 2, common + 2 * (1 - me) + j,
                jnp.where(j < common + 2, j - 2, 2 * me + j - 2))
            for dependent in range(2):
                first = half * (me if dependent else 1 - me)
                @tiles(half)
                def _(at):
                    product = transform(twiddle[2 * unit:6 * unit, :], k, first + at)
                    there = pl.ds(pl.multiple_of(first + at, 128), tile)
                    for side in range(2):
                        for block in range(SEGMENT_NUMBER):
                            r = (side * SEGMENT_NUMBER + block) * unit
                            rows = product[r:r + unit]
                            if dependent and block != side:
                                rows = rows + n2_recv[block, k, :, pl.ds(at, tile)].astype(f32)
                            m1_send[side, k, block * unit:(block + 1) * unit, there] = rows.astype(bf16)

            @pl.when(j == 1)
            def _():
                for side in range(2):
                    batch_copy(m1_refs, me, side, k - 1, 2).start()

            @pl.when(k == 0)
            def _():
                for n in range(lifts + 1):
                    @pl.when(n == npy - 1 - py)
                    def _():
                        for c in range(n):
                            up_copy(me, c).start()
                        rest_copy(me, 0, n).start()
                rest_copy(me, 1, 0).start()

            @pl.when(k == common - 3)
            def _():
                for side in range(2):
                    batch_copy(m1_refs, me, side, 1, common - 3).start()

            @pl.when(k == common - 1)
            def _():
                for side in range(2):
                    batch_copy(m1_refs, me, side, common - 2, 2).start()

            @pl.when(j == steps - 2)
            def _():
                for side in range(2):
                    batch_copy(m1_refs, me, side, k, 1).start()

            @pl.when(j == steps - 1)
            def _():
                for n in range(tail):
                    for side in range(2):
                        tail_copy(me, side, k, n).start()

        weights()
        learn_of_peers()

        @pl.loop(0, steps)
        def _(k):
            for side in range(2):
                wait_batch(a_refs, side, k)
                wait_batch(n1_refs, side, k)

            for side in range(2):
                @tiles(half)
                def _(at):
                    both = transform(own[...], k, side * half + at)
                    both = both + a_recv[side, k, :, pl.ds(at, tile)].astype(f32)
                    extra = n1_recv[1 - side, k, :, pl.ds(at, tile)].astype(f32)
                    rows = [both[:unit], both[unit:]]
                    rows[1 - side] = rows[1 - side] + extra
                    parts = weighted(k, side * half + at, jnp.concatenate(rows, axis=0))
                    add_terms(0, parts)
                    store(k, side * half + at, parts)

        exchange(sums_of(0))
        for u in range(2):
            for side in range(2):
                p_copy(side, side, u).wait_recv()

                @tiles(span, 2)
                def _(at):
                    there = pl.ds(at, tile)
                    k = common + 2 * me + u
                    both = p_recv[side, u, :, there].astype(f32) + m1_send[side, k, :, there].astype(f32)
                    add_terms(1 + side, weighted(k, at, both))

        for side in range(2):
            e_send[side] = sums_of(1 + side)
            e_copy(me, side).start()

        gather()
        for side in range(2):
            e_copy(me, side).wait_send()
            wait_sent(a_refs, side)
            batch_copy(m1_refs, me, side, common + 2 * (1 - me), 2).wait_send()
            batch_copy(m1_refs, me, side, 1, common - 3).wait_send()
            batch_copy(m1_refs, me, side, common - 2, 2).wait_send()
            batch_copy(m1_refs, me, side, common + 2 * me, 1).wait_send()

            @pl.loop(0, tail)
            def _(n):
                tail_copy(me, side, common + 2 * me + 1, n).wait_send()

        for n in range(lifts + 1):
            @pl.when(n == npy - 1 - py)
            def _():
                for c in range(n):
                    up_copy(me, c).wait_send()
                rest_copy(me, 0, n).wait_send()
        rest_copy(me, 1, 0).wait_send()

    @pl.when(outer)
    def _():
        base = me * (3 * unit)
        far = pl.ds(pl.multiple_of(base, unit), unit)
        near = pl.ds(pl.multiple_of(base + unit, unit), 2 * unit)

        @pl.loop(0, steps)
        def _(k):
            loaded(k)
            for side in range(2):
                @tiles(half, 4)
                def _(at):
                    n2_send[side, k, :, pl.ds(at, tile)] = transform(
                        twiddle[far, :], k, side * half + at).astype(bf16)
                if side == 0:
                    meet(k)
                start_batch(n2_refs, side, k)

        @pl.loop(0, steps)
        def _(k):
            @tiles(half)
            def _(at):
                product = transform(twiddle[near, :], k, (1 - me) * half + at)
                for side in range(2):
                    n1_send[side, k, :, pl.ds(at, tile)] = product[side * unit:(side + 1) * unit].astype(bf16)
            for side in range(2):
                start_batch(n1_refs, side, k)
            for side in range(2):
                wait_batch(a_refs, side, k)

            @tiles(half)
            def _(at):
                here = pl.ds(at, tile)
                product = transform(twiddle[near, :], k, me * half + at)
                for side in range(2):
                    rows = product[side * unit:(side + 1) * unit]
                    for block in range(SEGMENT_NUMBER):
                        there = slice(block * unit, (block + 1) * unit)
                        came = a_recv[1 - side, k, there, here].astype(f32)
                        total = came + jnp.where(me == block, rows, 0.0)
                        a_send[side, k, there, here] = total.astype(bf16)
            for side in range(2):
                start_batch(a_refs, side, k)

        weights()

        for c in range(lifts):
            @pl.when(comes_up(c) & (me == 0))
            def _():
                for side in range(2):
                    up_copy(side, c).wait_recv()
                    down_copy(side, c).start()

        for u in range(2):
            for side in range(2):
                k = common + 2 * side + u
                if u == 0:
                    batch_copy(m1_refs, 1 - side, 1 - side, k, 2).wait_recv()

                @tiles(span, 2)
                def _(at):
                    there = pl.ds(at, tile)
                    both = transform(own[...], k, at) + m1_recv[1 - side, k, :, there].astype(f32)
                    p_send[side, u, :, there] = both.astype(bf16)
                    pre[side, u, :, there] = both

                p_copy(me, side, u).start()

        learn_of_peers()

        def arrived(k, at):
            there = pl.ds(at, tile)
            both = transform(own[...], k, at)
            return weighted(k, at, both + (
                m1_recv[0, k, :, there].astype(f32) + m1_recv[1, k, :, there].astype(f32)))

        def arrive(k, first, width):
            @tiles(width, 2)
            def _(at):
                at = pl.multiple_of(first + at, tile)
                parts = arrived(k, at)
                add_terms(0, parts)
                store(k, at, parts)

        @pl.loop(0, common)
        def _(k):
            @pl.when(k == 0)
            def _():
                for n in range(lifts + 1):
                    @pl.when((me == 0) & (n == npy - 1 - py))
                    def _():
                        for side in range(2):
                            for c in range(n):
                                down_copy(side, c).wait_recv()
                            rest_copy(side, side, n).wait_recv()

                @pl.when(me == 1)
                def _():
                    for side in range(2):
                        rest_copy(side, side, 0).wait_recv()

            for first, count in ((1, common - 3), (common - 2, 2)):
                @pl.when(k == first)
                def _():
                    for side in range(2):
                        batch_copy(m1_refs, side, side, first, count).wait_recv()

            arrive(k, 0, span)

        sums = sums_of(0)
        for side in range(2):
            e_copy(side, side).wait_recv()
            sums = sums + e_recv[side]
        exchange(sums)

        for side in range(2):
            for refs in (a_refs, n1_refs, n2_refs):
                wait_sent(refs, side)

        for side in range(2):
            for u in range(2):
                p_copy(me, side, u).wait_send()

        for c in range(lifts):
            @pl.when(comes_up(c) & (me == 0))
            def _():
                for side in range(2):
                    down_copy(side, c).wait_send()

        def complete(side, u, at):
            k = common + 2 * side + u
            there = pl.ds(at, tile)
            store(k, at, weighted(
                k, at, pre[side, u, :, there] + m1_recv[side, k, :, there].astype(f32)))

        for side in range(2):
            batch_copy(m1_refs, side, side, common + 2 * side, 1).wait_recv()
            tiles(span, 2)(functools.partial(complete, side, 0))

        @pl.loop(0, tail)
        def _(n):
            @pl.when(n == tail // 2)
            def _():
                gather()

            for side in range(2):
                tail_copy(side, side, common + 2 * side + 1, n).wait_recv()
                for c in range(0, short, tile):
                    complete(side, 1, pl.multiple_of(n * short + c, tile))


def flush_kernel(spectra, gram, spectra_out, gram_out, sems):
    copies = [pltpu.make_async_copy(gram, gram_out, sems.at[0])]
    for f in range(spectra.shape[0]):
        copies.append(pltpu.make_async_copy(spectra.at[f], spectra_out.at[f], sems.at[f + 1]))
    for copy in copies:
        copy.start()
    for copy in copies:
        copy.wait()


def kernel_on_device(snapshots, quad_weights, spectral_indices):
    record, variables, points = snapshots.shape
    groups = lax.axis_size("ta")
    npx, npy = lax.axis_size("px"), lax.axis_size("py")
    modes = spectral_indices.shape[0] // groups
    unit = 2 * modes
    pieces, tail = 2, 4
    span = points // pieces
    half = span // 2
    tile = math.gcd(512, span // tail)
    steps = variables * pieces
    lift = min(256, span // npy)
    lifts = npy - 1
    bf16, f32 = jnp.bfloat16, jnp.float32
    peers = npx * npy - 1
    dma = pltpu.SemaphoreType.DMA
    hbm = pl.BlockSpec(memory_space=pltpu.HBM)
    vmem = pl.BlockSpec(memory_space=pltpu.VMEM)
    spectra, gram = pl.pallas_call(
        functools.partial(
            window_kernel, pieces, tail, tile, 1.0 / (points * npx * npy * variables)),
        out_shape=(
            jax.ShapeDtypeStruct((modes, SEGMENT_NUMBER, variables, 2, points), f32),
            jax.ShapeDtypeStruct((SEGMENT_NUMBER * SEGMENT_NUMBER * 2, modes), f32),
        ),
        in_specs=[hbm, hbm, hbm],
        out_specs=(vmem, vmem),
        scratch_shapes=[
            pltpu.VMEM((variables, record, points), bf16),
            pltpu.SMEM(spectral_indices.shape, jnp.int32),
            pltpu.VMEM((1, points), f32),
            pltpu.VMEM((3 * SEGMENT_NUMBER * unit, record), bf16),
            pltpu.VMEM((SEGMENT_NUMBER * unit, record), bf16),
            pltpu.VMEM((1, points), f32),
            pltpu.VMEM((2, steps, SEGMENT_NUMBER * unit, half), bf16),
            pltpu.VMEM((2, steps, SEGMENT_NUMBER * unit, half), bf16),
            pltpu.VMEM((2, steps, unit, half), bf16),
            pltpu.VMEM((2, steps, unit, half), bf16),
            pltpu.VMEM((2, steps, unit, half), bf16),
            pltpu.VMEM((2, steps, unit, half), bf16),
            pltpu.VMEM((2, steps, SEGMENT_NUMBER * unit, span), bf16),
            pltpu.VMEM((2, steps, SEGMENT_NUMBER * unit, span), bf16),
            pltpu.VMEM((lifts, 2, SEGMENT_NUMBER * unit, lift), bf16),
            pltpu.VMEM((2, 2, SEGMENT_NUMBER * unit, span), bf16),
            pltpu.VMEM((2, 2, SEGMENT_NUMBER * unit, span), bf16),
            pltpu.VMEM((2, 2, SEGMENT_NUMBER * unit, span), f32),
            pltpu.VMEM((2, modes, 128), f32),
            pltpu.VMEM((2, modes, 128), f32),
            pltpu.VMEM((3, 4, modes, 128), f32),
            pltpu.VMEM((modes, 128), f32),
            pltpu.VMEM((peers, modes, 128), f32),
            dma((steps,)), dma, dma,
            dma((2, steps)), dma((2, steps)), dma((2, steps)), dma((2, steps)),
            dma((2, steps)), dma((2, steps)),
            dma((2, steps + tail)), dma((2, steps + tail)),
            dma((lifts, 2)), dma((lifts, 2)), dma((lifts,)), dma((lifts, 2)),
            dma((2, 2)), dma((2, 2)), dma((2,)), dma((2,)),
            dma((peers,)), dma((peers,)),
            pltpu.SemaphoreType.REGULAR((3,)),
        ],
        compiler_params=pltpu.CompilerParams(
            collective_id=0, has_side_effects=True, vmem_limit_bytes=44 * 1024 * 1024),
        name="window_transform",
    )(*(
        pltpu.with_memory_space_constraint(a, pltpu.HBM)
        for a in (snapshots.transpose(1, 0, 2), quad_weights.reshape(1, points), spectral_indices)
    ))
    spectra, gram = pl.pallas_call(
        flush_kernel,
        out_shape=(
            jax.ShapeDtypeStruct(spectra.shape, f32), jax.ShapeDtypeStruct(gram.shape, f32)),
        in_specs=[vmem, vmem],
        out_specs=(hbm, hbm),
        scratch_shapes=[dma((modes + 1,))],
        compiler_params=pltpu.CompilerParams(vmem_limit_bytes=1024 * 1024),
        name="flush",
    )(*(pltpu.with_memory_space_constraint(a, pltpu.VMEM) for a in (spectra, gram)))
    gram = gram.reshape(SEGMENT_NUMBER, SEGMENT_NUMBER, 2, modes)
    return spectra.transpose(0, 1, 3, 2, 4), gram.transpose(3, 0, 1, 2)


def solution(mesh):
    square = mesh.shape["ta"] == 4
    return jax.shard_map(
        kernel_on_device if square else plain_on_device,
        mesh=mesh,
        in_specs=(P("ta", None, ("px", "py")), P(("px", "py")), P()),
        out_specs=(P("ta", None, None, None, ("px", "py")), P("ta", None, None, None)),
        check_vma=False,
    )
```

```python
import functools
import math

import jax
import jax.numpy as jnp
from jax import lax
from jax.experimental import pallas as pl
from jax.experimental.pallas import tpu as pltpu
from jax.sharding import PartitionSpec as P

VARS = 5
BLK = 256
HOP = 128
SEGMENT_NUMBER = 2
RETAINED_MODES = 32

MESH = pl.DeviceIdType.MESH


def make_rotation_multipliers(spectral_indices, temporal_locations):
    segment_beginnings = jnp.arange(SEGMENT_NUMBER, dtype=jnp.int32) * HOP
    segment_shifts = temporal_locations[None, :] - segment_beginnings[:, None]
    inside = (segment_shifts >= 0) & (segment_shifts < BLK)
    window = 0.5 - 0.5 * jnp.cos(2.0 * math.pi * segment_shifts.astype(jnp.float32) / BLK)
    window = jnp.where(inside, window, jnp.float32(0.0)) / jnp.sqrt(jnp.float32(3.0 * BLK / 8.0))
    phases = jnp.mod(spectral_indices[:, None, None] * segment_shifts[None, :, :], BLK)
    angles = 2.0 * math.pi * phases.astype(jnp.float32) / BLK
    real_part = jnp.cos(angles) * window[None]
    imag_part = -jnp.sin(angles) * window[None]
    gathered_segments = jnp.stack([real_part, imag_part], axis=2)
    return gathered_segments.reshape(
        RETAINED_MODES * SEGMENT_NUMBER * 2, temporal_locations.shape[0]
    ).astype(jnp.bfloat16)


def gram_terms(spectra):
    flat = spectra.reshape(spectra.shape[0], 2 * SEGMENT_NUMBER, -1)
    inner = jnp.einsum("fam,fbm->fab", flat, flat, precision=lax.Precision.HIGHEST)
    inner = inner.reshape(spectra.shape[0], SEGMENT_NUMBER, 2, SEGMENT_NUMBER, 2)
    real_part = inner[:, :, 0, :, 0] + inner[:, :, 1, :, 1]
    imag_part = inner[:, :, 0, :, 1] - inner[:, :, 1, :, 0]
    return jnp.stack([real_part, imag_part], axis=-1)


def plain_on_device(snapshots, quad_weights, spectral_indices):
    record_length = snapshots.shape[0]
    point_count = snapshots.shape[2]
    groups = lax.axis_size("ta")
    temporal_locations = lax.axis_index("ta") * record_length + jnp.arange(
        record_length, dtype=jnp.int32
    )
    rotation_multipliers = make_rotation_multipliers(spectral_indices, temporal_locations)
    flat_snapshots = snapshots.reshape(record_length, VARS * point_count)
    raw = lax.psum_scatter(
        jnp.dot(rotation_multipliers, flat_snapshots, preferred_element_type=jnp.float32),
        "ta",
        scatter_dimension=0,
        tiled=True,
    )
    raw = raw.reshape(RETAINED_MODES // groups, SEGMENT_NUMBER, 2, VARS, point_count)
    spectra = raw * jnp.sqrt(quad_weights)
    summed = lax.psum(gram_terms(spectra), ("px", "py"))
    total_points = point_count * lax.axis_size("px") * lax.axis_size("py")
    gram = summed / jnp.float32(total_points * VARS)
    return (spectra, gram)


def sine_of_turn(m):
    quarter = BLK // 4
    r = jnp.bitwise_and(m + quarter, BLK - 1) - quarter
    r = jnp.where(r > quarter, BLK // 2 - r, r)
    x = r.astype(jnp.float32) * (2.0 * math.pi / BLK)
    y = x * x
    total = jnp.full_like(x, -1.0 / math.factorial(11))
    for n in (9, 7, 5, 3, 1):
        total = total * y + (1.0 if n % 4 == 1 else -1.0) / math.factorial(n)
    return total * x


def window_kernel(
    pieces, tail, tile, gram_scale,
    snap_hbm, weight_hbm, index_hbm, out_ref, gram_ref,
    snap, index_ref, weight_ref, twiddle, own, root,
    a_send, a_recv, n1_send, n1_recv, n2_send, n2_recv, m1_send, m1_recv,
    relay, moved, p_send, p_recv, pre, e_send, e_recv, acc, gram_send, gram_recv,
    load_sem, index_sem, weight_sem,
    a_ssem, a_rsem, n1_ssem, n1_rsem, n2_ssem, n2_rsem, m1_ssem, m1_rsem,
    moved_ssem, moved_rsem, relay_ssem, relay_rsem, lift_ssem, lift_rsem,
    p_ssem, p_rsem, e_ssem, e_rsem, gram_ssem, gram_rsem, ready_sem,
):
    px, py, ta = lax.axis_index("px"), lax.axis_index("py"), lax.axis_index("ta")
    npx, npy = lax.axis_size("px"), lax.axis_size("py")
    variables, record, points = snap_hbm.shape
    modes = out_ref.shape[0]
    unit = 2 * modes
    steps = variables * pieces
    span = points // pieces
    half = span // 2
    short = span // tail
    common = steps - 4
    batch = 3 if steps % 3 == 1 else 1
    lifts, lift = relay.shape[0], relay.shape[3]
    shift = moved.shape[2]
    kept, shifted = pl.ds(0, half - shift), pl.ds(half - shift, shift)
    f32, bf16 = jnp.float32, jnp.bfloat16

    inner = (ta == 1) | (ta == 2)
    outer = jnp.logical_not(inner)
    me = jnp.where(inner, ta - 1, ta // 3)
    sides = (jnp.where(inner, 0, 1), jnp.where(inner, 3, 2))

    @pl.when(outer & (me == 0))
    def _():
        a_recv[:, 0, :, shifted] = jnp.zeros((2, SEGMENT_NUMBER * unit, shift), bf16)

    def load(k):
        there = pl.ds(pl.multiple_of(lax.rem(k, pieces) * span, span), span)
        return pltpu.make_async_copy(
            snap_hbm.at[k // pieces, :, there], snap.at[k // pieces, :, there], load_sem.at[k])

    index_copy = pltpu.make_async_copy(index_hbm, index_ref, index_sem)
    weight_copy = pltpu.make_async_copy(weight_hbm, weight_ref, weight_sem)
    index_copy.start()
    load(0).start()

    peers = [
        (i, j, lax.rem(px + i, npx), lax.rem(py + j, npy))
        for i in range(npx) for j in range(npy) if i + j > 0
    ]
    barrier = pltpu.get_barrier_semaphore()
    for side in sides:
        pl.semaphore_signal(barrier, inc=1, device_id=(px, py, side), device_id_type=MESH)
    for i in range(1, npx):
        pl.semaphore_signal(barrier, inc=1, device_id=(lax.rem(px + i, npx), py, ta), device_id_type=MESH)
    below, above = py > 0, py < npy - 1
    for there, step in ((below, -1), (above, 1)):
        @pl.when(there)
        def _():
            pl.semaphore_signal(barrier, inc=1, device_id=(px, py + step, ta), device_id_type=MESH)
    greeted = len(sides) + npx - 1 + jnp.where(below, 1, 0) + jnp.where(above, 1, 0)

    sublane = lax.broadcasted_iota(jnp.int32, (modes, record), 0)
    moment = lax.broadcasted_iota(jnp.int32, (modes, record), 1) + ta * record
    shifts, windows = [], []
    for block in range(SEGMENT_NUMBER):
        shift = moment - block * HOP
        inside = (shift >= 0) & (shift < BLK)
        hann = 0.5 - 0.5 * sine_of_turn(shift + BLK // 4)
        shifts.append(shift)
        windows.append(jnp.where(inside, hann, 0.0) / math.sqrt(3.0 * BLK / 8.0))
    index_copy.wait()
    for place, owner in enumerate((3 - ta, sides[0], sides[1], ta)):
        bins = jnp.zeros((modes, record), jnp.int32)
        for f in range(modes):
            bins = jnp.where(sublane == f, index_ref[owner * modes + f], bins)
        for block in range(SEGMENT_NUMBER):
            shift, hann = shifts[block], windows[block]
            phase = bins * shift
            rows = jnp.concatenate(
                [sine_of_turn(phase + BLK // 4) * hann, -sine_of_turn(phase) * hann], axis=0)
            if place < 3:
                at = jnp.where(inner, place * SEGMENT_NUMBER + block, block * 3 + place)
                twiddle[pl.ds(pl.multiple_of(at * unit, unit), unit), :] = rows.astype(bf16)
            else:
                own[block * unit:(block + 1) * unit, :] = rows.astype(bf16)
    acc[...] = jnp.zeros_like(acc)

    a_refs = (a_send, a_recv, a_ssem, a_rsem)
    n1_refs = (n1_send, n1_recv, n1_ssem, n1_rsem)
    n2_refs = (n2_send, n2_recv, n2_ssem, n2_rsem)

    def batch_copy(refs, here, side, first, count):
        send, recv, ssem, rsem = refs
        units = pl.ds(first, count)
        return pltpu.make_async_remote_copy(
            src_ref=send.at[side, units], dst_ref=recv.at[here, units],
            send_sem=ssem.at[side, first], recv_sem=rsem.at[here, first],
            device_id=(px, py, sides[side]), device_id_type=MESH,
        )

    m1_refs = (m1_send, m1_recv, m1_ssem, m1_rsem)

    def kept_copy(here):
        return pltpu.make_async_remote_copy(
            src_ref=a_send.at[0, 0, :, kept], dst_ref=a_recv.at[here, 0, :, kept],
            send_sem=a_ssem.at[0, 0], recv_sem=a_rsem.at[here, 0],
            device_id=(px, py, sides[0]), device_id_type=MESH,
        )

    def shifted_copy(here):
        return pltpu.make_async_remote_copy(
            src_ref=a_send.at[0, 0, :, shifted], dst_ref=moved.at[here],
            send_sem=moved_ssem.at[0], recv_sem=moved_rsem.at[here],
            device_id=(px, py, sides[1]), device_id_type=MESH,
        )

    def forward_copy(here):
        return pltpu.make_async_remote_copy(
            src_ref=moved.at[here], dst_ref=moved.at[0],
            send_sem=moved_ssem.at[here], recv_sem=moved_rsem.at[0],
            device_id=(px, py, sides[1 - here]), device_id_type=MESH,
        )

    def start_batch(refs, side, k):
        @pl.when(k == 0)
        def _():
            if refs is a_refs and side == 0:
                @pl.when(inner)
                def _():
                    kept_copy(me).start()
                    shifted_copy(me).start()

                @pl.when(outer)
                def _():
                    batch_copy(refs, me, side, 0, 1).start()
            else:
                batch_copy(refs, me, side, 0, 1).start()

        @pl.when((k > 0) & (lax.rem(k, batch) == 0))
        def _():
            batch_copy(refs, me, side, k + 1 - batch, batch).start()

    def wait_batch(refs, side, k):
        @pl.when(k == 0)
        def _():
            if refs is a_refs:
                relays = outer & (me == 0)

                @pl.when(relays)
                def _():
                    kept_copy(side).wait_recv()

                @pl.when(jnp.logical_not(relays))
                def _():
                    batch_copy(refs, side, side, 0, 1).wait_recv()
            else:
                batch_copy(refs, side, side, 0, 1).wait_recv()

        @pl.when((k > 0) & (lax.rem(k - 1, batch) == 0))
        def _():
            batch_copy(refs, side, side, k, batch).wait_recv()

    def wait_sent(refs, side, first=None):
        (first or batch_copy(refs, me, side, 0, 1)).wait_send()

        @pl.loop(0, (steps - 1) // batch)
        def _(n):
            batch_copy(refs, me, side, 1 + n * batch, batch).wait_send()

    def tail_copy(here, side, k, n):
        columns = pl.ds(pl.multiple_of(n * short, short), short)
        return pltpu.make_async_remote_copy(
            src_ref=m1_send.at[side, k, :, columns], dst_ref=m1_recv.at[here, k, :, columns],
            send_sem=m1_ssem.at[side, steps + n], recv_sem=m1_rsem.at[here, steps + n],
            device_id=(px, py, sides[side]), device_id_type=MESH,
        )

    def up_copy(here, c):
        return pltpu.make_async_remote_copy(
            src_ref=m1_send.at[0, 0, :, pl.ds(c * lift, lift)], dst_ref=relay.at[c, here],
            send_sem=lift_ssem.at[c], recv_sem=relay_rsem.at[c, here],
            device_id=(px, py + 1, sides[0]), device_id_type=MESH,
        )

    def down_copy(side, c):
        return pltpu.make_async_remote_copy(
            src_ref=relay.at[c, side], dst_ref=m1_recv.at[side, 0, :, pl.ds(c * lift, lift)],
            send_sem=relay_ssem.at[c, side], recv_sem=lift_rsem.at[c, side],
            device_id=(px, py - 1, ta), device_id_type=MESH,
        )

    def comes_up(c):
        return (py > 0) & (c < npy - py)

    def rest_copy(here, side, n):
        columns = pl.ds(n * lift, span - n * lift)
        return pltpu.make_async_remote_copy(
            src_ref=m1_send.at[side, 0, :, columns], dst_ref=m1_recv.at[here, 0, :, columns],
            send_sem=m1_ssem.at[side, 0], recv_sem=m1_rsem.at[here, 0],
            device_id=(px, py, sides[side]), device_id_type=MESH,
        )

    def p_copy(here, side, u):
        return pltpu.make_async_remote_copy(
            src_ref=p_send.at[side, u], dst_ref=p_recv.at[here, u],
            send_sem=p_ssem.at[side, u], recv_sem=p_rsem.at[here, u],
            device_id=(px, py, sides[side]), device_id_type=MESH,
        )

    beside = jnp.bitwise_xor(py, 1) if npy % 2 == 0 else py

    def e_copy(here, side):
        return pltpu.make_async_remote_copy(
            src_ref=e_send.at[side], dst_ref=e_recv.at[here],
            send_sem=e_ssem.at[side], recv_sem=e_rsem.at[here],
            device_id=(px, beside, sides[side]), device_id_type=MESH,
        )

    def columns(k, at):
        return pl.ds(pl.multiple_of(lax.rem(k, pieces) * span + at, 128), tile)

    def transform(rows, k, at):
        return jnp.dot(rows, snap[k // pieces, :, columns(k, at)], preferred_element_type=f32)

    def loaded(k):
        load(k).wait()

        @pl.when(k == 0)
        def _():
            for later in range(1, steps):
                load(later).start()
            weight_copy.start()

    def tiles(width, unroll=1):
        def run(body):
            @pl.loop(0, width // tile, unroll=unroll)
            def _(i):
                body(pl.multiple_of(i * tile, tile))
        return run

    def meet(k):
        @pl.when(k == 0)
        def _():
            pl.semaphore_wait(barrier, greeted)

    def learn_of_peers():
        for n, (back, forth, step) in enumerate(((below, above, 1), (above, below, -1))):
            @pl.when(back)
            def _():
                pl.semaphore_wait(ready_sem.at[n], 1)

            @pl.when(forth)
            def _():
                pl.semaphore_signal(
                    ready_sem.at[n], inc=1, device_id=(px, py + step, ta), device_id_type=MESH)

        for i in range(1, npx):
            pl.semaphore_signal(
                ready_sem.at[2], inc=1, device_id=(lax.rem(px + i, npx), py, ta), device_id_type=MESH)
        if npx > 1:
            pl.semaphore_wait(ready_sem.at[2], npx - 1)

    def weighted(k, at, both):
        weight = root[:, columns(k, at)]
        return [
            (both[b * unit:b * unit + modes] * weight, both[b * unit + modes:(b + 1) * unit] * weight)
            for b in range(SEGMENT_NUMBER)]

    def add_terms(place, parts):
        (r0, i0), (r1, i1) = parts
        terms = (r0 * r0 + i0 * i0, r1 * r1 + i1 * i1, r0 * r1 + i0 * i1, r0 * i1 - i0 * r1)
        for n, term in enumerate(terms):
            lanes = [term[:, c:c + 128] for c in range(0, tile, 128)]
            acc[place, n] += functools.reduce(jnp.add, lanes)

    def store(k, at, parts):
        here = columns(k, at)
        for block, pair in enumerate(parts):
            for c in range(2):
                out_ref[:, block, k // pieces, c, here] = pair[c]

    def sums_of(place):
        lane = lax.broadcasted_iota(jnp.int32, gram_send.shape, 1)
        sums = jnp.zeros(gram_send.shape, f32)
        for n in range(4):
            sums = jnp.where(lane == n, jnp.sum(acc[place, n], axis=1, keepdims=True), sums)
        return sums

    def gram_copy(n):
        i, j, x, y = peers[n]
        return pltpu.make_async_remote_copy(
            src_ref=gram_send, dst_ref=gram_recv.at[n],
            send_sem=gram_ssem.at[n], recv_sem=gram_rsem.at[n],
            device_id=(x, y, ta), device_id_type=MESH,
        )

    def exchange(sums):
        gram_send[...] = sums
        for n in range(len(peers)):
            gram_copy(n).start()

    def weights():
        weight_copy.wait()
        root[...] = jnp.sqrt(weight_ref[...])

    def gather():
        total = gram_send[...]
        for n in range(len(peers)):
            gram_copy(n).wait()
            total = total + gram_recv[n]
        row = lax.broadcasted_iota(jnp.int32, (8, 128), 0)
        lane = lax.broadcasted_iota(jnp.int32, (8, 128), 1)
        pick = jnp.zeros((8, 128), f32)
        for r, n, sign in ((0, 0, 1.0), (2, 2, 1.0), (3, 3, 1.0), (4, 2, 1.0), (5, 3, -1.0), (6, 1, 1.0)):
            pick = jnp.where((row == r) & (lane == n), sign, pick)
        gram_ref[...] = gram_scale * lax.dot_general(
            pick, total, (((1,), (1,)), ((), ())),
            precision=lax.Precision.HIGHEST, preferred_element_type=f32,
        )

    @pl.when(inner)
    def _():
        @pl.loop(0, steps)
        def _(k):
            loaded(k)
            for side in range(2):
                @tiles(half, 4)
                def _(at):
                    a_send[side, k, :, pl.ds(at, tile)] = transform(
                        twiddle[0:2 * unit, :], k, side * half + at).astype(bf16)
                if side == 0:
                    meet(k)

                start_batch(a_refs, side, k)

        @pl.loop(0, steps)
        def _(k):
            for side in range(2):
                wait_batch(n2_refs, side, k)

        @pl.loop(0, steps)
        def _(j):
            k = jnp.where(
                j < 2, common + 2 * (1 - me) + j,
                jnp.where(j < common + 2, j - 2, 2 * me + j - 2))
            for dependent in range(2):
                first = half * (me if dependent else 1 - me)
                @tiles(half)
                def _(at):
                    product = transform(twiddle[2 * unit:6 * unit, :], k, first + at)
                    there = pl.ds(pl.multiple_of(first + at, 128), tile)
                    for side in range(2):
                        for block in range(SEGMENT_NUMBER):
                            r = (side * SEGMENT_NUMBER + block) * unit
                            rows = product[r:r + unit]
                            if dependent and block != side:
                                rows = rows + n2_recv[block, k, :, pl.ds(at, tile)].astype(f32)
                            m1_send[side, k, block * unit:(block + 1) * unit, there] = rows.astype(bf16)

            @pl.when(j == 1)
            def _():
                for side in range(2):
                    batch_copy(m1_refs, me, side, k - 1, 2).start()

            @pl.when(k == 0)
            def _():
                for n in range(lifts + 1):
                    @pl.when(n == npy - 1 - py)
                    def _():
                        for c in range(n):
                            up_copy(me, c).start()
                        rest_copy(me, 0, n).start()
                rest_copy(me, 1, 0).start()

            @pl.when(k == common - 3)
            def _():
                for side in range(2):
                    batch_copy(m1_refs, me, side, 1, common - 3).start()

            @pl.when(k == common - 1)
            def _():
                for side in range(2):
                    batch_copy(m1_refs, me, side, common - 2, 2).start()

            @pl.when(j == steps - 2)
            def _():
                for side in range(2):
                    batch_copy(m1_refs, me, side, k, 1).start()

            @pl.when(j == steps - 1)
            def _():
                for n in range(tail):
                    for side in range(2):
                        tail_copy(me, side, k, n).start()

        weights()
        learn_of_peers()

        @pl.loop(0, steps)
        def _(k):
            for side in range(2):
                wait_batch(a_refs, side, k)
                wait_batch(n1_refs, side, k)

            @pl.when(k == 0)
            def _():
                forward_copy(0).wait_recv()
                both = a_recv[0, 0, :, shifted].astype(f32) + moved[0].astype(f32)
                a_recv[0, 0, :, shifted] = both.astype(bf16)

            for side in range(2):
                @tiles(half)
                def _(at):
                    both = transform(own[...], k, side * half + at)
                    both = both + a_recv[side, k, :, pl.ds(at, tile)].astype(f32)
                    extra = n1_recv[1 - side, k, :, pl.ds(at, tile)].astype(f32)
                    rows = [both[:unit], both[unit:]]
                    rows[1 - side] = rows[1 - side] + extra
                    parts = weighted(k, side * half + at, jnp.concatenate(rows, axis=0))
                    add_terms(0, parts)
                    store(k, side * half + at, parts)

        exchange(sums_of(0))
        for u in range(2):
            for side in range(2):
                p_copy(side, side, u).wait_recv()

                @tiles(span, 2)
                def _(at):
                    there = pl.ds(at, tile)
                    k = common + 2 * me + u
                    both = p_recv[side, u, :, there].astype(f32) + m1_send[side, k, :, there].astype(f32)
                    add_terms(1 + side, weighted(k, at, both))

        for side in range(2):
            e_send[side] = sums_of(1 + side)
            e_copy(me, side).start()

        gather()
        shifted_copy(me).wait_send()
        for side in range(2):
            e_copy(me, side).wait_send()
            wait_sent(a_refs, side, kept_copy(me) if side == 0 else None)
            batch_copy(m1_refs, me, side, common + 2 * (1 - me), 2).wait_send()
            batch_copy(m1_refs, me, side, 1, common - 3).wait_send()
            batch_copy(m1_refs, me, side, common - 2, 2).wait_send()
            batch_copy(m1_refs, me, side, common + 2 * me, 1).wait_send()

            @pl.loop(0, tail)
            def _(n):
                tail_copy(me, side, common + 2 * me + 1, n).wait_send()

        for n in range(lifts + 1):
            @pl.when(n == npy - 1 - py)
            def _():
                for c in range(n):
                    up_copy(me, c).wait_send()
                rest_copy(me, 0, n).wait_send()
        rest_copy(me, 1, 0).wait_send()

    @pl.when(outer)
    def _():
        base = me * (3 * unit)
        far = pl.ds(pl.multiple_of(base, unit), unit)
        near = pl.ds(pl.multiple_of(base + unit, unit), 2 * unit)

        @pl.loop(0, steps)
        def _(k):
            loaded(k)
            for side in range(2):
                @tiles(half, 4)
                def _(at):
                    n2_send[side, k, :, pl.ds(at, tile)] = transform(
                        twiddle[far, :], k, side * half + at).astype(bf16)
                if side == 0:
                    meet(k)
                start_batch(n2_refs, side, k)

        @pl.loop(0, steps)
        def _(k):
            @tiles(half)
            def _(at):
                product = transform(twiddle[near, :], k, (1 - me) * half + at)
                for side in range(2):
                    n1_send[side, k, :, pl.ds(at, tile)] = product[side * unit:(side + 1) * unit].astype(bf16)
            for side in range(2):
                start_batch(n1_refs, side, k)
            for side in range(2):
                wait_batch(a_refs, side, k)

            @pl.when((k == 0) & (me == 1))
            def _():
                for side in range(2):
                    shifted_copy(side).wait_recv()
                    forward_copy(side).start()

            @tiles(half)
            def _(at):
                here = pl.ds(at, tile)
                product = transform(twiddle[near, :], k, me * half + at)
                for side in range(2):
                    rows = product[side * unit:(side + 1) * unit]
                    for block in range(SEGMENT_NUMBER):
                        there = slice(block * unit, (block + 1) * unit)
                        came = a_recv[1 - side, k, there, here].astype(f32)
                        total = came + jnp.where(me == block, rows, 0.0)
                        a_send[side, k, there, here] = total.astype(bf16)
            for side in range(2):
                start_batch(a_refs, side, k)

        weights()

        for c in range(lifts):
            @pl.when(comes_up(c) & (me == 0))
            def _():
                for side in range(2):
                    up_copy(side, c).wait_recv()
                    down_copy(side, c).start()

        for u in range(2):
            for side in range(2):
                k = common + 2 * side + u
                if u == 0:
                    batch_copy(m1_refs, 1 - side, 1 - side, k, 2).wait_recv()

                @tiles(span, 2)
                def _(at):
                    there = pl.ds(at, tile)
                    both = transform(own[...], k, at) + m1_recv[1 - side, k, :, there].astype(f32)
                    p_send[side, u, :, there] = both.astype(bf16)
                    pre[side, u, :, there] = both

                p_copy(me, side, u).start()

        learn_of_peers()

        def arrived(k, at):
            there = pl.ds(at, tile)
            both = transform(own[...], k, at)
            return weighted(k, at, both + (
                m1_recv[0, k, :, there].astype(f32) + m1_recv[1, k, :, there].astype(f32)))

        def arrive(k, first, width):
            @tiles(width, 2)
            def _(at):
                at = pl.multiple_of(first + at, tile)
                parts = arrived(k, at)
                add_terms(0, parts)
                store(k, at, parts)

        @pl.loop(0, common)
        def _(k):
            @pl.when(k == 0)
            def _():
                for n in range(lifts + 1):
                    @pl.when((me == 0) & (n == npy - 1 - py))
                    def _():
                        for side in range(2):
                            for c in range(n):
                                down_copy(side, c).wait_recv()
                            rest_copy(side, side, n).wait_recv()

                @pl.when(me == 1)
                def _():
                    for side in range(2):
                        rest_copy(side, side, 0).wait_recv()

            for first, count in ((1, common - 3), (common - 2, 2)):
                @pl.when(k == first)
                def _():
                    for side in range(2):
                        batch_copy(m1_refs, side, side, first, count).wait_recv()

            arrive(k, 0, span)

        sums = sums_of(0)
        for side in range(2):
            e_copy(side, side).wait_recv()
            sums = sums + e_recv[side]
        exchange(sums)

        for side in range(2):
            for refs in (a_refs, n1_refs, n2_refs):
                wait_sent(refs, side)

            @pl.when(me == 1)
            def _():
                forward_copy(side).wait_send()

        for side in range(2):
            for u in range(2):
                p_copy(me, side, u).wait_send()

        for c in range(lifts):
            @pl.when(comes_up(c) & (me == 0))
            def _():
                for side in range(2):
                    down_copy(side, c).wait_send()

        def complete(side, u, at):
            k = common + 2 * side + u
            there = pl.ds(at, tile)
            store(k, at, weighted(
                k, at, pre[side, u, :, there] + m1_recv[side, k, :, there].astype(f32)))

        for side in range(2):
            batch_copy(m1_refs, side, side, common + 2 * side, 1).wait_recv()
            tiles(span, 2)(functools.partial(complete, side, 0))

        @pl.loop(0, tail)
        def _(n):
            @pl.when(n == tail // 2)
            def _():
                gather()

            for side in range(2):
                tail_copy(side, side, common + 2 * side + 1, n).wait_recv()
                for c in range(0, short, tile):
                    complete(side, 1, pl.multiple_of(n * short + c, tile))


def flush_kernel(spectra, gram, spectra_out, gram_out, sems):
    copies = [pltpu.make_async_copy(gram, gram_out, sems.at[0])]
    for f in range(spectra.shape[0]):
        copies.append(pltpu.make_async_copy(spectra.at[f], spectra_out.at[f], sems.at[f + 1]))
    for copy in copies:
        copy.start()
    for copy in copies:
        copy.wait()


def kernel_on_device(snapshots, quad_weights, spectral_indices):
    record, variables, points = snapshots.shape
    groups = lax.axis_size("ta")
    npx, npy = lax.axis_size("px"), lax.axis_size("py")
    modes = spectral_indices.shape[0] // groups
    unit = 2 * modes
    pieces, tail = 2, 4
    span = points // pieces
    half = span // 2
    tile = math.gcd(512, span // tail)
    steps = variables * pieces
    lift = min(256, span // npy)
    lifts = npy - 1
    shift = min(384, half // 2)
    bf16, f32 = jnp.bfloat16, jnp.float32
    peers = npx * npy - 1
    dma = pltpu.SemaphoreType.DMA
    hbm = pl.BlockSpec(memory_space=pltpu.HBM)
    vmem = pl.BlockSpec(memory_space=pltpu.VMEM)
    spectra, gram = pl.pallas_call(
        functools.partial(
            window_kernel, pieces, tail, tile, 1.0 / (points * npx * npy * variables)),
        out_shape=(
            jax.ShapeDtypeStruct((modes, SEGMENT_NUMBER, variables, 2, points), f32),
            jax.ShapeDtypeStruct((SEGMENT_NUMBER * SEGMENT_NUMBER * 2, modes), f32),
        ),
        in_specs=[hbm, hbm, hbm],
        out_specs=(vmem, vmem),
        scratch_shapes=[
            pltpu.VMEM((variables, record, points), bf16),
            pltpu.SMEM(spectral_indices.shape, jnp.int32),
            pltpu.VMEM((1, points), f32),
            pltpu.VMEM((3 * SEGMENT_NUMBER * unit, record), bf16),
            pltpu.VMEM((SEGMENT_NUMBER * unit, record), bf16),
            pltpu.VMEM((1, points), f32),
            pltpu.VMEM((2, steps, SEGMENT_NUMBER * unit, half), bf16),
            pltpu.VMEM((2, steps, SEGMENT_NUMBER * unit, half), bf16),
            pltpu.VMEM((2, steps, unit, half), bf16),
            pltpu.VMEM((2, steps, unit, half), bf16),
            pltpu.VMEM((2, steps, unit, half), bf16),
            pltpu.VMEM((2, steps, unit, half), bf16),
            pltpu.VMEM((2, steps, SEGMENT_NUMBER * unit, span), bf16),
            pltpu.VMEM((2, steps, SEGMENT_NUMBER * unit, span), bf16),
            pltpu.VMEM((lifts, 2, SEGMENT_NUMBER * unit, lift), bf16),
            pltpu.VMEM((2, SEGMENT_NUMBER * unit, shift), bf16),
            pltpu.VMEM((2, 2, SEGMENT_NUMBER * unit, span), bf16),
            pltpu.VMEM((2, 2, SEGMENT_NUMBER * unit, span), bf16),
            pltpu.VMEM((2, 2, SEGMENT_NUMBER * unit, span), f32),
            pltpu.VMEM((2, modes, 128), f32),
            pltpu.VMEM((2, modes, 128), f32),
            pltpu.VMEM((3, 4, modes, 128), f32),
            pltpu.VMEM((modes, 128), f32),
            pltpu.VMEM((peers, modes, 128), f32),
            dma((steps,)), dma, dma,
            dma((2, steps)), dma((2, steps)), dma((2, steps)), dma((2, steps)),
            dma((2, steps)), dma((2, steps)),
            dma((2, steps + tail)), dma((2, steps + tail)),
            dma((2,)), dma((2,)), dma((lifts, 2)), dma((lifts, 2)), dma((lifts,)), dma((lifts, 2)),
            dma((2, 2)), dma((2, 2)), dma((2,)), dma((2,)),
            dma((peers,)), dma((peers,)),
            pltpu.SemaphoreType.REGULAR((3,)),
        ],
        compiler_params=pltpu.CompilerParams(
            collective_id=0, has_side_effects=True, vmem_limit_bytes=44 * 1024 * 1024),
        name="window_transform",
    )(*(
        pltpu.with_memory_space_constraint(a, pltpu.HBM)
        for a in (snapshots.transpose(1, 0, 2), quad_weights.reshape(1, points), spectral_indices)
    ))
    spectra, gram = pl.pallas_call(
        flush_kernel,
        out_shape=(
            jax.ShapeDtypeStruct(spectra.shape, f32), jax.ShapeDtypeStruct(gram.shape, f32)),
        in_specs=[vmem, vmem],
        out_specs=(hbm, hbm),
        scratch_shapes=[dma((modes + 1,))],
        compiler_params=pltpu.CompilerParams(vmem_limit_bytes=1024 * 1024),
        name="flush",
    )(*(pltpu.with_memory_space_constraint(a, pltpu.VMEM) for a in (spectra, gram)))
    gram = gram.reshape(SEGMENT_NUMBER, SEGMENT_NUMBER, 2, modes)
    return spectra.transpose(0, 1, 3, 2, 4), gram.transpose(3, 0, 1, 2)


def solution(mesh):
    square = mesh.shape["ta"] == 4
    return jax.shard_map(
        kernel_on_device if square else plain_on_device,
        mesh=mesh,
        in_specs=(P("ta", None, ("px", "py")), P(("px", "py")), P()),
        out_specs=(P("ta", None, None, None, ("px", "py")), P("ta", None, None, None)),
        check_vma=False,
    )
```

```python
import functools
import math

import jax
import jax.numpy as jnp
from jax import lax
from jax.experimental import pallas as pl
from jax.experimental.pallas import tpu as pltpu
from jax.sharding import PartitionSpec as P

VARS = 5
BLK = 256
HOP = 128
SEGMENT_NUMBER = 2
RETAINED_MODES = 32

MESH = pl.DeviceIdType.MESH


def make_rotation_multipliers(spectral_indices, temporal_locations):
    segment_beginnings = jnp.arange(SEGMENT_NUMBER, dtype=jnp.int32) * HOP
    segment_shifts = temporal_locations[None, :] - segment_beginnings[:, None]
    inside = (segment_shifts >= 0) & (segment_shifts < BLK)
    window = 0.5 - 0.5 * jnp.cos(2.0 * math.pi * segment_shifts.astype(jnp.float32) / BLK)
    window = jnp.where(inside, window, jnp.float32(0.0)) / jnp.sqrt(jnp.float32(3.0 * BLK / 8.0))
    phases = jnp.mod(spectral_indices[:, None, None] * segment_shifts[None, :, :], BLK)
    angles = 2.0 * math.pi * phases.astype(jnp.float32) / BLK
    real_part = jnp.cos(angles) * window[None]
    imag_part = -jnp.sin(angles) * window[None]
    gathered_segments = jnp.stack([real_part, imag_part], axis=2)
    return gathered_segments.reshape(
        RETAINED_MODES * SEGMENT_NUMBER * 2, temporal_locations.shape[0]
    ).astype(jnp.bfloat16)


def gram_terms(spectra):
    flat = spectra.reshape(spectra.shape[0], 2 * SEGMENT_NUMBER, -1)
    inner = jnp.einsum("fam,fbm->fab", flat, flat, precision=lax.Precision.HIGHEST)
    inner = inner.reshape(spectra.shape[0], SEGMENT_NUMBER, 2, SEGMENT_NUMBER, 2)
    real_part = inner[:, :, 0, :, 0] + inner[:, :, 1, :, 1]
    imag_part = inner[:, :, 0, :, 1] - inner[:, :, 1, :, 0]
    return jnp.stack([real_part, imag_part], axis=-1)


def plain_on_device(snapshots, quad_weights, spectral_indices):
    record_length = snapshots.shape[0]
    point_count = snapshots.shape[2]
    groups = lax.axis_size("ta")
    temporal_locations = lax.axis_index("ta") * record_length + jnp.arange(
        record_length, dtype=jnp.int32
    )
    rotation_multipliers = make_rotation_multipliers(spectral_indices, temporal_locations)
    flat_snapshots = snapshots.reshape(record_length, VARS * point_count)
    raw = lax.psum_scatter(
        jnp.dot(rotation_multipliers, flat_snapshots, preferred_element_type=jnp.float32),
        "ta",
        scatter_dimension=0,
        tiled=True,
    )
    raw = raw.reshape(RETAINED_MODES // groups, SEGMENT_NUMBER, 2, VARS, point_count)
    spectra = raw * jnp.sqrt(quad_weights)
    summed = lax.psum(gram_terms(spectra), ("px", "py"))
    total_points = point_count * lax.axis_size("px") * lax.axis_size("py")
    gram = summed / jnp.float32(total_points * VARS)
    return (spectra, gram)


def sine_of_turn(m):
    quarter = BLK // 4
    r = jnp.bitwise_and(m + quarter, BLK - 1) - quarter
    r = jnp.where(r > quarter, BLK // 2 - r, r)
    x = r.astype(jnp.float32) * (2.0 * math.pi / BLK)
    y = x * x
    total = jnp.full_like(x, -1.0 / math.factorial(11))
    for n in (9, 7, 5, 3, 1):
        total = total * y + (1.0 if n % 4 == 1 else -1.0) / math.factorial(n)
    return total * x


def window_kernel(
    pieces, tail, tile, gram_scale,
    snap_hbm, weight_hbm, index_hbm, out_ref, gram_ref,
    snap, index_ref, weight_ref, twiddle, own, root,
    a_send, a_recv, n1_send, n1_recv, n2_send, n2_recv, m1_send, m1_recv,
    relay, moved, p_send, p_recv, pre, e_send, e_recv, acc, gram_send, gram_recv,
    load_sem, index_sem, weight_sem,
    a_ssem, a_rsem, n1_ssem, n1_rsem, n2_ssem, n2_rsem, m1_ssem, m1_rsem,
    moved_ssem, moved_rsem, relay_ssem, relay_rsem, lift_ssem, lift_rsem,
    p_ssem, p_rsem, e_ssem, e_rsem, gram_ssem, gram_rsem, ready_sem,
):
    px, py, ta = lax.axis_index("px"), lax.axis_index("py"), lax.axis_index("ta")
    npx, npy = lax.axis_size("px"), lax.axis_size("py")
    variables, record, points = snap_hbm.shape
    modes = out_ref.shape[0]
    unit = 2 * modes
    steps = variables * pieces
    span = points // pieces
    half = span // 2
    short = span // tail
    common = steps - 4
    batch = 3 if steps % 3 == 1 else 1
    lifts, lift = relay.shape[0], relay.shape[3]
    shift = moved.shape[2]
    kept, shifted = pl.ds(0, half - shift), pl.ds(half - shift, shift)
    f32, bf16 = jnp.float32, jnp.bfloat16

    inner = (ta == 1) | (ta == 2)
    outer = jnp.logical_not(inner)
    me = jnp.where(inner, ta - 1, ta // 3)
    sides = (jnp.where(inner, 0, 1), jnp.where(inner, 3, 2))

    moves = px == 0

    @pl.when(outer & (me == 0) & moves)
    def _():
        a_recv[:, 0, :, shifted] = jnp.zeros((2, SEGMENT_NUMBER * unit, shift), bf16)

    def load(k):
        there = pl.ds(pl.multiple_of(lax.rem(k, pieces) * span, span), span)
        return pltpu.make_async_copy(
            snap_hbm.at[k // pieces, :, there], snap.at[k // pieces, :, there], load_sem.at[k])

    index_copy = pltpu.make_async_copy(index_hbm, index_ref, index_sem)
    weight_copy = pltpu.make_async_copy(weight_hbm, weight_ref, weight_sem)
    index_copy.start()
    load(0).start()

    peers = [
        (i, j, lax.rem(px + i, npx), lax.rem(py + j, npy))
        for i in range(npx) for j in range(npy) if i + j > 0
    ]
    barrier = pltpu.get_barrier_semaphore()
    for side in sides:
        pl.semaphore_signal(barrier, inc=1, device_id=(px, py, side), device_id_type=MESH)
    for i in range(1, npx):
        pl.semaphore_signal(barrier, inc=1, device_id=(lax.rem(px + i, npx), py, ta), device_id_type=MESH)
    below, above = py > 0, py < npy - 1
    for there, step in ((below, -1), (above, 1)):
        @pl.when(there)
        def _():
            pl.semaphore_signal(barrier, inc=1, device_id=(px, py + step, ta), device_id_type=MESH)
    greeted = len(sides) + npx - 1 + jnp.where(below, 1, 0) + jnp.where(above, 1, 0)

    sublane = lax.broadcasted_iota(jnp.int32, (modes, record), 0)
    moment = lax.broadcasted_iota(jnp.int32, (modes, record), 1) + ta * record
    shifts, windows = [], []
    for block in range(SEGMENT_NUMBER):
        shift = moment - block * HOP
        inside = (shift >= 0) & (shift < BLK)
        hann = 0.5 - 0.5 * sine_of_turn(shift + BLK // 4)
        shifts.append(shift)
        windows.append(jnp.where(inside, hann, 0.0) / math.sqrt(3.0 * BLK / 8.0))
    index_copy.wait()
    for place, owner in enumerate((3 - ta, sides[0], sides[1], ta)):
        bins = jnp.zeros((modes, record), jnp.int32)
        for f in range(modes):
            bins = jnp.where(sublane == f, index_ref[owner * modes + f], bins)
        for block in range(SEGMENT_NUMBER):
            shift, hann = shifts[block], windows[block]
            phase = bins * shift
            rows = jnp.concatenate(
                [sine_of_turn(phase + BLK // 4) * hann, -sine_of_turn(phase) * hann], axis=0)
            if place < 3:
                at = jnp.where(inner, place * SEGMENT_NUMBER + block, block * 3 + place)
                twiddle[pl.ds(pl.multiple_of(at * unit, unit), unit), :] = rows.astype(bf16)
            else:
                own[block * unit:(block + 1) * unit, :] = rows.astype(bf16)
    acc[...] = jnp.zeros_like(acc)

    a_refs = (a_send, a_recv, a_ssem, a_rsem)
    n1_refs = (n1_send, n1_recv, n1_ssem, n1_rsem)
    n2_refs = (n2_send, n2_recv, n2_ssem, n2_rsem)

    def batch_copy(refs, here, side, first, count):
        send, recv, ssem, rsem = refs
        units = pl.ds(first, count)
        return pltpu.make_async_remote_copy(
            src_ref=send.at[side, units], dst_ref=recv.at[here, units],
            send_sem=ssem.at[side, first], recv_sem=rsem.at[here, first],
            device_id=(px, py, sides[side]), device_id_type=MESH,
        )

    m1_refs = (m1_send, m1_recv, m1_ssem, m1_rsem)

    def kept_copy(here):
        return pltpu.make_async_remote_copy(
            src_ref=a_send.at[0, 0, :, kept], dst_ref=a_recv.at[here, 0, :, kept],
            send_sem=a_ssem.at[0, 0], recv_sem=a_rsem.at[here, 0],
            device_id=(px, py, sides[0]), device_id_type=MESH,
        )

    def shifted_copy(here):
        return pltpu.make_async_remote_copy(
            src_ref=a_send.at[0, 0, :, shifted], dst_ref=moved.at[here],
            send_sem=moved_ssem.at[0], recv_sem=moved_rsem.at[here],
            device_id=(px, py, sides[1]), device_id_type=MESH,
        )

    def forward_copy(here):
        return pltpu.make_async_remote_copy(
            src_ref=moved.at[here], dst_ref=moved.at[0],
            send_sem=moved_ssem.at[here], recv_sem=moved_rsem.at[0],
            device_id=(px, py, sides[1 - here]), device_id_type=MESH,
        )

    def start_batch(refs, side, k):
        @pl.when(k == 0)
        def _():
            if refs is a_refs and side == 0:
                @pl.when(inner & moves)
                def _():
                    kept_copy(me).start()
                    shifted_copy(me).start()

                @pl.when(jnp.logical_not(inner & moves))
                def _():
                    batch_copy(refs, me, side, 0, 1).start()
            else:
                batch_copy(refs, me, side, 0, 1).start()

        @pl.when((k > 0) & (lax.rem(k, batch) == 0))
        def _():
            batch_copy(refs, me, side, k + 1 - batch, batch).start()

    def wait_batch(refs, side, k):
        @pl.when(k == 0)
        def _():
            if refs is a_refs:
                relays = outer & (me == 0) & moves

                @pl.when(relays)
                def _():
                    kept_copy(side).wait_recv()

                @pl.when(jnp.logical_not(relays))
                def _():
                    batch_copy(refs, side, side, 0, 1).wait_recv()
            else:
                batch_copy(refs, side, side, 0, 1).wait_recv()

        @pl.when((k > 0) & (lax.rem(k - 1, batch) == 0))
        def _():
            batch_copy(refs, side, side, k, batch).wait_recv()

    def wait_sent(refs, side):
        if refs is a_refs and side == 0:
            @pl.when(inner & moves)
            def _():
                kept_copy(me).wait_send()
                shifted_copy(me).wait_send()

            @pl.when(jnp.logical_not(inner & moves))
            def _():
                batch_copy(refs, me, side, 0, 1).wait_send()
        else:
            batch_copy(refs, me, side, 0, 1).wait_send()

        @pl.loop(0, (steps - 1) // batch)
        def _(n):
            batch_copy(refs, me, side, 1 + n * batch, batch).wait_send()

    def tail_copy(here, side, k, n):
        columns = pl.ds(pl.multiple_of(n * short, short), short)
        return pltpu.make_async_remote_copy(
            src_ref=m1_send.at[side, k, :, columns], dst_ref=m1_recv.at[here, k, :, columns],
            send_sem=m1_ssem.at[side, steps + n], recv_sem=m1_rsem.at[here, steps + n],
            device_id=(px, py, sides[side]), device_id_type=MESH,
        )

    def up_copy(here, c):
        return pltpu.make_async_remote_copy(
            src_ref=m1_send.at[0, 0, :, pl.ds(c * lift, lift)], dst_ref=relay.at[c, here],
            send_sem=lift_ssem.at[c], recv_sem=relay_rsem.at[c, here],
            device_id=(px, py + 1, sides[0]), device_id_type=MESH,
        )

    def down_copy(side, c):
        return pltpu.make_async_remote_copy(
            src_ref=relay.at[c, side], dst_ref=m1_recv.at[side, 0, :, pl.ds(c * lift, lift)],
            send_sem=relay_ssem.at[c, side], recv_sem=lift_rsem.at[c, side],
            device_id=(px, py - 1, ta), device_id_type=MESH,
        )

    def comes_up(c):
        return (py > 0) & (c < npy - py)

    def rest_copy(here, side, n):
        columns = pl.ds(n * lift, span - n * lift)
        return pltpu.make_async_remote_copy(
            src_ref=m1_send.at[side, 0, :, columns], dst_ref=m1_recv.at[here, 0, :, columns],
            send_sem=m1_ssem.at[side, 0], recv_sem=m1_rsem.at[here, 0],
            device_id=(px, py, sides[side]), device_id_type=MESH,
        )

    def p_copy(here, side, u):
        return pltpu.make_async_remote_copy(
            src_ref=p_send.at[side, u], dst_ref=p_recv.at[here, u],
            send_sem=p_ssem.at[side, u], recv_sem=p_rsem.at[here, u],
            device_id=(px, py, sides[side]), device_id_type=MESH,
        )

    beside = jnp.bitwise_xor(py, 1) if npy % 2 == 0 else py

    def e_copy(here, side):
        return pltpu.make_async_remote_copy(
            src_ref=e_send.at[side], dst_ref=e_recv.at[here],
            send_sem=e_ssem.at[side], recv_sem=e_rsem.at[here],
            device_id=(px, beside, sides[side]), device_id_type=MESH,
        )

    def columns(k, at):
        return pl.ds(pl.multiple_of(lax.rem(k, pieces) * span + at, 128), tile)

    def transform(rows, k, at):
        return jnp.dot(rows, snap[k // pieces, :, columns(k, at)], preferred_element_type=f32)

    def loaded(k):
        load(k).wait()

        @pl.when(k == 0)
        def _():
            for later in range(1, steps):
                load(later).start()
            weight_copy.start()

    def tiles(width, unroll=1):
        def run(body):
            @pl.loop(0, width // tile, unroll=unroll)
            def _(i):
                body(pl.multiple_of(i * tile, tile))
        return run

    def meet(k):
        @pl.when(k == 0)
        def _():
            pl.semaphore_wait(barrier, greeted)

    def learn_of_peers():
        for n, (back, forth, step) in enumerate(((below, above, 1), (above, below, -1))):
            @pl.when(back)
            def _():
                pl.semaphore_wait(ready_sem.at[n], 1)

            @pl.when(forth)
            def _():
                pl.semaphore_signal(
                    ready_sem.at[n], inc=1, device_id=(px, py + step, ta), device_id_type=MESH)

        for i in range(1, npx):
            pl.semaphore_signal(
                ready_sem.at[2], inc=1, device_id=(lax.rem(px + i, npx), py, ta), device_id_type=MESH)
        if npx > 1:
            pl.semaphore_wait(ready_sem.at[2], npx - 1)

    def weighted(k, at, both):
        weight = root[:, columns(k, at)]
        return [
            (both[b * unit:b * unit + modes] * weight, both[b * unit + modes:(b + 1) * unit] * weight)
            for b in range(SEGMENT_NUMBER)]

    def add_terms(place, parts):
        (r0, i0), (r1, i1) = parts
        terms = (r0 * r0 + i0 * i0, r1 * r1 + i1 * i1, r0 * r1 + i0 * i1, r0 * i1 - i0 * r1)
        for n, term in enumerate(terms):
            lanes = [term[:, c:c + 128] for c in range(0, tile, 128)]
            acc[place, n] += functools.reduce(jnp.add, lanes)

    def store(k, at, parts):
        here = columns(k, at)
        for block, pair in enumerate(parts):
            for c in range(2):
                out_ref[:, block, k // pieces, c, here] = pair[c]

    def sums_of(place):
        lane = lax.broadcasted_iota(jnp.int32, gram_send.shape, 1)
        sums = jnp.zeros(gram_send.shape, f32)
        for n in range(4):
            sums = jnp.where(lane == n, jnp.sum(acc[place, n], axis=1, keepdims=True), sums)
        return sums

    def gram_copy(n):
        i, j, x, y = peers[n]
        return pltpu.make_async_remote_copy(
            src_ref=gram_send, dst_ref=gram_recv.at[n],
            send_sem=gram_ssem.at[n], recv_sem=gram_rsem.at[n],
            device_id=(x, y, ta), device_id_type=MESH,
        )

    def exchange(sums):
        gram_send[...] = sums
        for n in range(len(peers)):
            gram_copy(n).start()

    def weights():
        weight_copy.wait()
        root[...] = jnp.sqrt(weight_ref[...])

    def gather():
        total = gram_send[...]
        for n in range(len(peers)):
            gram_copy(n).wait()
            total = total + gram_recv[n]
        row = lax.broadcasted_iota(jnp.int32, (8, 128), 0)
        lane = lax.broadcasted_iota(jnp.int32, (8, 128), 1)
        pick = jnp.zeros((8, 128), f32)
        for r, n, sign in ((0, 0, 1.0), (2, 2, 1.0), (3, 3, 1.0), (4, 2, 1.0), (5, 3, -1.0), (6, 1, 1.0)):
            pick = jnp.where((row == r) & (lane == n), sign, pick)
        gram_ref[...] = gram_scale * lax.dot_general(
            pick, total, (((1,), (1,)), ((), ())),
            precision=lax.Precision.HIGHEST, preferred_element_type=f32,
        )

    @pl.when(inner)
    def _():
        @pl.loop(0, steps)
        def _(k):
            loaded(k)
            for side in range(2):
                @tiles(half, 4)
                def _(at):
                    a_send[side, k, :, pl.ds(at, tile)] = transform(
                        twiddle[0:2 * unit, :], k, side * half + at).astype(bf16)
                if side == 0:
                    meet(k)

                start_batch(a_refs, side, k)

        @pl.loop(0, steps)
        def _(k):
            for side in range(2):
                wait_batch(n2_refs, side, k)

        @pl.loop(0, steps)
        def _(j):
            k = jnp.where(
                j < 2, common + 2 * (1 - me) + j,
                jnp.where(j < common + 2, j - 2, 2 * me + j - 2))
            for dependent in range(2):
                first = half * (me if dependent else 1 - me)
                @tiles(half)
                def _(at):
                    product = transform(twiddle[2 * unit:6 * unit, :], k, first + at)
                    there = pl.ds(pl.multiple_of(first + at, 128), tile)
                    for side in range(2):
                        for block in range(SEGMENT_NUMBER):
                            r = (side * SEGMENT_NUMBER + block) * unit
                            rows = product[r:r + unit]
                            if dependent and block != side:
                                rows = rows + n2_recv[block, k, :, pl.ds(at, tile)].astype(f32)
                            m1_send[side, k, block * unit:(block + 1) * unit, there] = rows.astype(bf16)

            @pl.when(j == 1)
            def _():
                for side in range(2):
                    batch_copy(m1_refs, me, side, k - 1, 2).start()

            @pl.when(k == 0)
            def _():
                for n in range(lifts + 1):
                    @pl.when(n == npy - 1 - py)
                    def _():
                        for c in range(n):
                            up_copy(me, c).start()
                        rest_copy(me, 0, n).start()
                rest_copy(me, 1, 0).start()

            @pl.when(k == common - 3)
            def _():
                for side in range(2):
                    batch_copy(m1_refs, me, side, 1, common - 3).start()

            @pl.when(k == common - 1)
            def _():
                for side in range(2):
                    batch_copy(m1_refs, me, side, common - 2, 2).start()

            @pl.when(j == steps - 2)
            def _():
                for side in range(2):
                    batch_copy(m1_refs, me, side, k, 1).start()

            @pl.when(j == steps - 1)
            def _():
                for n in range(tail):
                    for side in range(2):
                        tail_copy(me, side, k, n).start()

        weights()
        learn_of_peers()

        @pl.loop(0, steps)
        def _(k):
            for side in range(2):
                wait_batch(a_refs, side, k)
                wait_batch(n1_refs, side, k)

            @pl.when((k == 0) & moves)
            def _():
                forward_copy(0).wait_recv()
                both = a_recv[0, 0, :, shifted].astype(f32) + moved[0].astype(f32)
                a_recv[0, 0, :, shifted] = both.astype(bf16)

            for side in range(2):
                @tiles(half)
                def _(at):
                    both = transform(own[...], k, side * half + at)
                    both = both + a_recv[side, k, :, pl.ds(at, tile)].astype(f32)
                    extra = n1_recv[1 - side, k, :, pl.ds(at, tile)].astype(f32)
                    rows = [both[:unit], both[unit:]]
                    rows[1 - side] = rows[1 - side] + extra
                    parts = weighted(k, side * half + at, jnp.concatenate(rows, axis=0))
                    add_terms(0, parts)
                    store(k, side * half + at, parts)

        exchange(sums_of(0))
        for u in range(2):
            for side in range(2):
                p_copy(side, side, u).wait_recv()

                @tiles(span, 2)
                def _(at):
                    there = pl.ds(at, tile)
                    k = common + 2 * me + u
                    both = p_recv[side, u, :, there].astype(f32) + m1_send[side, k, :, there].astype(f32)
                    add_terms(1 + side, weighted(k, at, both))

        for side in range(2):
            e_send[side] = sums_of(1 + side)
            e_copy(me, side).start()

        gather()
        for side in range(2):
            e_copy(me, side).wait_send()
            wait_sent(a_refs, side)
            batch_copy(m1_refs, me, side, common + 2 * (1 - me), 2).wait_send()
            batch_copy(m1_refs, me, side, 1, common - 3).wait_send()
            batch_copy(m1_refs, me, side, common - 2, 2).wait_send()
            batch_copy(m1_refs, me, side, common + 2 * me, 1).wait_send()

            @pl.loop(0, tail)
            def _(n):
                tail_copy(me, side, common + 2 * me + 1, n).wait_send()

        for n in range(lifts + 1):
            @pl.when(n == npy - 1 - py)
            def _():
                for c in range(n):
                    up_copy(me, c).wait_send()
                rest_copy(me, 0, n).wait_send()
        rest_copy(me, 1, 0).wait_send()

    @pl.when(outer)
    def _():
        base = me * (3 * unit)
        far = pl.ds(pl.multiple_of(base, unit), unit)
        near = pl.ds(pl.multiple_of(base + unit, unit), 2 * unit)

        @pl.loop(0, steps)
        def _(k):
            loaded(k)
            for side in range(2):
                @tiles(half, 4)
                def _(at):
                    n2_send[side, k, :, pl.ds(at, tile)] = transform(
                        twiddle[far, :], k, side * half + at).astype(bf16)
                if side == 0:
                    meet(k)
                start_batch(n2_refs, side, k)

        @pl.loop(0, steps)
        def _(k):
            @tiles(half)
            def _(at):
                product = transform(twiddle[near, :], k, (1 - me) * half + at)
                for side in range(2):
                    n1_send[side, k, :, pl.ds(at, tile)] = product[side * unit:(side + 1) * unit].astype(bf16)
            for side in range(2):
                start_batch(n1_refs, side, k)
            for side in range(2):
                wait_batch(a_refs, side, k)

            @pl.when((k == 0) & (me == 1) & moves)
            def _():
                for side in range(2):
                    shifted_copy(side).wait_recv()
                    forward_copy(side).start()

            @tiles(half)
            def _(at):
                here = pl.ds(at, tile)
                product = transform(twiddle[near, :], k, me * half + at)
                for side in range(2):
                    rows = product[side * unit:(side + 1) * unit]
                    for block in range(SEGMENT_NUMBER):
                        there = slice(block * unit, (block + 1) * unit)
                        came = a_recv[1 - side, k, there, here].astype(f32)
                        total = came + jnp.where(me == block, rows, 0.0)
                        a_send[side, k, there, here] = total.astype(bf16)
            for side in range(2):
                start_batch(a_refs, side, k)

        weights()

        for c in range(lifts):
            @pl.when(comes_up(c) & (me == 0))
            def _():
                for side in range(2):
                    up_copy(side, c).wait_recv()
                    down_copy(side, c).start()

        for u in range(2):
            for side in range(2):
                k = common + 2 * side + u
                if u == 0:
                    batch_copy(m1_refs, 1 - side, 1 - side, k, 2).wait_recv()

                @tiles(span, 2)
                def _(at):
                    there = pl.ds(at, tile)
                    both = transform(own[...], k, at) + m1_recv[1 - side, k, :, there].astype(f32)
                    p_send[side, u, :, there] = both.astype(bf16)
                    pre[side, u, :, there] = both

                p_copy(me, side, u).start()

        learn_of_peers()

        def arrived(k, at):
            there = pl.ds(at, tile)
            both = transform(own[...], k, at)
            return weighted(k, at, both + (
                m1_recv[0, k, :, there].astype(f32) + m1_recv[1, k, :, there].astype(f32)))

        def arrive(k, first, width):
            @tiles(width, 2)
            def _(at):
                at = pl.multiple_of(first + at, tile)
                parts = arrived(k, at)
                add_terms(0, parts)
                store(k, at, parts)

        @pl.loop(0, common)
        def _(k):
            @pl.when(k == 0)
            def _():
                for n in range(lifts + 1):
                    @pl.when((me == 0) & (n == npy - 1 - py))
                    def _():
                        for side in range(2):
                            for c in range(n):
                                down_copy(side, c).wait_recv()
                            rest_copy(side, side, n).wait_recv()

                @pl.when(me == 1)
                def _():
                    for side in range(2):
                        rest_copy(side, side, 0).wait_recv()

            for first, count in ((1, common - 3), (common - 2, 2)):
                @pl.when(k == first)
                def _():
                    for side in range(2):
                        batch_copy(m1_refs, side, side, first, count).wait_recv()

            arrive(k, 0, span)

        sums = sums_of(0)
        for side in range(2):
            e_copy(side, side).wait_recv()
            sums = sums + e_recv[side]
        exchange(sums)

        for side in range(2):
            for refs in (a_refs, n1_refs, n2_refs):
                wait_sent(refs, side)

            @pl.when((me == 1) & moves)
            def _():
                forward_copy(side).wait_send()

        for side in range(2):
            for u in range(2):
                p_copy(me, side, u).wait_send()

        for c in range(lifts):
            @pl.when(comes_up(c) & (me == 0))
            def _():
                for side in range(2):
                    down_copy(side, c).wait_send()

        def complete(side, u, at):
            k = common + 2 * side + u
            there = pl.ds(at, tile)
            store(k, at, weighted(
                k, at, pre[side, u, :, there] + m1_recv[side, k, :, there].astype(f32)))

        for side in range(2):
            batch_copy(m1_refs, side, side, common + 2 * side, 1).wait_recv()
            tiles(span, 2)(functools.partial(complete, side, 0))

        @pl.loop(0, tail)
        def _(n):
            @pl.when(n == tail // 2)
            def _():
                gather()

            for side in range(2):
                tail_copy(side, side, common + 2 * side + 1, n).wait_recv()
                for c in range(0, short, tile):
                    complete(side, 1, pl.multiple_of(n * short + c, tile))


def flush_kernel(spectra, gram, spectra_out, gram_out, sems):
    copies = [pltpu.make_async_copy(gram, gram_out, sems.at[0])]
    for f in range(spectra.shape[0]):
        copies.append(pltpu.make_async_copy(spectra.at[f], spectra_out.at[f], sems.at[f + 1]))
    for copy in copies:
        copy.start()
    for copy in copies:
        copy.wait()


def kernel_on_device(snapshots, quad_weights, spectral_indices):
    record, variables, points = snapshots.shape
    groups = lax.axis_size("ta")
    npx, npy = lax.axis_size("px"), lax.axis_size("py")
    modes = spectral_indices.shape[0] // groups
    unit = 2 * modes
    pieces, tail = 2, 4
    span = points // pieces
    half = span // 2
    tile = math.gcd(512, span // tail)
    steps = variables * pieces
    lift = min(256, span // npy)
    lifts = npy - 1
    shift = min(768, half // 2)
    bf16, f32 = jnp.bfloat16, jnp.float32
    peers = npx * npy - 1
    dma = pltpu.SemaphoreType.DMA
    hbm = pl.BlockSpec(memory_space=pltpu.HBM)
    vmem = pl.BlockSpec(memory_space=pltpu.VMEM)
    spectra, gram = pl.pallas_call(
        functools.partial(
            window_kernel, pieces, tail, tile, 1.0 / (points * npx * npy * variables)),
        out_shape=(
            jax.ShapeDtypeStruct((modes, SEGMENT_NUMBER, variables, 2, points), f32),
            jax.ShapeDtypeStruct((SEGMENT_NUMBER * SEGMENT_NUMBER * 2, modes), f32),
        ),
        in_specs=[hbm, hbm, hbm],
        out_specs=(vmem, vmem),
        scratch_shapes=[
            pltpu.VMEM((variables, record, points), bf16),
            pltpu.SMEM(spectral_indices.shape, jnp.int32),
            pltpu.VMEM((1, points), f32),
            pltpu.VMEM((3 * SEGMENT_NUMBER * unit, record), bf16),
            pltpu.VMEM((SEGMENT_NUMBER * unit, record), bf16),
            pltpu.VMEM((1, points), f32),
            pltpu.VMEM((2, steps, SEGMENT_NUMBER * unit, half), bf16),
            pltpu.VMEM((2, steps, SEGMENT_NUMBER * unit, half), bf16),
            pltpu.VMEM((2, steps, unit, half), bf16),
            pltpu.VMEM((2, steps, unit, half), bf16),
            pltpu.VMEM((2, steps, unit, half), bf16),
            pltpu.VMEM((2, steps, unit, half), bf16),
            pltpu.VMEM((2, steps, SEGMENT_NUMBER * unit, span), bf16),
            pltpu.VMEM((2, steps, SEGMENT_NUMBER * unit, span), bf16),
            pltpu.VMEM((lifts, 2, SEGMENT_NUMBER * unit, lift), bf16),
            pltpu.VMEM((2, SEGMENT_NUMBER * unit, shift), bf16),
            pltpu.VMEM((2, 2, SEGMENT_NUMBER * unit, span), bf16),
            pltpu.VMEM((2, 2, SEGMENT_NUMBER * unit, span), bf16),
            pltpu.VMEM((2, 2, SEGMENT_NUMBER * unit, span), f32),
            pltpu.VMEM((2, modes, 128), f32),
            pltpu.VMEM((2, modes, 128), f32),
            pltpu.VMEM((3, 4, modes, 128), f32),
            pltpu.VMEM((modes, 128), f32),
            pltpu.VMEM((peers, modes, 128), f32),
            dma((steps,)), dma, dma,
            dma((2, steps)), dma((2, steps)), dma((2, steps)), dma((2, steps)),
            dma((2, steps)), dma((2, steps)),
            dma((2, steps + tail)), dma((2, steps + tail)),
            dma((2,)), dma((2,)), dma((lifts, 2)), dma((lifts, 2)), dma((lifts,)), dma((lifts, 2)),
            dma((2, 2)), dma((2, 2)), dma((2,)), dma((2,)),
            dma((peers,)), dma((peers,)),
            pltpu.SemaphoreType.REGULAR((3,)),
        ],
        compiler_params=pltpu.CompilerParams(
            collective_id=0, has_side_effects=True, vmem_limit_bytes=44 * 1024 * 1024),
        name="window_transform",
    )(*(
        pltpu.with_memory_space_constraint(a, pltpu.HBM)
        for a in (snapshots.transpose(1, 0, 2), quad_weights.reshape(1, points), spectral_indices)
    ))
    spectra, gram = pl.pallas_call(
        flush_kernel,
        out_shape=(
            jax.ShapeDtypeStruct(spectra.shape, f32), jax.ShapeDtypeStruct(gram.shape, f32)),
        in_specs=[vmem, vmem],
        out_specs=(hbm, hbm),
        scratch_shapes=[dma((modes + 1,))],
        compiler_params=pltpu.CompilerParams(vmem_limit_bytes=1024 * 1024),
        name="flush",
    )(*(pltpu.with_memory_space_constraint(a, pltpu.VMEM) for a in (spectra, gram)))
    gram = gram.reshape(SEGMENT_NUMBER, SEGMENT_NUMBER, 2, modes)
    return spectra.transpose(0, 1, 3, 2, 4), gram.transpose(3, 0, 1, 2)


def solution(mesh):
    square = mesh.shape["ta"] == 4
    return jax.shard_map(
        kernel_on_device if square else plain_on_device,
        mesh=mesh,
        in_specs=(P("ta", None, ("px", "py")), P(("px", "py")), P()),
        out_specs=(P("ta", None, None, None, ("px", "py")), P("ta", None, None, None)),
        check_vma=False,
    )
```

```python
import functools
import math

import jax
import jax.numpy as jnp
from jax import lax
from jax.experimental import pallas as pl
from jax.experimental.pallas import tpu as pltpu
from jax.sharding import PartitionSpec as P

VARS = 5
BLK = 256
HOP = 128
SEGMENT_NUMBER = 2
RETAINED_MODES = 32

MESH = pl.DeviceIdType.MESH


def make_rotation_multipliers(spectral_indices, temporal_locations):
    segment_beginnings = jnp.arange(SEGMENT_NUMBER, dtype=jnp.int32) * HOP
    segment_shifts = temporal_locations[None, :] - segment_beginnings[:, None]
    inside = (segment_shifts >= 0) & (segment_shifts < BLK)
    window = 0.5 - 0.5 * jnp.cos(2.0 * math.pi * segment_shifts.astype(jnp.float32) / BLK)
    window = jnp.where(inside, window, jnp.float32(0.0)) / jnp.sqrt(jnp.float32(3.0 * BLK / 8.0))
    phases = jnp.mod(spectral_indices[:, None, None] * segment_shifts[None, :, :], BLK)
    angles = 2.0 * math.pi * phases.astype(jnp.float32) / BLK
    real_part = jnp.cos(angles) * window[None]
    imag_part = -jnp.sin(angles) * window[None]
    gathered_segments = jnp.stack([real_part, imag_part], axis=2)
    return gathered_segments.reshape(
        RETAINED_MODES * SEGMENT_NUMBER * 2, temporal_locations.shape[0]
    ).astype(jnp.bfloat16)


def gram_terms(spectra):
    flat = spectra.reshape(spectra.shape[0], 2 * SEGMENT_NUMBER, -1)
    inner = jnp.einsum("fam,fbm->fab", flat, flat, precision=lax.Precision.HIGHEST)
    inner = inner.reshape(spectra.shape[0], SEGMENT_NUMBER, 2, SEGMENT_NUMBER, 2)
    real_part = inner[:, :, 0, :, 0] + inner[:, :, 1, :, 1]
    imag_part = inner[:, :, 0, :, 1] - inner[:, :, 1, :, 0]
    return jnp.stack([real_part, imag_part], axis=-1)


def plain_on_device(snapshots, quad_weights, spectral_indices):
    record_length = snapshots.shape[0]
    point_count = snapshots.shape[2]
    groups = lax.axis_size("ta")
    temporal_locations = lax.axis_index("ta") * record_length + jnp.arange(
        record_length, dtype=jnp.int32
    )
    rotation_multipliers = make_rotation_multipliers(spectral_indices, temporal_locations)
    flat_snapshots = snapshots.reshape(record_length, VARS * point_count)
    raw = lax.psum_scatter(
        jnp.dot(rotation_multipliers, flat_snapshots, preferred_element_type=jnp.float32),
        "ta",
        scatter_dimension=0,
        tiled=True,
    )
    raw = raw.reshape(RETAINED_MODES // groups, SEGMENT_NUMBER, 2, VARS, point_count)
    spectra = raw * jnp.sqrt(quad_weights)
    summed = lax.psum(gram_terms(spectra), ("px", "py"))
    total_points = point_count * lax.axis_size("px") * lax.axis_size("py")
    gram = summed / jnp.float32(total_points * VARS)
    return (spectra, gram)


def sine_of_turn(m):
    quarter = BLK // 4
    r = jnp.bitwise_and(m + quarter, BLK - 1) - quarter
    r = jnp.where(r > quarter, BLK // 2 - r, r)
    x = r.astype(jnp.float32) * (2.0 * math.pi / BLK)
    y = x * x
    total = jnp.full_like(x, -1.0 / math.factorial(11))
    for n in (9, 7, 5, 3, 1):
        total = total * y + (1.0 if n % 4 == 1 else -1.0) / math.factorial(n)
    return total * x


def window_kernel(
    pieces, tail, tile, gram_scale,
    snap_hbm, weight_hbm, index_hbm, out_ref, gram_ref,
    snap, index_ref, weight_ref, twiddle, own, root,
    a_send, a_recv, n1_send, n1_recv, n2_send, n2_recv, m1_send, m1_recv,
    relay, moved, p_send, p_recv, pre, e_send, e_recv, acc, gram_send, gram_recv,
    load_sem, index_sem, weight_sem,
    a_ssem, a_rsem, n1_ssem, n1_rsem, n2_ssem, n2_rsem, m1_ssem, m1_rsem,
    moved_ssem, moved_rsem, relay_ssem, relay_rsem, lift_ssem, lift_rsem,
    p_ssem, p_rsem, e_ssem, e_rsem, gram_ssem, gram_rsem, ready_sem,
):
    px, py, ta = lax.axis_index("px"), lax.axis_index("py"), lax.axis_index("ta")
    npx, npy = lax.axis_size("px"), lax.axis_size("py")
    variables, record, points = snap_hbm.shape
    modes = out_ref.shape[0]
    unit = 2 * modes
    steps = variables * pieces
    span = points // pieces
    half = span // 2
    short = span // tail
    common = steps - 4
    batch = 3 if steps % 3 == 1 else 1
    lifts, lift = relay.shape[0], relay.shape[3]
    shift = moved.shape[2]
    kept, shifted = pl.ds(0, half - shift), pl.ds(half - shift, shift)
    f32, bf16 = jnp.float32, jnp.bfloat16

    inner = (ta == 1) | (ta == 2)
    outer = jnp.logical_not(inner)
    me = jnp.where(inner, ta - 1, ta // 3)
    sides = (jnp.where(inner, 0, 1), jnp.where(inner, 3, 2))

    @pl.when(outer & (me == 0))
    def _():
        a_recv[:, 0, :, shifted] = jnp.zeros((2, SEGMENT_NUMBER * unit, shift), bf16)

    def load(k):
        there = pl.ds(pl.multiple_of(lax.rem(k, pieces) * span, span), span)
        return pltpu.make_async_copy(
            snap_hbm.at[k // pieces, :, there], snap.at[k // pieces, :, there], load_sem.at[k])

    index_copy = pltpu.make_async_copy(index_hbm, index_ref, index_sem)
    weight_copy = pltpu.make_async_copy(weight_hbm, weight_ref, weight_sem)
    index_copy.start()
    load(0).start()

    peers = [
        (i, j, lax.rem(px + i, npx), lax.rem(py + j, npy))
        for i in range(npx) for j in range(npy) if i + j > 0
    ]
    barrier = pltpu.get_barrier_semaphore()
    for side in sides:
        pl.semaphore_signal(barrier, inc=1, device_id=(px, py, side), device_id_type=MESH)
    for i in range(1, npx):
        pl.semaphore_signal(barrier, inc=1, device_id=(lax.rem(px + i, npx), py, ta), device_id_type=MESH)
    below, above = py > 0, py < npy - 1
    for there, step in ((below, -1), (above, 1)):
        @pl.when(there)
        def _():
            pl.semaphore_signal(barrier, inc=1, device_id=(px, py + step, ta), device_id_type=MESH)
    greeted = len(sides) + npx - 1 + jnp.where(below, 1, 0) + jnp.where(above, 1, 0)

    sublane = lax.broadcasted_iota(jnp.int32, (modes, record), 0)
    moment = lax.broadcasted_iota(jnp.int32, (modes, record), 1) + ta * record
    shifts, windows = [], []
    for block in range(SEGMENT_NUMBER):
        shift = moment - block * HOP
        inside = (shift >= 0) & (shift < BLK)
        hann = 0.5 - 0.5 * sine_of_turn(shift + BLK // 4)
        shifts.append(shift)
        windows.append(jnp.where(inside, hann, 0.0) / math.sqrt(3.0 * BLK / 8.0))
    index_copy.wait()
    for place, owner in enumerate((3 - ta, sides[0], sides[1], ta)):
        bins = jnp.zeros((modes, record), jnp.int32)
        for f in range(modes):
            bins = jnp.where(sublane == f, index_ref[owner * modes + f], bins)
        for block in range(SEGMENT_NUMBER):
            shift, hann = shifts[block], windows[block]
            phase = bins * shift
            rows = jnp.concatenate(
                [sine_of_turn(phase + BLK // 4) * hann, -sine_of_turn(phase) * hann], axis=0)
            if place < 3:
                at = jnp.where(inner, place * SEGMENT_NUMBER + block, block * 3 + place)
                twiddle[pl.ds(pl.multiple_of(at * unit, unit), unit), :] = rows.astype(bf16)
            else:
                own[block * unit:(block + 1) * unit, :] = rows.astype(bf16)
    acc[...] = jnp.zeros_like(acc)

    a_refs = (a_send, a_recv, a_ssem, a_rsem)
    n1_refs = (n1_send, n1_recv, n1_ssem, n1_rsem)
    n2_refs = (n2_send, n2_recv, n2_ssem, n2_rsem)

    def batch_copy(refs, here, side, first, count):
        send, recv, ssem, rsem = refs
        units = pl.ds(first, count)
        return pltpu.make_async_remote_copy(
            src_ref=send.at[side, units], dst_ref=recv.at[here, units],
            send_sem=ssem.at[side, first], recv_sem=rsem.at[here, first],
            device_id=(px, py, sides[side]), device_id_type=MESH,
        )

    m1_refs = (m1_send, m1_recv, m1_ssem, m1_rsem)

    def kept_copy(here):
        return pltpu.make_async_remote_copy(
            src_ref=a_send.at[0, 0, :, kept], dst_ref=a_recv.at[here, 0, :, kept],
            send_sem=a_ssem.at[0, 0], recv_sem=a_rsem.at[here, 0],
            device_id=(px, py, sides[0]), device_id_type=MESH,
        )

    def shifted_copy(here):
        return pltpu.make_async_remote_copy(
            src_ref=a_send.at[0, 0, :, shifted], dst_ref=moved.at[here],
            send_sem=moved_ssem.at[0], recv_sem=moved_rsem.at[here],
            device_id=(px, py, sides[1]), device_id_type=MESH,
        )

    def forward_copy(here):
        return pltpu.make_async_remote_copy(
            src_ref=moved.at[here], dst_ref=moved.at[0],
            send_sem=moved_ssem.at[here], recv_sem=moved_rsem.at[0],
            device_id=(px, py, sides[1 - here]), device_id_type=MESH,
        )

    def start_batch(refs, side, k):
        @pl.when(k == 0)
        def _():
            if refs is a_refs and side == 0:
                @pl.when(inner)
                def _():
                    kept_copy(me).start()
                    shifted_copy(me).start()

                @pl.when(outer)
                def _():
                    batch_copy(refs, me, side, 0, 1).start()
            else:
                batch_copy(refs, me, side, 0, 1).start()

        @pl.when((k > 0) & (lax.rem(k, batch) == 0))
        def _():
            batch_copy(refs, me, side, k + 1 - batch, batch).start()

    def wait_batch(refs, side, k):
        @pl.when(k == 0)
        def _():
            if refs is a_refs:
                relays = outer & (me == 0)

                @pl.when(relays)
                def _():
                    kept_copy(side).wait_recv()

                @pl.when(jnp.logical_not(relays))
                def _():
                    batch_copy(refs, side, side, 0, 1).wait_recv()
            else:
                batch_copy(refs, side, side, 0, 1).wait_recv()

        @pl.when((k > 0) & (lax.rem(k - 1, batch) == 0))
        def _():
            batch_copy(refs, side, side, k, batch).wait_recv()

    def wait_sent(refs, side, first=None):
        (first or batch_copy(refs, me, side, 0, 1)).wait_send()

        @pl.loop(0, (steps - 1) // batch)
        def _(n):
            batch_copy(refs, me, side, 1 + n * batch, batch).wait_send()

    def tail_copy(here, side, k, n):
        columns = pl.ds(pl.multiple_of(n * short, short), short)
        return pltpu.make_async_remote_copy(
            src_ref=m1_send.at[side, k, :, columns], dst_ref=m1_recv.at[here, k, :, columns],
            send_sem=m1_ssem.at[side, steps + n], recv_sem=m1_rsem.at[here, steps + n],
            device_id=(px, py, sides[side]), device_id_type=MESH,
        )

    def up_copy(here, c):
        return pltpu.make_async_remote_copy(
            src_ref=m1_send.at[0, 0, :, pl.ds(c * lift, lift)], dst_ref=relay.at[c, here],
            send_sem=lift_ssem.at[c], recv_sem=relay_rsem.at[c, here],
            device_id=(px, py + 1, sides[0]), device_id_type=MESH,
        )

    def down_copy(side, c):
        return pltpu.make_async_remote_copy(
            src_ref=relay.at[c, side], dst_ref=m1_recv.at[side, 0, :, pl.ds(c * lift, lift)],
            send_sem=relay_ssem.at[c, side], recv_sem=lift_rsem.at[c, side],
            device_id=(px, py - 1, ta), device_id_type=MESH,
        )

    def comes_up(c):
        return (py > 0) & (c < npy - py)

    def rest_copy(here, side, n):
        columns = pl.ds(n * lift, span - n * lift)
        return pltpu.make_async_remote_copy(
            src_ref=m1_send.at[side, 0, :, columns], dst_ref=m1_recv.at[here, 0, :, columns],
            send_sem=m1_ssem.at[side, 0], recv_sem=m1_rsem.at[here, 0],
            device_id=(px, py, sides[side]), device_id_type=MESH,
        )

    def p_copy(here, side, u):
        return pltpu.make_async_remote_copy(
            src_ref=p_send.at[side, u], dst_ref=p_recv.at[here, u],
            send_sem=p_ssem.at[side, u], recv_sem=p_rsem.at[here, u],
            device_id=(px, py, sides[side]), device_id_type=MESH,
        )

    beside = jnp.bitwise_xor(py, 1) if npy % 2 == 0 else py

    def e_copy(here, side):
        return pltpu.make_async_remote_copy(
            src_ref=e_send.at[side], dst_ref=e_recv.at[here],
            send_sem=e_ssem.at[side], recv_sem=e_rsem.at[here],
            device_id=(px, beside, sides[side]), device_id_type=MESH,
        )

    def columns(k, at):
        return pl.ds(pl.multiple_of(lax.rem(k, pieces) * span + at, 128), tile)

    def transform(rows, k, at):
        return jnp.dot(rows, snap[k // pieces, :, columns(k, at)], preferred_element_type=f32)

    def loaded(k):
        load(k).wait()

        @pl.when(k == 0)
        def _():
            for later in range(1, steps):
                load(later).start()
            weight_copy.start()

    def tiles(width, unroll=1):
        def run(body):
            @pl.loop(0, width // tile, unroll=unroll)
            def _(i):
                body(pl.multiple_of(i * tile, tile))
        return run

    def meet(k):
        @pl.when(k == 0)
        def _():
            pl.semaphore_wait(barrier, greeted)

    def learn_of_peers():
        for n, (back, forth, step) in enumerate(((below, above, 1), (above, below, -1))):
            @pl.when(back)
            def _():
                pl.semaphore_wait(ready_sem.at[n], 1)

            @pl.when(forth)
            def _():
                pl.semaphore_signal(
                    ready_sem.at[n], inc=1, device_id=(px, py + step, ta), device_id_type=MESH)

        for i in range(1, npx):
            pl.semaphore_signal(
                ready_sem.at[2], inc=1, device_id=(lax.rem(px + i, npx), py, ta), device_id_type=MESH)
        if npx > 1:
            pl.semaphore_wait(ready_sem.at[2], npx - 1)

    def weighted(k, at, both):
        weight = root[:, columns(k, at)]
        return [
            (both[b * unit:b * unit + modes] * weight, both[b * unit + modes:(b + 1) * unit] * weight)
            for b in range(SEGMENT_NUMBER)]

    def add_terms(place, parts):
        (r0, i0), (r1, i1) = parts
        terms = (r0 * r0 + i0 * i0, r1 * r1 + i1 * i1, r0 * r1 + i0 * i1, r0 * i1 - i0 * r1)
        for n, term in enumerate(terms):
            lanes = [term[:, c:c + 128] for c in range(0, tile, 128)]
            acc[place, n] += functools.reduce(jnp.add, lanes)

    def store(k, at, parts):
        here = columns(k, at)
        for block, pair in enumerate(parts):
            for c in range(2):
                out_ref[:, block, k // pieces, c, here] = pair[c]

    def sums_of(place):
        lane = lax.broadcasted_iota(jnp.int32, gram_send.shape, 1)
        sums = jnp.zeros(gram_send.shape, f32)
        for n in range(4):
            sums = jnp.where(lane == n, jnp.sum(acc[place, n], axis=1, keepdims=True), sums)
        return sums

    def gram_copy(n):
        i, j, x, y = peers[n]
        return pltpu.make_async_remote_copy(
            src_ref=gram_send, dst_ref=gram_recv.at[n],
            send_sem=gram_ssem.at[n], recv_sem=gram_rsem.at[n],
            device_id=(x, y, ta), device_id_type=MESH,
        )

    def exchange(sums):
        gram_send[...] = sums
        for n in range(len(peers)):
            gram_copy(n).start()

    def weights():
        weight_copy.wait()
        root[...] = jnp.sqrt(weight_ref[...])

    def gather():
        total = gram_send[...]
        for n in range(len(peers)):
            gram_copy(n).wait()
            total = total + gram_recv[n]
        row = lax.broadcasted_iota(jnp.int32, (8, 128), 0)
        lane = lax.broadcasted_iota(jnp.int32, (8, 128), 1)
        pick = jnp.zeros((8, 128), f32)
        for r, n, sign in ((0, 0, 1.0), (2, 2, 1.0), (3, 3, 1.0), (4, 2, 1.0), (5, 3, -1.0), (6, 1, 1.0)):
            pick = jnp.where((row == r) & (lane == n), sign, pick)
        gram_ref[...] = gram_scale * lax.dot_general(
            pick, total, (((1,), (1,)), ((), ())),
            precision=lax.Precision.HIGHEST, preferred_element_type=f32,
        )

    @pl.when(inner)
    def _():
        @pl.loop(0, steps)
        def _(k):
            loaded(k)
            for side in range(2):
                @tiles(half, 4)
                def _(at):
                    a_send[side, k, :, pl.ds(at, tile)] = transform(
                        twiddle[0:2 * unit, :], k, side * half + at).astype(bf16)
                if side == 0:
                    meet(k)

                start_batch(a_refs, side, k)

        @pl.loop(0, steps)
        def _(k):
            for side in range(2):
                wait_batch(n2_refs, side, k)

        @pl.loop(0, steps)
        def _(j):
            k = jnp.where(
                j < 2, common + 2 * (1 - me) + j,
                jnp.where(j < common + 2, j - 2, 2 * me + j - 2))
            for dependent in range(2):
                first = half * (me if dependent else 1 - me)
                @tiles(half)
                def _(at):
                    product = transform(twiddle[2 * unit:6 * unit, :], k, first + at)
                    there = pl.ds(pl.multiple_of(first + at, 128), tile)
                    for side in range(2):
                        for block in range(SEGMENT_NUMBER):
                            r = (side * SEGMENT_NUMBER + block) * unit
                            rows = product[r:r + unit]
                            if dependent and block != side:
                                rows = rows + n2_recv[block, k, :, pl.ds(at, tile)].astype(f32)
                            m1_send[side, k, block * unit:(block + 1) * unit, there] = rows.astype(bf16)

            @pl.when(j == 1)
            def _():
                for side in range(2):
                    batch_copy(m1_refs, me, side, k - 1, 2).start()

            @pl.when(k == 0)
            def _():
                for n in range(lifts + 1):
                    @pl.when(n == npy - 1 - py)
                    def _():
                        for c in range(n):
                            up_copy(me, c).start()
                        rest_copy(me, 0, n).start()
                rest_copy(me, 1, 0).start()

            @pl.when(k == common - 3)
            def _():
                for side in range(2):
                    batch_copy(m1_refs, me, side, 1, common - 3).start()

            @pl.when(k == common - 1)
            def _():
                for side in range(2):
                    batch_copy(m1_refs, me, side, common - 2, 2).start()

            @pl.when(j == steps - 2)
            def _():
                for side in range(2):
                    batch_copy(m1_refs, me, side, k, 1).start()

            @pl.when(j == steps - 1)
            def _():
                for n in range(tail):
                    for side in range(2):
                        tail_copy(me, side, k, n).start()

        weights()
        learn_of_peers()

        @pl.loop(0, steps)
        def _(k):
            for side in range(2):
                wait_batch(a_refs, side, k)
                wait_batch(n1_refs, side, k)

            @pl.when(k == 0)
            def _():
                forward_copy(0).wait_recv()
                both = a_recv[0, 0, :, shifted].astype(f32) + moved[0].astype(f32)
                a_recv[0, 0, :, shifted] = both.astype(bf16)

            for side in range(2):
                @tiles(half)
                def _(at):
                    both = transform(own[...], k, side * half + at)
                    both = both + a_recv[side, k, :, pl.ds(at, tile)].astype(f32)
                    extra = n1_recv[1 - side, k, :, pl.ds(at, tile)].astype(f32)
                    rows = [both[:unit], both[unit:]]
                    rows[1 - side] = rows[1 - side] + extra
                    parts = weighted(k, side * half + at, jnp.concatenate(rows, axis=0))
                    add_terms(0, parts)
                    store(k, side * half + at, parts)

        exchange(sums_of(0))
        for u in range(2):
            for side in range(2):
                p_copy(side, side, u).wait_recv()

                @tiles(span, 2)
                def _(at):
                    there = pl.ds(at, tile)
                    k = common + 2 * me + u
                    both = p_recv[side, u, :, there].astype(f32) + m1_send[side, k, :, there].astype(f32)
                    add_terms(1 + side, weighted(k, at, both))

        for side in range(2):
            e_send[side] = sums_of(1 + side)
            e_copy(me, side).start()

        gather()
        shifted_copy(me).wait_send()
        for side in range(2):
            e_copy(me, side).wait_send()
            wait_sent(a_refs, side, kept_copy(me) if side == 0 else None)
            batch_copy(m1_refs, me, side, common + 2 * (1 - me), 2).wait_send()
            batch_copy(m1_refs, me, side, 1, common - 3).wait_send()
            batch_copy(m1_refs, me, side, common - 2, 2).wait_send()
            batch_copy(m1_refs, me, side, common + 2 * me, 1).wait_send()

            @pl.loop(0, tail)
            def _(n):
                tail_copy(me, side, common + 2 * me + 1, n).wait_send()

        for n in range(lifts + 1):
            @pl.when(n == npy - 1 - py)
            def _():
                for c in range(n):
                    up_copy(me, c).wait_send()
                rest_copy(me, 0, n).wait_send()
        rest_copy(me, 1, 0).wait_send()

    @pl.when(outer)
    def _():
        base = me * (3 * unit)
        far = pl.ds(pl.multiple_of(base, unit), unit)
        near = pl.ds(pl.multiple_of(base + unit, unit), 2 * unit)

        @pl.loop(0, steps)
        def _(k):
            loaded(k)
            for side in range(2):
                @tiles(half, 4)
                def _(at):
                    n2_send[side, k, :, pl.ds(at, tile)] = transform(
                        twiddle[far, :], k, side * half + at).astype(bf16)
                if side == 0:
                    meet(k)
                start_batch(n2_refs, side, k)

        @pl.loop(0, steps)
        def _(k):
            @tiles(half)
            def _(at):
                product = transform(twiddle[near, :], k, (1 - me) * half + at)
                for side in range(2):
                    n1_send[side, k, :, pl.ds(at, tile)] = product[side * unit:(side + 1) * unit].astype(bf16)
            for side in range(2):
                start_batch(n1_refs, side, k)
            for side in range(2):
                wait_batch(a_refs, side, k)

            @pl.when((k == 0) & (me == 1))
            def _():
                for side in range(2):
                    shifted_copy(side).wait_recv()
                    forward_copy(side).start()

            @tiles(half)
            def _(at):
                here = pl.ds(at, tile)
                product = transform(twiddle[near, :], k, me * half + at)
                for side in range(2):
                    rows = product[side * unit:(side + 1) * unit]
                    for block in range(SEGMENT_NUMBER):
                        there = slice(block * unit, (block + 1) * unit)
                        came = a_recv[1 - side, k, there, here].astype(f32)
                        total = came + jnp.where(me == block, rows, 0.0)
                        a_send[side, k, there, here] = total.astype(bf16)
            for side in range(2):
                start_batch(a_refs, side, k)

        weights()

        for c in range(lifts):
            @pl.when(comes_up(c) & (me == 0))
            def _():
                for side in range(2):
                    up_copy(side, c).wait_recv()
                    down_copy(side, c).start()

        for u in range(2):
            for side in range(2):
                k = common + 2 * side + u
                if u == 0:
                    batch_copy(m1_refs, 1 - side, 1 - side, k, 2).wait_recv()

                @tiles(span, 2)
                def _(at):
                    there = pl.ds(at, tile)
                    both = transform(own[...], k, at) + m1_recv[1 - side, k, :, there].astype(f32)
                    p_send[side, u, :, there] = both.astype(bf16)
                    pre[side, u, :, there] = both

                p_copy(me, side, u).start()

        learn_of_peers()

        def arrived(k, at):
            there = pl.ds(at, tile)
            both = transform(own[...], k, at)
            return weighted(k, at, both + (
                m1_recv[0, k, :, there].astype(f32) + m1_recv[1, k, :, there].astype(f32)))

        def arrive(k, first, width):
            @tiles(width, 2)
            def _(at):
                at = pl.multiple_of(first + at, tile)
                parts = arrived(k, at)
                add_terms(0, parts)
                store(k, at, parts)

        @pl.loop(0, common)
        def _(k):
            @pl.when(k == 0)
            def _():
                for n in range(lifts + 1):
                    @pl.when((me == 0) & (n == npy - 1 - py))
                    def _():
                        for side in range(2):
                            for c in range(n):
                                down_copy(side, c).wait_recv()
                            rest_copy(side, side, n).wait_recv()

                @pl.when(me == 1)
                def _():
                    for side in range(2):
                        rest_copy(side, side, 0).wait_recv()

            for first, count in ((1, common - 3), (common - 2, 2)):
                @pl.when(k == first)
                def _():
                    for side in range(2):
                        batch_copy(m1_refs, side, side, first, count).wait_recv()

            arrive(k, 0, span)

        sums = sums_of(0)
        for side in range(2):
            e_copy(side, side).wait_recv()
            sums = sums + e_recv[side]
        exchange(sums)

        for side in range(2):
            for refs in (a_refs, n1_refs, n2_refs):
                wait_sent(refs, side)

            @pl.when(me == 1)
            def _():
                forward_copy(side).wait_send()

        for side in range(2):
            for u in range(2):
                p_copy(me, side, u).wait_send()

        for c in range(lifts):
            @pl.when(comes_up(c) & (me == 0))
            def _():
                for side in range(2):
                    down_copy(side, c).wait_send()

        def complete(side, u, at):
            k = common + 2 * side + u
            there = pl.ds(at, tile)
            store(k, at, weighted(
                k, at, pre[side, u, :, there] + m1_recv[side, k, :, there].astype(f32)))

        for side in range(2):
            batch_copy(m1_refs, side, side, common + 2 * side, 1).wait_recv()
            tiles(span, 2)(functools.partial(complete, side, 0))

        @pl.loop(0, tail)
        def _(n):
            @pl.when(n == tail // 2)
            def _():
                gather()

            for side in range(2):
                tail_copy(side, side, common + 2 * side + 1, n).wait_recv()
                for c in range(0, short, tile):
                    complete(side, 1, pl.multiple_of(n * short + c, tile))


def flush_kernel(spectra, gram, spectra_out, gram_out, sems):
    copies = [pltpu.make_async_copy(gram, gram_out, sems.at[0])]
    for f in range(spectra.shape[0]):
        copies.append(pltpu.make_async_copy(spectra.at[f], spectra_out.at[f], sems.at[f + 1]))
    for copy in copies:
        copy.start()
    for copy in copies:
        copy.wait()


def kernel_on_device(snapshots, quad_weights, spectral_indices):
    record, variables, points = snapshots.shape
    groups = lax.axis_size("ta")
    npx, npy = lax.axis_size("px"), lax.axis_size("py")
    modes = spectral_indices.shape[0] // groups
    unit = 2 * modes
    pieces, tail = 2, 4
    span = points // pieces
    half = span // 2
    tile = math.gcd(512, span // tail)
    steps = variables * pieces
    lift = min(256, span // npy)
    lifts = npy - 1
    shift = min(512, half // 2)
    bf16, f32 = jnp.bfloat16, jnp.float32
    peers = npx * npy - 1
    dma = pltpu.SemaphoreType.DMA
    hbm = pl.BlockSpec(memory_space=pltpu.HBM)
    vmem = pl.BlockSpec(memory_space=pltpu.VMEM)
    spectra, gram = pl.pallas_call(
        functools.partial(
            window_kernel, pieces, tail, tile, 1.0 / (points * npx * npy * variables)),
        out_shape=(
            jax.ShapeDtypeStruct((modes, SEGMENT_NUMBER, variables, 2, points), f32),
            jax.ShapeDtypeStruct((SEGMENT_NUMBER * SEGMENT_NUMBER * 2, modes), f32),
        ),
        in_specs=[hbm, hbm, hbm],
        out_specs=(vmem, vmem),
        scratch_shapes=[
            pltpu.VMEM((variables, record, points), bf16),
            pltpu.SMEM(spectral_indices.shape, jnp.int32),
            pltpu.VMEM((1, points), f32),
            pltpu.VMEM((3 * SEGMENT_NUMBER * unit, record), bf16),
            pltpu.VMEM((SEGMENT_NUMBER * unit, record), bf16),
            pltpu.VMEM((1, points), f32),
            pltpu.VMEM((2, steps, SEGMENT_NUMBER * unit, half), bf16),
            pltpu.VMEM((2, steps, SEGMENT_NUMBER * unit, half), bf16),
            pltpu.VMEM((2, steps, unit, half), bf16),
            pltpu.VMEM((2, steps, unit, half), bf16),
            pltpu.VMEM((2, steps, unit, half), bf16),
            pltpu.VMEM((2, steps, unit, half), bf16),
            pltpu.VMEM((2, steps, SEGMENT_NUMBER * unit, span), bf16),
            pltpu.VMEM((2, steps, SEGMENT_NUMBER * unit, span), bf16),
            pltpu.VMEM((lifts, 2, SEGMENT_NUMBER * unit, lift), bf16),
            pltpu.VMEM((2, SEGMENT_NUMBER * unit, shift), bf16),
            pltpu.VMEM((2, 2, SEGMENT_NUMBER * unit, span), bf16),
            pltpu.VMEM((2, 2, SEGMENT_NUMBER * unit, span), bf16),
            pltpu.VMEM((2, 2, SEGMENT_NUMBER * unit, span), f32),
            pltpu.VMEM((2, modes, 128), f32),
            pltpu.VMEM((2, modes, 128), f32),
            pltpu.VMEM((3, 4, modes, 128), f32),
            pltpu.VMEM((modes, 128), f32),
            pltpu.VMEM((peers, modes, 128), f32),
            dma((steps,)), dma, dma,
            dma((2, steps)), dma((2, steps)), dma((2, steps)), dma((2, steps)),
            dma((2, steps)), dma((2, steps)),
            dma((2, steps + tail)), dma((2, steps + tail)),
            dma((2,)), dma((2,)), dma((lifts, 2)), dma((lifts, 2)), dma((lifts,)), dma((lifts, 2)),
            dma((2, 2)), dma((2, 2)), dma((2,)), dma((2,)),
            dma((peers,)), dma((peers,)),
            pltpu.SemaphoreType.REGULAR((3,)),
        ],
        compiler_params=pltpu.CompilerParams(
            collective_id=0, has_side_effects=True, vmem_limit_bytes=44 * 1024 * 1024),
        name="window_transform",
    )(*(
        pltpu.with_memory_space_constraint(a, pltpu.HBM)
        for a in (snapshots.transpose(1, 0, 2), quad_weights.reshape(1, points), spectral_indices)
    ))
    spectra, gram = pl.pallas_call(
        flush_kernel,
        out_shape=(
            jax.ShapeDtypeStruct(spectra.shape, f32), jax.ShapeDtypeStruct(gram.shape, f32)),
        in_specs=[vmem, vmem],
        out_specs=(hbm, hbm),
        scratch_shapes=[dma((modes + 1,))],
        compiler_params=pltpu.CompilerParams(vmem_limit_bytes=1024 * 1024),
        name="flush",
    )(*(pltpu.with_memory_space_constraint(a, pltpu.VMEM) for a in (spectra, gram)))
    gram = gram.reshape(SEGMENT_NUMBER, SEGMENT_NUMBER, 2, modes)
    return spectra.transpose(0, 1, 3, 2, 4), gram.transpose(3, 0, 1, 2)


def solution(mesh):
    square = mesh.shape["ta"] == 4
    return jax.shard_map(
        kernel_on_device if square else plain_on_device,
        mesh=mesh,
        in_specs=(P("ta", None, ("px", "py")), P(("px", "py")), P()),
        out_specs=(P("ta", None, None, None, ("px", "py")), P("ta", None, None, None)),
        check_vma=False,
    )
```
